128 devices in a mesh: asset: 32 (over y, z, core), tm: 4 (over x).
Axes of the slice: x: 4, y: 4, z: 4, core: 2. Of those that a mesh axis runs over, the one named last changes fastest.
Arguments:
- values: float32 [4, 1024, 65536], P(None, 'tm', 'asset'), may hold values from -64 to 64
- listed_from: int32 [65536], P('asset'), may hold values from -1024 to 1023, as said below
- listed_until: int32 [65536], P('asset'), may hold values from -960 to 3070, as said below
Outputs:
- standardized: float32 [4, 1024, 65536], P(None, 'tm', 'asset')
The draws below stay inside these ranges and needn't reach their ends.
Inputs may be any that keep to these rules, and one draw needn't show every extreme that they name: listed_until[a] - listed_from[a] is at least 64. listed_until[a] - listed_from[a] is at least 64.
All inputs are finite; a program needn't handle non-finite values.
Results may differ from the reference program's by a relative error of at most 0.00005.
Values sent between devices are 32-bit elements; how exact they have to be, the bound alone decides.
A program may use at most 128 MiB of HBM per device.

```python
import jax
import jax.numpy as jnp
from jax import lax

F = 4
WINDOW = 64
TIME = 1024
ASSETS = 65536


def listing_dates(key):
    base = jax.random.fold_in(key, 7)
    key_start, key_length = jax.random.split(base)
    first_stamp = jax.random.randint(key_start, (ASSETS,), -TIME, TIME, dtype=jnp.int32)
    length = jax.random.randint(key_length, (ASSETS,), WINDOW, 2 * TIME, dtype=jnp.int32)
    return (first_stamp, first_stamp + length)


def draw_listed_from(key, part):
    return listing_dates(key)[0]


def draw_listed_until(key, part):
    return listing_dates(key)[1]


def draw_values(key, part):
    base = jax.random.fold_in(key, 11)
    key_noise, key_scale, key_common, key_drift = jax.random.split(base, 4)
    noise_draw = jax.random.normal(key_noise, (F, TIME, ASSETS), jnp.float32)
    field_values = 8.0 * noise_draw
    return jnp.clip(field_values, -64.0, 64.0)


def setup_inputs(seed: int = 0) -> dict:
    arg_keys = jax.random.split(jax.random.key(seed), 4)
    values = draw_values(jax.random.fold_in(arg_keys[3], 71), 0)
    listed_from = draw_listed_from(jax.random.fold_in(arg_keys[3], 71), 0)
    listed_until = draw_listed_until(jax.random.fold_in(arg_keys[3], 71), 0)
    return {"values": values, "listed_from": listed_from, "listed_until": listed_until}


def standardize(field_values, weight, present):
    center = lax.optimization_barrier(jnp.sum(weight * field_values, axis=1)) / present
    deviate = (field_values - center[:, None]) * weight
    spread = lax.optimization_barrier(jnp.sum(deviate * deviate, axis=1)) / present
    return deviate / jnp.sqrt(spread + 0.1)[:, None]

def reference(values, listed_from, listed_until):
    stamps = jnp.arange(TIME, dtype=jnp.int32)[:, None]
    opened = listed_from[None, :]
    closed = listed_until[None, :]
    weight = ((stamps >= opened) & (stamps < closed)).astype(values.dtype)
    window_low = jnp.maximum(jnp.maximum(stamps - (WINDOW - 1), opened), 0)
    window_high = jnp.minimum(stamps, closed - 1)
    counted = jnp.maximum(window_high - window_low + 1, 1).astype(values.dtype)
    present = jnp.maximum(lax.optimization_barrier(jnp.sum(weight, axis=1)), 1.0)

    def one_field(field_values):
        window_sum = lax.reduce_window(field_values * weight, jnp.zeros((), field_values.dtype), lax.add, (WINDOW, 1), (1, 1), ((WINDOW - 1, 0), (0, 0)))
        rolling = window_sum / counted
        clipped = jnp.clip(standardize(rolling, weight, present), -3.0, 3.0)
        return standardize(clipped, weight, present)
    return lax.map(one_field, values)
```

```python
import functools

import jax
import jax.numpy as jnp
from jax import lax
from jax.experimental import pallas as pl
from jax.experimental.pallas import tpu as pltpu
from jax.sharding import PartitionSpec as P

WINDOW = 64
TILE = 8
LANES = 128
CHUNK = 512
MESH = pl.DeviceIdType.MESH


def kernel(
    sizes,
    vals,
    opened,
    closed,
    out,
    halo,
    hop1,
    hop2,
    ring,
    total,
    base,
    ahead,
    pivot,
    msg_b1,
    msg_b2,
    msg_h1,
    msg_h2,
    got_b1,
    got_b2,
    got_h1,
    got_h2,
    count_b,
    count_h,
    floor_b,
    floor_h,
    row_b1,
    row_b2,
    row_h1,
    row_h2,
    load_sem,
    direct_send,
    back_send,
    relay1_send,
    relay2_send,
    halo_recv,
    hop1_recv,
    hop2_recv,
    ex_send,
    ex_recv,
):
    blocks_t, peers = sizes
    fields, rows, assets = vals.shape
    tiles = rows // TILE
    wt = WINDOW // TILE
    chunks = assets // CHUNK
    bulk = tiles - wt
    back_field = fields - 1
    x = lax.axis_index("tm")
    me = lax.axis_index("asset")
    nxt = lax.rem(x + 1, blocks_t)
    prv = lax.rem(x + blocks_t - 1, blocks_t)
    t0 = x * rows

    def load(f, b):
        part = pl.ds(b * WINDOW, WINDOW)
        return pltpu.make_async_copy(
            vals.at[f, part, :], out.at[f, part, :], load_sem.at[f, b]
        )

    for b in range(rows // WINDOW):
        for f in range(fields):
            load(f, b).start()

    barrier = pltpu.get_barrier_semaphore()
    for t in (nxt, prv):
        pl.semaphore_signal(barrier, 1, device_id={"tm": t}, device_id_type=MESH)

    def greet(k, carry):
        peer = lax.rem(me + k, peers)
        pl.semaphore_signal(barrier, 1, device_id={"asset": peer}, device_id_type=MESH)
        return carry

    lax.fori_loop(1, peers, greet, 0)
    pl.semaphore_wait(barrier, peers + 1)

    tail = rows - WINDOW

    def tile_rows(r):
        return pl.ds(r * TILE, TILE)

    def direct(f, r):
        return pltpu.make_async_remote_copy(
            src_ref=vals.at[f, pl.ds(tail + r * TILE, TILE), :],
            dst_ref=halo.at[f, tile_rows(r), :],
            send_sem=direct_send,
            recv_sem=halo_recv.at[f, r],
            device_id={"tm": nxt},
            device_id_type=MESH,
        )

    def back(r):
        return pltpu.make_async_remote_copy(
            src_ref=vals.at[back_field, pl.ds(tail + r * TILE, TILE), :],
            dst_ref=hop1.at[tile_rows(r), :],
            send_sem=back_send,
            recv_sem=hop1_recv.at[r],
            device_id={"tm": prv},
            device_id_type=MESH,
        )

    def relay1(r):
        return pltpu.make_async_remote_copy(
            src_ref=hop1.at[tile_rows(r), :],
            dst_ref=hop2.at[tile_rows(r), :],
            send_sem=relay1_send,
            recv_sem=hop2_recv.at[r],
            device_id={"tm": prv},
            device_id_type=MESH,
        )

    def relay2(r):
        return pltpu.make_async_remote_copy(
            src_ref=hop2.at[tile_rows(r), :],
            dst_ref=halo.at[back_field, tile_rows(r), :],
            send_sem=relay2_send,
            recv_sem=halo_recv.at[back_field, r],
            device_id={"tm": prv},
            device_id_type=MESH,
        )

    has_next = x < blocks_t - 1
    order = list(range(wt - 1, -1, -1))

    @pl.when(has_next)
    def _():
        for r in order:
            back(r).start()
            for f in range(back_field):
                direct(f, r).start()

    def exchange(g, msg, got, k):
        return pltpu.make_async_remote_copy(
            src_ref=msg,
            dst_ref=got.at[k],
            send_sem=ex_send.at[g],
            recv_sem=ex_recv.at[g],
            device_id={"asset": lax.rem(me + k, peers)},
            device_id_type=MESH,
        )

    def exchange_start(g, msg, got):
        def one(k, carry):
            exchange(g, msg, got, k).start()
            return carry

        lax.fori_loop(1, peers, one, 0)
        got[0] = msg[...]

    def exchange_all(g, got):
        others = got.at[pl.ds(1, peers - 1)]
        return pltpu.make_async_remote_copy(
            src_ref=others,
            dst_ref=others,
            send_sem=ex_send.at[g],
            recv_sem=ex_recv.at[g],
            device_id={"asset": me},
            device_id_type=MESH,
        )

    sub = lax.broadcasted_iota(jnp.int32, (TILE, LANES), 0)
    lane = lax.broadcasted_iota(jnp.int32, (TILE, LANES), 1)
    subc = lax.broadcasted_iota(jnp.int32, (TILE, CHUNK), 0)
    width = fields * TILE

    def lanes(c):
        return pl.ds(c * CHUNK, CHUNK)

    def fold(v):
        acc = v[:, :LANES]
        for i in range(1, CHUNK // LANES):
            acc = acc + v[:, i * LANES : (i + 1) * LANES]
        return acc

    def across(v):
        return jnp.sum(v, axis=1, keepdims=True)

    def flat(columns):
        z = jnp.zeros((TILE, LANES), jnp.float32)
        for at, column in columns:
            z = jnp.where(lane == sub + at, column, z)
        return jnp.sum(z, axis=0, keepdims=True)

    def column(row, at):
        return across(jnp.where(lane == sub + at, row, 0.0))

    def listed(c, first):
        t = subc + first
        o = opened[:, lanes(c)]
        u = closed[:, lanes(c)]
        return t, o, u, (t >= o) & (t < u)

    def share(t, o, u, w):
        low = jnp.maximum(jnp.maximum(t - (WINDOW - 1), o), 0)
        high = jnp.minimum(t, u - 1)
        counted = jnp.maximum(high - low + 1, 1).astype(jnp.float32)
        return jnp.where(w, 1.0 / counted, 0.0)

    def moments(n, s, q, pivots):
        count = across(n)
        inverse = 1.0 / jnp.maximum(count, 1.0)
        columns = []
        means = []
        for f in range(fields):
            s_f, q_f = across(s[f]), across(q[f])
            lift = s_f * inverse
            mean = pivots[f] + lift
            means.append(mean)
            columns.append((f * TILE, mean))
            columns.append((width + f * TILE, jnp.maximum(q_f - s_f * lift, 0.0)))
        return count, means, columns

    def counts_at(count, at):
        return [(at + f * TILE, count) for f in range(fields)]

    zero = jnp.zeros((TILE, LANES), jnp.float32)

    msg_b1[...] = jnp.zeros_like(msg_b1)
    base[...] = jnp.zeros_like(base)
    for f in range(fields):
        load(f, 0).wait()

    def prefix(f, c, w, v):
        p = jnp.where(w, v, 0.0)
        for k in (1, 2, 4):
            p = p + jnp.where(subc >= k, pltpu.roll(p, k, 0), 0.0)
        p = p + base[f, :, lanes(c)]
        base[f, :, lanes(c)] = jnp.broadcast_to(p[TILE - 1 :, :], p.shape)
        return p

    def first_tile(r, carry):
        n = zero
        here = pl.ds(pl.multiple_of(r * TILE, TILE), TILE)
        for c in range(chunks):
            _, _, _, w = listed(c, t0 + r * TILE)
            n = n + fold(jnp.where(w, 1.0, 0.0))
            for f in range(fields):
                p = prefix(f, c, w, out[f, here, lanes(c)])
                ring[f, here, lanes(c)] = p
                out[f, here, lanes(c)] = p
        msg_b1[pl.ds(r, 1), :] = flat(counts_at(across(n), 3 * width))
        return carry

    lax.fori_loop(0, wt, first_tile, 0)

    for f in range(fields):
        rough = zero
        for c in range(chunks):
            rough = rough + fold(base[f, :, lanes(c)])
        pivot[f] = jnp.broadcast_to(across(rough) * (1.0 / (WINDOW * assets)), zero.shape)

    def bulk_block(b, carry):
        total[...] = base[...]
        base[...] = jnp.zeros_like(base)

        def bulk_tile(i, carry):
            r = b * wt + i
            here = pl.ds(pl.multiple_of(r * TILE, TILE), TILE)
            slot = pl.ds(pl.multiple_of(i * TILE, TILE), TILE)
            n = zero
            s = [zero] * fields
            q = [zero] * fields
            pivots = [pivot[f][:, :1] for f in range(fields)]
            for c in range(chunks):
                t, o, u, w = listed(c, t0 + r * TILE)
                n = n + fold(jnp.where(w, 1.0, 0.0))
                part = share(t, o, u, w)
                for f in range(fields):
                    p = prefix(f, c, w, out[f, here, lanes(c)])
                    old = ring[f, slot, lanes(c)]
                    ring[f, slot, lanes(c)] = p
                    rolled = (p + (total[f, :, lanes(c)] - old)) * part
                    out[f, here, lanes(c)] = rolled
                    d = jnp.where(w, rolled - pivots[f], 0.0)
                    s[f] = s[f] + fold(d)
                    q[f] = q[f] + fold(d * d)
            count, means, columns = moments(n, s, q, pivots)
            for f in range(fields):
                pivot[f] = jnp.broadcast_to(means[f], zero.shape)
            at = pl.ds(r - wt, 1)
            msg_b1[at, :] = msg_b1[at, :] + flat(columns + counts_at(count, 2 * width))

            @pl.when(r == wt)
            def _():
                for f in range(fields):
                    ahead[f] = jnp.broadcast_to(means[f], zero.shape)

            return carry

        lax.fori_loop(0, wt, bulk_tile, 0)
        return carry

    for b in range(1, rows // WINDOW):
        for f in range(fields):
            load(f, b).wait()
    lax.fori_loop(1, rows // WINDOW, bulk_block, 0)
    exchange_start(0, msg_b1, got_b1)

    @pl.when(x != blocks_t - 2)
    def _():
        for r in order:
            back(r).wait_recv()
            relay1(r).start()

    def scaled(center, spread):
        inv = 1.0 / jnp.sqrt(jnp.maximum(spread, 0.0) + 0.1)
        wide = lax.broadcasted_iota(jnp.int32, center.shape, 1)
        return jnp.where(wide < width, center, pltpu.roll(inv, width, 1))

    def merge(got, counts, floor, m2, rows_out):
        shape = rows_out.shape

        def add(p, acc):
            return acc + counts[p] * got[p]

        center = lax.fori_loop(0, peers, add, jnp.zeros(shape, jnp.float32)) / floor[...]

        def add2(p, acc):
            d = got[p] - center
            return acc + counts[p] * d * d

        between = lax.fori_loop(0, peers, add2, jnp.zeros(shape, jnp.float32))
        rows_out[...] = scaled(center, (between + m2) / floor[...])

    def summed(got, shape):
        return lax.fori_loop(
            0, peers, lambda p, acc: acc + got[p], jnp.zeros(shape, jnp.float32)
        )

    def left(v, by):
        return pltpu.roll(v, LANES - by, 1)

    def clip_tile(r, row, row_in, msg, msg_row):
        here = pl.ds(pl.multiple_of(r * TILE, TILE), TILE)
        line = jnp.broadcast_to(row_in[pl.ds(row, 1), :], zero.shape)
        center = [column(line, f * TILE) for f in range(fields)]
        inv = [column(line, width + f * TILE) for f in range(fields)]
        s = [zero] * fields
        q = [zero] * fields
        for c in range(chunks):
            _, _, _, w = listed(c, t0 + r * TILE)
            for f in range(fields):
                y = (out[f, here, lanes(c)] - center[f]) * inv[f]
                y = jnp.where(w, jnp.clip(y, -3.0, 3.0), 0.0)
                out[f, here, lanes(c)] = y
                s[f] = s[f] + fold(y)
                q[f] = q[f] + fold(y * y)
        columns = []
        for f in range(fields):
            columns.append((f * TILE, across(s[f])))
            columns.append((width + f * TILE, across(q[f])))
        msg[pl.ds(msg_row, 1), :] = flat(columns)

    def merge2(got, floor, rows_out):
        sums = summed(got, rows_out.shape)
        center = sums / floor[...]
        spread = left(sums, width) / floor[...] - center * center
        rows_out[...] = scaled(center, spread)

    def final_tile(r, row, row_in):
        here = pl.ds(pl.multiple_of(r * TILE, TILE), TILE)
        line = jnp.broadcast_to(row_in[pl.ds(row, 1), :], zero.shape)
        center = [column(line, f * TILE) for f in range(fields)]
        inv = [column(line, width + f * TILE) for f in range(fields)]
        for c in range(chunks):
            _, _, _, w = listed(c, t0 + r * TILE)
            for f in range(fields):
                y = (out[f, here, lanes(c)] - center[f]) * inv[f]
                out[f, here, lanes(c)] = jnp.where(w, y, 0.0)

    def over(n, step):
        def one(i, carry):
            step(i)
            return carry

        lax.fori_loop(0, n, one, 0)

    exchange_all(0, got_b1).wait_recv()

    def split(p):
        v = got_b1[p]
        count_b[p] = left(v, 2 * width)
        count_h[p] = left(v[:wt, :], 3 * width)

    over(peers, split)
    sums = summed(got_b1, (bulk, LANES))
    floor_b[...] = jnp.maximum(left(sums, 2 * width), 1.0)
    floor_h[...] = jnp.maximum(left(sums[:wt, :], 3 * width), 1.0)
    merge(got_b1, count_b, floor_b, left(sums, width), row_b1)
    over(bulk, lambda i: clip_tile(i + wt, i, row_b1, msg_b2, i))
    exchange_start(1, msg_b2, got_b2)

    @pl.when(x != blocks_t - 3)
    def _():
        for r in order:
            relay1(r).wait_recv()
            relay2(r).start()

    exchange_all(1, got_b2).wait_recv()
    merge2(got_b2, floor_b, row_b2)
    over(bulk, lambda i: final_tile(i + wt, i, row_b2))

    base[...] = jnp.zeros_like(base)
    pivot[...] = ahead[...]

    def halo_tile(k):
        r = wt - 1 - k
        here = pl.ds(pl.multiple_of(r * TILE, TILE), TILE)

        @pl.when(x > 0)
        def _():
            for f in range(back_field):
                direct(f, r).wait_recv()
            relay2(r).wait_recv()

        n = zero
        s = [zero] * fields
        q = [zero] * fields
        pivots = [pivot[f][:, :1] for f in range(fields)]
        for c in range(chunks):
            t, o, u, w = listed(c, t0 + r * TILE)
            _, _, _, past = listed(c, t0 + r * TILE - WINDOW)
            past = past & (t >= WINDOW)
            n = n + fold(jnp.where(w, 1.0, 0.0))
            part = share(t, o, u, w)
            for f in range(fields):
                h = jnp.where(past, halo[f, here, lanes(c)], 0.0)
                for j in (1, 2, 4):
                    up = pltpu.roll(h, TILE - j, 0)
                    h = h + jnp.where(subc < TILE - j, up, 0.0)
                before = base[f, :, lanes(c)]
                after = jnp.where(subc < TILE - 1, pltpu.roll(h, TILE - 1, 0), 0.0)
                base[f, :, lanes(c)] = before + jnp.broadcast_to(h[:1, :], h.shape)
                rolled = (out[f, here, lanes(c)] + (before + after)) * part
                out[f, here, lanes(c)] = rolled
                d = jnp.where(w, rolled - pivots[f], 0.0)
                s[f] = s[f] + fold(d)
                q[f] = q[f] + fold(d * d)
        _, means, columns = moments(n, s, q, pivots)
        for f in range(fields):
            pivot[f] = jnp.broadcast_to(means[f], zero.shape)
        msg_h1[pl.ds(r, 1), :] = flat(columns)

    over(wt, halo_tile)
    exchange_start(2, msg_h1, got_h1)
    exchange_all(2, got_h1).wait_recv()
    m2 = left(summed(got_h1, (wt, LANES)), width)
    merge(got_h1, count_h, floor_h, m2, row_h1)
    over(wt, lambda i: clip_tile(i, i, row_h1, msg_h2, i))
    exchange_start(3, msg_h2, got_h2)
    exchange_all(3, got_h2).wait_recv()
    merge2(got_h2, floor_h, row_h2)
    over(wt, lambda i: final_tile(i, i, row_h2))

    for g, got in enumerate((got_b1, got_b2, got_h1, got_h2)):
        exchange_all(g, got).wait_send()

    @pl.when(has_next)
    def _():
        for r in order:
            back(r).wait_send()
            for f in range(back_field):
                direct(f, r).wait_send()

    @pl.when(x != blocks_t - 2)
    def _():
        for r in order:
            relay1(r).wait_send()

    @pl.when(x != blocks_t - 3)
    def _():
        for r in order:
            relay2(r).wait_send()


def per_device(blocks_t, peers, values, listed_from, listed_until):
    fields, rows, assets = values.shape
    tiles = rows // TILE
    wt = WINDOW // TILE
    bulk = tiles - wt
    f32 = jnp.float32
    vmem = pltpu.VMEM
    dma = pltpu.SemaphoreType.DMA
    scratch = [
        vmem((fields, WINDOW, assets), f32),
        vmem((WINDOW, assets), f32),
        vmem((WINDOW, assets), f32),
        vmem((fields, WINDOW, assets), f32),
        vmem((fields, TILE, assets), f32),
        vmem((fields, TILE, assets), f32),
        vmem((fields, TILE, LANES), f32),
        vmem((fields, TILE, LANES), f32),
        vmem((bulk, LANES), f32),
        vmem((bulk, LANES), f32),
        vmem((wt, LANES), f32),
        vmem((wt, LANES), f32),
        vmem((peers, bulk, LANES), f32),
        vmem((peers, bulk, LANES), f32),
        vmem((peers, wt, LANES), f32),
        vmem((peers, wt, LANES), f32),
        vmem((peers, bulk, LANES), f32),
        vmem((peers, wt, LANES), f32),
        vmem((bulk, LANES), f32),
        vmem((wt, LANES), f32),
        vmem((bulk, LANES), f32),
        vmem((bulk, LANES), f32),
        vmem((wt, LANES), f32),
        vmem((wt, LANES), f32),
        dma((fields, rows // WINDOW)),
        dma,
        dma,
        dma,
        dma,
        dma((fields, wt)),
        dma((wt,)),
        dma((wt,)),
        dma((4,)),
        dma((4,)),
    ]
    return pl.pallas_call(
        functools.partial(kernel, (blocks_t, peers)),
        out_shape=jax.ShapeDtypeStruct(values.shape, values.dtype),
        in_specs=[
            pl.BlockSpec(memory_space=pltpu.HBM),
            pl.BlockSpec(memory_space=pltpu.VMEM),
            pl.BlockSpec(memory_space=pltpu.VMEM),
        ],
        out_specs=pl.BlockSpec(memory_space=pltpu.VMEM),
        scratch_shapes=scratch,
        compiler_params=pltpu.CompilerParams(
            collective_id=0,
            has_side_effects=True,
            vmem_limit_bytes=32 * 1024 * 1024,
        ),
    )(values, listed_from[None, :], listed_until[None, :])


def solution(mesh):
    in_specs = (P(None, "tm", "asset"), P("asset"), P("asset"))
    out_specs = P(None, "tm", "asset")
    body = functools.partial(per_device, mesh.shape["tm"], mesh.shape["asset"])
    return jax.shard_map(
        body, mesh=mesh, in_specs=in_specs, out_specs=out_specs, check_vma=False
    )
```

```python
import functools

import jax
import jax.numpy as jnp
from jax import lax
from jax.experimental import pallas as pl
from jax.experimental.pallas import tpu as pltpu
from jax.sharding import PartitionSpec as P

WINDOW = 64
TILE = 8
LANES = 128
CHUNK = 512
MESH = pl.DeviceIdType.MESH


def kernel(
    sizes,
    vals,
    opened_in,
    closed_in,
    out,
    opened,
    closed,
    list_sem,
    rounds,
    local_count,
    halo,
    hop1,
    hop2,
    ring,
    total,
    base,
    suffix,
    ahead,
    pivot,
    msg_b1,
    msg_b2,
    msg_g1,
    msg_g2,
    msg_h1,
    msg_h2,
    got_b1,
    got_b2,
    got_g1,
    got_g2,
    got_h1,
    got_h2,
    count_b,
    count_h,
    floor_b,
    floor_h,
    row_b1,
    row_b2,
    row_g1,
    row_g2,
    row_h1,
    row_h2,
    load_sem,
    direct_send,
    back_send,
    relay1_send,
    relay2_send,
    halo_recv,
    hop1_recv,
    hop2_recv,
    ex_send,
    ex_recv,
):
    blocks_t, peers = sizes
    fields, rows, assets = vals.shape
    tiles = rows // TILE
    wt = WINDOW // TILE
    chunks = assets // CHUNK
    bulk = tiles - wt
    back_field = fields - 1
    x = lax.axis_index("tm")
    me = lax.axis_index("asset")
    nxt = lax.rem(x + 1, blocks_t)
    prv = lax.rem(x + blocks_t - 1, blocks_t)
    t0 = x * rows

    dates = [
        pltpu.make_async_copy(opened_in, opened, list_sem.at[0]),
        pltpu.make_async_copy(closed_in, closed, list_sem.at[1]),
    ]
    for copy in dates:
        copy.start()

    def load(f, b):
        part = pl.ds(b * WINDOW, WINDOW)
        return pltpu.make_async_copy(
            vals.at[f, part, :], out.at[f, part, :], load_sem.at[f, b]
        )

    for b in range(rows // WINDOW):
        for f in range(fields):
            load(f, b).start()

    core = lax.rem(me, 2)
    chip = me // 2
    y, z = chip // 4, lax.rem(chip, 4)

    def at_place(dy, dz, dc):
        to = lax.rem(y + dy, 4) * 4 + lax.rem(z + dz, 4)
        return to * 2 + lax.rem(core + dc, 2)

    near = [at_place(0, 0, 1)]
    near += [at_place(1, 0, 0), at_place(3, 0, 0), at_place(0, 1, 0), at_place(0, 3, 0)]
    barrier = pltpu.get_barrier_semaphore()
    for t in (nxt, prv):
        pl.semaphore_signal(barrier, 1, device_id={"tm": t}, device_id_type=MESH)
    for peer in near:
        pl.semaphore_signal(barrier, 1, device_id={"asset": peer}, device_id_type=MESH)
    pl.semaphore_wait(barrier, 2 + len(near))

    def tell(i):
        for peer in near:
            pl.semaphore_signal(
                rounds.at[i], 1, device_id={"asset": peer}, device_id_type=MESH
            )

    def hear(i):
        pl.semaphore_wait(rounds.at[i], len(near))

    tell(0)

    tail = rows - WINDOW

    def tile_rows(r):
        return pl.ds(r * TILE, TILE)

    def direct(f, r):
        return pltpu.make_async_remote_copy(
            src_ref=vals.at[f, pl.ds(tail + r * TILE, TILE), :],
            dst_ref=halo.at[f, tile_rows(r), :],
            send_sem=direct_send,
            recv_sem=halo_recv.at[f, r],
            device_id={"tm": nxt},
            device_id_type=MESH,
        )

    def back(r):
        return pltpu.make_async_remote_copy(
            src_ref=vals.at[back_field, pl.ds(tail + r * TILE, TILE), :],
            dst_ref=hop1.at[tile_rows(r), :],
            send_sem=back_send,
            recv_sem=hop1_recv.at[r],
            device_id={"tm": prv},
            device_id_type=MESH,
        )

    def relay1(r):
        return pltpu.make_async_remote_copy(
            src_ref=hop1.at[tile_rows(r), :],
            dst_ref=hop2.at[tile_rows(r), :],
            send_sem=relay1_send,
            recv_sem=hop2_recv.at[r],
            device_id={"tm": prv},
            device_id_type=MESH,
        )

    def relay2(r):
        return pltpu.make_async_remote_copy(
            src_ref=hop2.at[tile_rows(r), :],
            dst_ref=halo.at[back_field, tile_rows(r), :],
            send_sem=relay2_send,
            recv_sem=halo_recv.at[back_field, r],
            device_id={"tm": prv},
            device_id_type=MESH,
        )

    has_next = x < blocks_t - 1
    order = list(range(wt - 1, -1, -1))

    @pl.when(has_next)
    def _():
        for r in order:
            back(r).start()
            for f in range(back_field):
                direct(f, r).start()

    def hops(d):
        return min(d[0], 4 - d[0]) + min(d[1], 4 - d[1]) + d[2] / 2

    places = [(dy, dz, dc) for dy in range(4) for dz in range(4) for dc in range(2)]
    places = sorted(places[1:], key=hops, reverse=True)

    def exchange(g, msg, got, k, peer):
        return pltpu.make_async_remote_copy(
            src_ref=msg,
            dst_ref=got.at[k],
            send_sem=ex_send.at[g],
            recv_sem=ex_recv.at[g],
            device_id={"asset": peer},
            device_id_type=MESH,
        )

    def exchange_start(g, msg, got):
        for d in places:
            k = (d[0] * 4 + d[1]) * 2 + d[2]
            exchange(g, msg, got, k, at_place(*d)).start()
        got[0] = msg[...]

    def exchange_all(g, got):
        others = got.at[pl.ds(1, peers - 1)]
        return pltpu.make_async_remote_copy(
            src_ref=others,
            dst_ref=others,
            send_sem=ex_send.at[g],
            recv_sem=ex_recv.at[g],
            device_id={"asset": me},
            device_id_type=MESH,
        )

    sub = lax.broadcasted_iota(jnp.int32, (TILE, LANES), 0)
    lane = lax.broadcasted_iota(jnp.int32, (TILE, LANES), 1)
    subc = lax.broadcasted_iota(jnp.int32, (TILE, CHUNK), 0)
    width = fields * TILE

    def lanes(c):
        return pl.ds(c * CHUNK, CHUNK)

    def fold(v):
        acc = v[:, :LANES]
        for i in range(1, CHUNK // LANES):
            acc = acc + v[:, i * LANES : (i + 1) * LANES]
        return acc

    def across(v):
        return jnp.sum(v, axis=1, keepdims=True)

    def flat(columns):
        z = jnp.zeros((TILE, LANES), jnp.float32)
        for at, column in columns:
            z = jnp.where(lane == sub + at, column, z)
        return jnp.sum(z, axis=0, keepdims=True)

    def column(row, at):
        return across(jnp.where(lane == sub + at, row, 0.0))

    def listed(c, first):
        t = subc + first
        o = opened[:, lanes(c)]
        u = closed[:, lanes(c)]
        return t, o, u, (t >= o) & (t < u)

    def share(t, o, u, w):
        low = jnp.maximum(jnp.maximum(t - (WINDOW - 1), o), 0)
        high = jnp.minimum(t, u - 1)
        counted = jnp.maximum(high - low + 1, 1).astype(jnp.float32)
        return jnp.where(w, 1.0 / counted, 0.0)

    def moments(count, s, q, pivots, which):
        inverse = 1.0 / jnp.maximum(count, 1.0)
        columns = []
        means = []
        for f, s_l, q_l, pivot_f in zip(which, s, q, pivots):
            s_f, q_f = across(s_l), across(q_l)
            lift = s_f * inverse
            mean = pivot_f + lift
            means.append(mean)
            columns.append((f * TILE, mean))
            columns.append((width + f * TILE, jnp.maximum(q_f - s_f * lift, 0.0)))
        return means, columns

    def counts_at(count, at):
        return [(at + f * TILE, count) for f in range(fields)]

    zero = jnp.zeros((TILE, LANES), jnp.float32)

    for copy in dates:
        copy.wait()
    msg_b1[...] = jnp.zeros_like(msg_b1)
    base[...] = jnp.zeros_like(base)
    for f in range(fields):
        load(f, 0).wait()

    def prefix(f, c, w, v):
        p = jnp.where(w, v, 0.0)
        for k in (1, 2, 4):
            p = p + jnp.where(subc >= k, pltpu.roll(p, k, 0), 0.0)
        p = p + base[f, :, lanes(c)]
        base[f, :, lanes(c)] = jnp.broadcast_to(p[TILE - 1 :, :], p.shape)
        return p

    def first_tile(r, carry):
        n = zero
        here = pl.ds(pl.multiple_of(r * TILE, TILE), TILE)
        for c in range(chunks):
            _, _, _, w = listed(c, t0 + r * TILE)
            n = n + fold(jnp.where(w, 1.0, 0.0))
            for f in range(fields):
                p = prefix(f, c, w, out[f, here, lanes(c)])
                ring[f, here, lanes(c)] = p
                out[f, here, lanes(c)] = p
        count = across(n)
        local_count[r] = jnp.broadcast_to(count, zero.shape)
        msg_b1[pl.ds(wt - 1 - r, 1), :] = flat(counts_at(count, 3 * width))
        return carry

    lax.fori_loop(0, wt, first_tile, 0)

    for f in range(fields):
        rough = zero
        for c in range(chunks):
            rough = rough + fold(base[f, :, lanes(c)])
        pivot[f] = jnp.broadcast_to(across(rough) * (1.0 / (WINDOW * assets)), zero.shape)

    every = list(range(fields))

    def bulk_tile(b, i, pivots):
        r = b * wt + i
        here = pl.ds(pl.multiple_of(r * TILE, TILE), TILE)
        slot = pl.ds(pl.multiple_of(i * TILE, TILE), TILE)
        n = zero
        s = [zero] * fields
        q = [zero] * fields
        for c in range(chunks):
            t, o, u, w = listed(c, t0 + r * TILE)
            n = n + fold(jnp.where(w, 1.0, 0.0))
            part = share(t, o, u, w)
            for f in range(fields):
                p = prefix(f, c, w, out[f, here, lanes(c)])
                old = ring[f, slot, lanes(c)]
                ring[f, slot, lanes(c)] = p
                rolled = (p + (total[f, :, lanes(c)] - old)) * part
                out[f, here, lanes(c)] = rolled
                d = jnp.where(w, rolled - pivots[f], 0.0)
                s[f] = s[f] + fold(d)
                q[f] = q[f] + fold(d * d)
        count = across(n)
        means, columns = moments(count, s, q, pivots, every)
        at = pl.ds(r - wt, 1)
        msg_b1[at, :] = msg_b1[at, :] + flat(columns + counts_at(count, 2 * width))
        return means

    def bulk_block(b):
        total[...] = base[...]
        base[...] = jnp.zeros_like(base)

        def pair(i, carry):
            pivots = [pivot[f][:, :1] for f in range(fields)]
            lower = bulk_tile(b, 2 * i, pivots)
            upper = bulk_tile(b, 2 * i + 1, pivots)
            for f in range(fields):
                pivot[f] = jnp.broadcast_to(upper[f], zero.shape)
            if b == 1:

                @pl.when(i == 0)
                def _():
                    for f in range(fields):
                        ahead[f] = jnp.broadcast_to(lower[f], zero.shape)

            return carry

        lax.fori_loop(0, wt // 2, pair, 0)

    for b in range(1, rows // WINDOW):
        hear(b - 1)
        tell(b)
        for f in range(fields):
            load(f, b).wait()
        bulk_block(b)
    hear(rows // WINDOW - 1)
    exchange_start(0, msg_b1, got_b1)

    @pl.when(x != blocks_t - 2)
    def _():
        for r in order:
            back(r).wait_recv()
            relay1(r).start()

    def scaled(center, spread):
        inv = 1.0 / jnp.sqrt(jnp.maximum(spread, 0.0) + 0.1)
        wide = lax.broadcasted_iota(jnp.int32, center.shape, 1)
        return jnp.where(wide < width, center, pltpu.roll(inv, width, 1))

    def left(v, by):
        return pltpu.roll(v, LANES - by, 1)

    def sum_over(term, shape):
        step = 8
        nothing = tuple(jnp.zeros(shape, jnp.float32) for _ in range(2))

        def some(i, acc):
            acc = list(acc)
            for j in range(step):
                acc[j % 2] = acc[j % 2] + term(i * step + j)
            return tuple(acc)

        if shape[0] == 1:
            acc = nothing
            for i in range(peers // step):
                acc = some(i, acc)
        else:
            acc = lax.fori_loop(0, peers // step, some, nothing)
        return acc[0] + acc[1]

    def merge(got, counts, floor, m2, rows_out):
        shape = rows_out.shape
        center = sum_over(lambda p: counts(p) * got[p], shape) / floor

        def spread_term(p):
            d = got[p] - center
            return counts(p) * d * d

        rows_out[...] = scaled(center, (sum_over(spread_term, shape) + m2) / floor)

    def summed(got):
        return sum_over(lambda p: got[p], got.shape[1:])

    def apply_tile(r, row, row_in, clipping):
        here = pl.ds(pl.multiple_of(r * TILE, TILE), TILE)
        line = jnp.broadcast_to(row_in[pl.ds(row, 1), :], zero.shape)
        center = [column(line, f * TILE) for f in range(fields)]
        inv = [column(line, width + f * TILE) for f in range(fields)]
        s = [zero] * fields
        q = [zero] * fields
        for c in range(chunks):
            _, _, _, w = listed(c, t0 + r * TILE)
            for f in range(fields):
                y = (out[f, here, lanes(c)] - center[f]) * inv[f]
                if clipping:
                    y = jnp.clip(y, -3.0, 3.0)
                y = jnp.where(w, y, 0.0)
                out[f, here, lanes(c)] = y
                if clipping:
                    s[f] = s[f] + fold(y)
                    q[f] = q[f] + fold(y * y)
        return s, q

    def clip_tile(r, row, row_in, msg, msg_row):
        s, q = apply_tile(r, row, row_in, True)
        columns = []
        for f in range(fields):
            columns.append((f * TILE, across(s[f])))
            columns.append((width + f * TILE, across(q[f])))
        msg[pl.ds(msg_row, 1), :] = flat(columns)

    def merge2(got, floor, rows_out):
        sums = summed(got)
        center = sums / floor
        spread = left(sums, width) / floor - center * center
        rows_out[...] = scaled(center, spread)

    def final_tile(r, row, row_in):
        apply_tile(r, row, row_in, False)

    def over(n, step, unroll=1):
        def one(i, carry):
            step(i)
            return carry

        lax.fori_loop(0, n, one, 0, unroll=unroll)

    def halo_part(r, which):
        here = tile_rows(r)

        @pl.when(x > 0)
        def _():
            for f in which:
                if f == back_field:
                    relay2(r).wait_recv()
                else:
                    direct(f, r).wait_recv()

        s = [zero] * len(which)
        q = [zero] * len(which)
        pivots = [ahead[f][:, :1] for f in which]
        for c in range(chunks):
            t, o, u, w = listed(c, t0 + r * TILE)
            _, _, _, past = listed(c, t0 + r * TILE - WINDOW)
            past = past & (t >= WINDOW)
            part = share(t, o, u, w)
            for i, f in enumerate(which):
                h = jnp.where(past, halo[f, here, lanes(c)], 0.0)
                for j in (1, 2, 4):
                    up = pltpu.roll(h, TILE - j, 0)
                    h = h + jnp.where(subc < TILE - j, up, 0.0)
                before = suffix[f, :, lanes(c)]
                after = jnp.where(subc < TILE - 1, pltpu.roll(h, TILE - 1, 0), 0.0)
                suffix[f, :, lanes(c)] = before + jnp.broadcast_to(h[:1, :], h.shape)
                rolled = (out[f, here, lanes(c)] + (before + after)) * part
                out[f, here, lanes(c)] = rolled
                d = jnp.where(w, rolled - pivots[i], 0.0)
                s[i] = s[i] + fold(d)
                q[i] = q[i] + fold(d * d)
        count = local_count[r][:, :1]
        means, columns = moments(count, s, q, pivots, which)
        for i, f in enumerate(which):
            ahead[f] = jnp.broadcast_to(means[i], zero.shape)
        line = flat(columns)
        if r == 0:
            at, msg = pl.ds(0, 1), msg_h1
        else:
            at, msg = pl.ds(wt - 1 - r, 1), msg_g1
        msg[at, :] = msg[at, :] + line

    suffix[...] = jnp.zeros_like(suffix)
    msg_h1[...] = jnp.zeros_like(msg_h1)
    msg_g1[...] = jnp.zeros_like(msg_g1)
    fore = every[:back_field]
    rear = [back_field]

    halo_part(7, fore)
    halo_part(6, fore)
    exchange_all(0, got_b1).wait_recv()

    def split(p):
        v = got_b1[p]
        count_b[p] = left(v, 2 * width)
        count_h[p] = left(v[:wt, :], 3 * width)

    over(peers, split, 8)
    sums = summed(got_b1)
    floor_b[...] = jnp.maximum(left(sums, 2 * width), 1.0)
    floor_h[...] = jnp.maximum(left(sums[:wt, :], 3 * width), 1.0)
    merge(got_b1, lambda p: count_b[p], floor_b[...], left(sums, width), row_b1)
    halo_part(5, fore)
    over(bulk, lambda i: clip_tile(i + wt, i, row_b1, msg_b2, i), 2)
    exchange_start(1, msg_b2, got_b2)
    halo_part(4, fore)

    @pl.when(x != blocks_t - 3)
    def _():
        for r in order:
            relay1(r).wait_recv()
            relay2(r).start()

    halo_part(3, fore)
    exchange_all(1, got_b2).wait_recv()
    merge2(got_b2, floor_b[...], row_b2)
    over(bulk, lambda i: final_tile(i + wt, i, row_b2), 2)
    halo_part(2, fore)
    for r in order[:5]:
        halo_part(r, rear)
    halo_part(1, fore)
    for r in order[5:7]:
        halo_part(r, rear)
    exchange_start(2, msg_g1, got_g1)
    halo_part(0, fore)
    halo_part(0, rear)
    exchange_start(3, msg_h1, got_h1)

    front = wt - 1
    exchange_all(2, got_g1).wait_recv()
    m2 = left(summed(got_g1), width)
    merge(got_g1, lambda p: count_h[p, :front, :], floor_h[:front, :], m2, row_g1)
    over(front, lambda i: clip_tile(front - i, i, row_g1, msg_g2, i), front)
    exchange_start(4, msg_g2, got_g2)
    exchange_all(3, got_h1).wait_recv()
    m2 = left(summed(got_h1), width)
    merge(got_h1, lambda p: count_h[p, front:, :], floor_h[front:, :], m2, row_h1)
    clip_tile(0, 0, row_h1, msg_h2, 0)
    exchange_start(5, msg_h2, got_h2)
    exchange_all(4, got_g2).wait_recv()
    merge2(got_g2, floor_h[:front, :], row_g2)
    over(front, lambda i: final_tile(front - i, i, row_g2), front)
    exchange_all(5, got_h2).wait_recv()
    merge2(got_h2, floor_h[front:, :], row_h2)
    final_tile(0, 0, row_h2)

    for g, got in enumerate((got_b1, got_b2, got_g1, got_h1, got_g2, got_h2)):
        exchange_all(g, got).wait_send()

    @pl.when(has_next)
    def _():
        for r in order:
            back(r).wait_send()
            for f in range(back_field):
                direct(f, r).wait_send()

    @pl.when(x != blocks_t - 2)
    def _():
        for r in order:
            relay1(r).wait_send()

    @pl.when(x != blocks_t - 3)
    def _():
        for r in order:
            relay2(r).wait_send()


def per_device(blocks_t, peers, values, listed_from, listed_until):
    fields, rows, assets = values.shape
    tiles = rows // TILE
    wt = WINDOW // TILE
    bulk = tiles - wt
    f32 = jnp.float32
    vmem = pltpu.VMEM
    dma = pltpu.SemaphoreType.DMA
    scratch = [
        vmem((1, assets), jnp.int32),
        vmem((1, assets), jnp.int32),
        dma((2,)),
        pltpu.SemaphoreType.REGULAR((4,)),
        vmem((wt, TILE, LANES), f32),
        vmem((fields, WINDOW, assets), f32),
        vmem((WINDOW, assets), f32),
        vmem((WINDOW, assets), f32),
        vmem((fields, WINDOW, assets), f32),
        vmem((fields, TILE, assets), f32),
        vmem((fields, TILE, assets), f32),
        vmem((fields, TILE, assets), f32),
        vmem((fields, TILE, LANES), f32),
        vmem((fields, TILE, LANES), f32),
        *[vmem((n, LANES), f32) for n in (bulk, bulk, wt - 1, wt - 1, 1, 1)],
        *[vmem((peers, n, LANES), f32) for n in (bulk, bulk, wt - 1, wt - 1, 1, 1)],
        *[vmem((peers, n, LANES), f32) for n in (bulk, wt)],
        *[vmem((n, LANES), f32) for n in (bulk, wt)],
        *[vmem((n, LANES), f32) for n in (bulk, bulk, wt - 1, wt - 1, 1, 1)],
        dma((fields, rows // WINDOW)),
        dma,
        dma,
        dma,
        dma,
        dma((fields, wt)),
        dma((wt,)),
        dma((wt,)),
        dma((6,)),
        dma((6,)),
    ]
    return pl.pallas_call(
        functools.partial(kernel, (blocks_t, peers)),
        out_shape=pltpu.VMEM(values.shape, values.dtype),
        in_specs=[
            pl.BlockSpec(memory_space=pltpu.HBM),
            pl.BlockSpec(memory_space=pltpu.HBM),
            pl.BlockSpec(memory_space=pltpu.HBM),
        ],
        out_specs=pl.BlockSpec(memory_space=pltpu.VMEM),
        scratch_shapes=scratch,
        compiler_params=pltpu.CompilerParams(
            collective_id=0,
            has_side_effects=True,
            vmem_limit_bytes=48 * 1024 * 1024,
        ),
    )(values, listed_from[None, :], listed_until[None, :])


def solution(mesh):
    in_specs = (P(None, "tm", "asset"), P("asset"), P("asset"))
    out_specs = P(None, "tm", "asset")
    body = functools.partial(per_device, mesh.shape["tm"], mesh.shape["asset"])
    return jax.shard_map(
        body, mesh=mesh, in_specs=in_specs, out_specs=out_specs, check_vma=False
    )
```

```python
import functools

import jax
import jax.numpy as jnp
from jax import lax
from jax.experimental import pallas as pl
from jax.experimental.pallas import tpu as pltpu
from jax.sharding import PartitionSpec as P

WINDOW = 64
EARLY = 3
LATE = 2
TILE = 8
LANES = 128
CHUNK = 512
MESH = pl.DeviceIdType.MESH


def kernel(
    sizes,
    vals,
    opened_in,
    closed_in,
    out,
    opened,
    closed,
    list_sem,
    rounds,
    local_count,
    halo,
    hop1,
    hop2,
    ext,
    params,
    told,
    ring,
    total,
    base,
    suffix,
    ahead,
    pivot,
    msg_b1,
    msg_b2,
    msg_e1,
    msg_e2,
    msg_g1,
    msg_g2,
    got_b1,
    got_b2,
    got_e1,
    got_e2,
    got_g1,
    got_g2,
    count_b,
    count_e,
    count_h,
    floor_b,
    floor_h,
    row_b1,
    row_b2,
    row_g1,
    row_g2,
    load_sem,
    direct_send,
    ext_send,
    ext_recv,
    told_send,
    told_recv,
    back_send,
    relay1_send,
    relay2_send,
    halo_recv,
    hop1_recv,
    hop2_recv,
    ex_send,
    ex_recv,
):
    blocks_t, peers = sizes
    fields, rows, assets = vals.shape
    tiles = rows // TILE
    wt = WINDOW // TILE
    chunks = assets // CHUNK
    bulk = tiles - wt
    x = lax.axis_index("tm")
    me = lax.axis_index("asset")
    nxt = lax.rem(x + 1, blocks_t)
    prv = lax.rem(x + blocks_t - 1, blocks_t)
    t0 = x * rows

    dates = [
        pltpu.make_async_copy(opened_in, opened, list_sem.at[0]),
        pltpu.make_async_copy(closed_in, closed, list_sem.at[1]),
    ]
    for copy in dates:
        copy.start()

    def load(f, b):
        part = pl.ds(b * WINDOW, WINDOW)
        return pltpu.make_async_copy(
            vals.at[f, part, :], out.at[f, part, :], load_sem.at[f, b]
        )

    for b in range(rows // WINDOW):
        for f in range(fields):
            load(f, b).start()

    core = lax.rem(me, 2)
    chip = me // 2
    y, z = chip // 4, lax.rem(chip, 4)

    def at_place(dy, dz, dc):
        to = lax.rem(y + dy, 4) * 4 + lax.rem(z + dz, 4)
        return to * 2 + lax.rem(core + dc, 2)

    near = [at_place(0, 0, 1)]
    near += [at_place(1, 0, 0), at_place(3, 0, 0), at_place(0, 1, 0), at_place(0, 3, 0)]
    barrier = pltpu.get_barrier_semaphore()
    for t in (nxt, prv):
        pl.semaphore_signal(barrier, 1, device_id={"tm": t}, device_id_type=MESH)
    for peer in near:
        pl.semaphore_signal(barrier, 1, device_id={"asset": peer}, device_id_type=MESH)
    pl.semaphore_wait(barrier, 2 + len(near))

    def tell(i):
        for peer in near:
            pl.semaphore_signal(
                rounds.at[i], 1, device_id={"asset": peer}, device_id_type=MESH
            )

    def hear(i):
        pl.semaphore_wait(rounds.at[i], len(near))

    tell(0)

    tail = rows - WINDOW

    def tile_rows(r):
        return pl.ds(r * TILE, TILE)

    every = list(range(fields))
    fore, rear = every[: fields - LATE], every[fields - LATE :]
    around = [(f, r) for r in range(EARLY - 1, -1, -1) for f in rear]

    def direct(f, r):
        return pltpu.make_async_remote_copy(
            src_ref=vals.at[f, pl.ds(tail + r * TILE, TILE), :],
            dst_ref=halo.at[f, tile_rows(r), :],
            send_sem=direct_send,
            recv_sem=halo_recv.at[f, r],
            device_id={"tm": nxt},
            device_id_type=MESH,
        )

    def back(k):
        f, r = around[k]
        return pltpu.make_async_remote_copy(
            src_ref=vals.at[f, pl.ds(tail + r * TILE, TILE), :],
            dst_ref=hop1.at[tile_rows(k), :],
            send_sem=back_send,
            recv_sem=hop1_recv.at[k],
            device_id={"tm": prv},
            device_id_type=MESH,
        )

    def relay1(k):
        return pltpu.make_async_remote_copy(
            src_ref=hop1.at[tile_rows(k), :],
            dst_ref=hop2.at[tile_rows(k), :],
            send_sem=relay1_send,
            recv_sem=hop2_recv.at[k],
            device_id={"tm": prv},
            device_id_type=MESH,
        )

    def relay2(k):
        f, r = around[k]
        return pltpu.make_async_remote_copy(
            src_ref=hop2.at[tile_rows(k), :],
            dst_ref=halo.at[f, tile_rows(r), :],
            send_sem=relay2_send,
            recv_sem=halo_recv.at[f, r],
            device_id={"tm": prv},
            device_id_type=MESH,
        )

    def pass1(ks):
        for k in ks:
            back(k).wait_recv()
            relay1(k).start()

    def pass2(ks):
        for k in ks:
            relay1(k).wait_recv()
            relay2(k).start()

    extension = pltpu.make_async_remote_copy(
        src_ref=vals.at[:, pl.ds(0, EARLY * TILE), :],
        dst_ref=ext,
        send_sem=ext_send,
        recv_sem=ext_recv,
        device_id={"tm": prv},
        device_id_type=MESH,
    )
    telling = pltpu.make_async_remote_copy(
        src_ref=params,
        dst_ref=told,
        send_sem=told_send,
        recv_sem=told_recv,
        device_id={"tm": nxt},
        device_id_type=MESH,
    )

    has_prev = x > 0
    has_next = x < blocks_t - 1
    last = x == blocks_t - 1
    hops1 = x != blocks_t - 2
    hops2 = x != blocks_t - 3
    straight = [
        (f, r) for r in range(wt - 1, -1, -1) for f in every if (f, r) not in around
    ]

    @pl.when(has_prev)
    def _():
        extension.start()

    @pl.when(has_next)
    def _():
        for k in range(len(around)):
            back(k).start()
        for f, r in straight:
            direct(f, r).start()

    def hops(d):
        return min(d[0], 4 - d[0]) + min(d[1], 4 - d[1]) + d[2] / 2

    places = [(dy, dz, dc) for dy in range(4) for dz in range(4) for dc in range(2)]
    places = sorted(places[1:], key=hops, reverse=True)

    def exchange(g, msg, got, k, peer):
        return pltpu.make_async_remote_copy(
            src_ref=msg,
            dst_ref=got.at[k],
            send_sem=ex_send.at[g],
            recv_sem=ex_recv.at[g],
            device_id={"asset": peer},
            device_id_type=MESH,
        )

    def exchange_start(g, msg, got):
        for d in places:
            k = (d[0] * 4 + d[1]) * 2 + d[2]
            exchange(g, msg, got, k, at_place(*d)).start()
        got[0] = msg[...]

    def exchange_all(g, got):
        others = got.at[pl.ds(1, peers - 1)]
        return pltpu.make_async_remote_copy(
            src_ref=others,
            dst_ref=others,
            send_sem=ex_send.at[g],
            recv_sem=ex_recv.at[g],
            device_id={"asset": me},
            device_id_type=MESH,
        )

    sub = lax.broadcasted_iota(jnp.int32, (TILE, LANES), 0)
    lane = lax.broadcasted_iota(jnp.int32, (TILE, LANES), 1)
    subc = lax.broadcasted_iota(jnp.int32, (TILE, CHUNK), 0)
    width = fields * TILE

    def lanes(c):
        return pl.ds(c * CHUNK, CHUNK)

    def fold(v):
        acc = v[:, :LANES]
        for i in range(1, CHUNK // LANES):
            acc = acc + v[:, i * LANES : (i + 1) * LANES]
        return acc

    def across(v):
        return jnp.sum(v, axis=1, keepdims=True)

    def flat(columns):
        z = jnp.zeros((TILE, LANES), jnp.float32)
        for at, column in columns:
            z = jnp.where(lane == sub + at, column, z)
        return jnp.sum(z, axis=0, keepdims=True)

    def column(row, at):
        return across(jnp.where(lane == sub + at, row, 0.0))

    def listed(c, first):
        t = subc + first
        o = opened[:, lanes(c)]
        u = closed[:, lanes(c)]
        return t, o, u, (t >= o) & (t < u)

    def share(t, o, u, w):
        low = jnp.maximum(jnp.maximum(t - (WINDOW - 1), o), 0)
        high = jnp.minimum(t, u - 1)
        counted = jnp.maximum(high - low + 1, 1).astype(jnp.float32)
        return jnp.where(w, 1.0 / counted, 0.0)

    def moments(count, s, q, pivots, which):
        inverse = 1.0 / jnp.maximum(count, 1.0)
        columns = []
        means = []
        for f, s_l, q_l, pivot_f in zip(which, s, q, pivots):
            s_f, q_f = across(s_l), across(q_l)
            lift = s_f * inverse
            mean = pivot_f + lift
            means.append(mean)
            columns.append((f * TILE, mean))
            columns.append((width + f * TILE, jnp.maximum(q_f - s_f * lift, 0.0)))
        return means, columns

    def counts_at(count, at):
        return [(at + f * TILE, count) for f in range(fields)]

    zero = jnp.zeros((TILE, LANES), jnp.float32)

    for copy in dates:
        copy.wait()
    msg_b1[...] = jnp.zeros_like(msg_b1)
    base[...] = jnp.zeros_like(base)
    for f in range(fields):
        load(f, 0).wait()

    def prefix(f, c, w, v):
        p = jnp.where(w, v, 0.0)
        for k in (1, 2, 4):
            p = p + jnp.where(subc >= k, pltpu.roll(p, k, 0), 0.0)
        p = p + base[f, :, lanes(c)]
        base[f, :, lanes(c)] = jnp.broadcast_to(p[TILE - 1 :, :], p.shape)
        return p

    def first_tile(r, carry):
        n = zero
        here = pl.ds(pl.multiple_of(r * TILE, TILE), TILE)
        for c in range(chunks):
            _, _, _, w = listed(c, t0 + r * TILE)
            n = n + fold(jnp.where(w, 1.0, 0.0))
            for f in range(fields):
                p = prefix(f, c, w, out[f, here, lanes(c)])
                ring[f, here, lanes(c)] = p
                out[f, here, lanes(c)] = p
        count = across(n)
        local_count[r] = jnp.broadcast_to(count, zero.shape)
        msg_b1[pl.ds(wt - 1 - r, 1), :] = flat(counts_at(count, 3 * width))
        return carry

    lax.fori_loop(0, wt, first_tile, 0)

    for f in range(fields):
        rough = zero
        for c in range(chunks):
            rough = rough + fold(base[f, :, lanes(c)])
        pivot[f] = jnp.broadcast_to(across(rough) * (1.0 / (WINDOW * assets)), zero.shape)

    def window_tile(ref, here, first, i, pivots):
        slot = pl.ds(pl.multiple_of(i * TILE, TILE), TILE)
        n = zero
        s = [zero] * fields
        q = [zero] * fields
        for c in range(chunks):
            t, o, u, w = listed(c, first)
            n = n + fold(jnp.where(w, 1.0, 0.0))
            part = share(t, o, u, w)
            for f in range(fields):
                p = prefix(f, c, w, ref[f, here, lanes(c)])
                old = ring[f, slot, lanes(c)]
                ring[f, slot, lanes(c)] = p
                rolled = (p + (total[f, :, lanes(c)] - old)) * part
                ref[f, here, lanes(c)] = rolled
                d = jnp.where(w, rolled - pivots[f], 0.0)
                s[f] = s[f] + fold(d)
                q[f] = q[f] + fold(d * d)
        count = across(n)
        means, columns = moments(count, s, q, pivots, every)
        return means, flat(columns + counts_at(count, 2 * width))

    def bulk_tile(b, i, pivots):
        r = b * wt + i
        here = pl.ds(pl.multiple_of(r * TILE, TILE), TILE)
        means, line = window_tile(out, here, t0 + r * TILE, i, pivots)
        at = pl.ds(r - wt, 1)
        msg_b1[at, :] = msg_b1[at, :] + line
        return means

    def bulk_block(b):
        total[...] = base[...]
        base[...] = jnp.zeros_like(base)

        def pair(i, carry):
            pivots = [pivot[f][:, :1] for f in range(fields)]
            lower = bulk_tile(b, 2 * i, pivots)
            upper = bulk_tile(b, 2 * i + 1, pivots)
            for f in range(fields):
                pivot[f] = jnp.broadcast_to(upper[f], zero.shape)
            if b == 1:

                @pl.when(i == 0)
                def _():
                    for f in range(fields):
                        ahead[f] = jnp.broadcast_to(lower[f], zero.shape)

            return carry

        lax.fori_loop(0, wt // 2, pair, 0)

    for b in range(1, rows // WINDOW):
        hear(b - 1)
        tell(b)
        for f in range(fields):
            load(f, b).wait()
        bulk_block(b)
    hear(rows // WINDOW - 1)
    exchange_start(0, msg_b1, got_b1)


    @pl.when(last)
    def _():
        pass1(range(len(around)))

    def scaled(center, spread):
        inv = 1.0 / jnp.sqrt(jnp.maximum(spread, 0.0) + 0.1)
        wide = lax.broadcasted_iota(jnp.int32, center.shape, 1)
        return jnp.where(wide < width, center, pltpu.roll(inv, width, 1))

    def left(v, by):
        return pltpu.roll(v, LANES - by, 1)

    def sum_over(term, shape):
        step = 8
        nothing = tuple(jnp.zeros(shape, jnp.float32) for _ in range(2))

        def some(i, acc):
            acc = list(acc)
            for j in range(step):
                acc[j % 2] = acc[j % 2] + term(i * step + j)
            return tuple(acc)

        if shape[0] <= TILE:
            acc = nothing
            for i in range(peers // step):
                acc = some(i, acc)
        else:
            acc = lax.fori_loop(0, peers // step, some, nothing)
        return acc[0] + acc[1]

    def merge(got, counts, floor, m2, rows_out):
        shape = rows_out.shape
        center = sum_over(lambda p: counts(p) * got[p], shape) / floor

        def spread_term(p):
            d = got[p] - center
            return counts(p) * d * d

        rows_out[...] = scaled(center, (sum_over(spread_term, shape) + m2) / floor)

    def summed(got):
        return sum_over(lambda p: got[p], got.shape[1:])

    def apply_tile(ref, r, row, row_in, clipping, keep=True):
        here = pl.ds(pl.multiple_of(r * TILE, TILE), TILE)
        first = t0 + r * TILE if ref is out else t0 + rows + r * TILE
        line = jnp.broadcast_to(row_in[pl.ds(row, 1), :], zero.shape)
        center = [column(line, f * TILE) for f in range(fields)]
        inv = [column(line, width + f * TILE) for f in range(fields)]
        s = [zero] * fields
        q = [zero] * fields
        for c in range(chunks):
            _, _, _, w = listed(c, first)
            for f in range(fields):
                y = (ref[f, here, lanes(c)] - center[f]) * inv[f]
                if clipping:
                    y = jnp.clip(y, -3.0, 3.0)
                y = jnp.where(w, y, 0.0)
                if keep:
                    ref[f, here, lanes(c)] = y
                if clipping:
                    s[f] = s[f] + fold(y)
                    q[f] = q[f] + fold(y * y)
        return s, q

    def clip_tile(ref, r, row, row_in, msg, msg_row):
        s, q = apply_tile(ref, r, row, row_in, True, ref is out)
        columns = []
        for f in range(fields):
            columns.append((f * TILE, across(s[f])))
            columns.append((width + f * TILE, across(q[f])))
        msg[pl.ds(msg_row, 1), :] = flat(columns)

    def merge2(got, floor, rows_out):
        sums = summed(got)
        center = sums / floor
        spread = left(sums, width) / floor - center * center
        rows_out[...] = scaled(center, spread)

    def final_tile(r, row, row_in):
        apply_tile(out, r, row, row_in, False)

    def over(n, step, unroll=1):
        def one(i, carry):
            step(i)
            return carry

        lax.fori_loop(0, n, one, 0, unroll=unroll)

    def arrival(f, r):
        k = around.index((f, r)) if (f, r) in around else None
        return direct(f, r) if k is None else relay2(k)

    def joined(f, c, here, past):
        h = jnp.where(past, halo[f, here, lanes(c)], 0.0)
        for j in (1, 2, 4):
            up = pltpu.roll(h, TILE - j, 0)
            h = h + jnp.where(subc < TILE - j, up, 0.0)
        before = suffix[f, :, lanes(c)]
        after = jnp.where(subc < TILE - 1, pltpu.roll(h, TILE - 1, 0), 0.0)
        suffix[f, :, lanes(c)] = before + jnp.broadcast_to(h[:1, :], h.shape)
        return out[f, here, lanes(c)] + (before + after)

    def before_mask(c, t, r):
        _, _, _, past = listed(c, t0 + r * TILE - WINDOW)
        return past & (t >= WINDOW)

    def halo_part(r, msg, row, extra):
        here = tile_rows(r)
        s = [zero] * fields
        q = [zero] * fields
        pivots = [ahead[f][:, :1] for f in every]
        for c in range(chunks):
            t, o, u, w = listed(c, t0 + r * TILE)
            past = before_mask(c, t, r)
            part = share(t, o, u, w)
            for f in every:
                rolled = joined(f, c, here, past) * part
                out[f, here, lanes(c)] = rolled
                d = jnp.where(w, rolled - pivots[f], 0.0)
                s[f] = s[f] + fold(d)
                q[f] = q[f] + fold(d * d)
        count = local_count[r][:, :1]
        means, columns = moments(count, s, q, pivots, every)
        for f in every:
            ahead[f] = jnp.broadcast_to(means[f], zero.shape)
        if extra:
            columns = columns + counts_at(count, 2 * width)
        msg[pl.ds(row, 1), :] = flat(columns)

    def group_tile(r):
        @pl.when(has_prev)
        def _():
            for f in every:
                arrival(f, r).wait_recv()

        halo_part(r, msg_g1, wt - 1 - r, False)

    def finish(r, which):
        here = tile_rows(r)
        lines = [jnp.broadcast_to(told[i, pl.ds(r, 1), :], zero.shape) for i in range(2)]
        center = [[column(line, f * TILE) for f in which] for line in lines]
        inv = [[column(line, width + f * TILE) for f in which] for line in lines]
        for f in which:
            arrival(f, r).wait_recv()
        for c in range(chunks):
            t, o, u, w = listed(c, t0 + r * TILE)
            past = before_mask(c, t, r)
            part = share(t, o, u, w)
            for i, f in enumerate(which):
                rolled = joined(f, c, here, past) * part
                y = jnp.clip((rolled - center[0][i]) * inv[0][i], -3.0, 3.0)
                y = (y - center[1][i]) * inv[1][i]
                out[f, here, lanes(c)] = jnp.where(w, y, 0.0)

    suffix[...] = jnp.zeros_like(suffix)
    msg_e1[...] = jnp.zeros_like(msg_e1)
    msg_e2[...] = jnp.zeros_like(msg_e2)


    def second(ks):
        @pl.when((x == 0) | last)
        def _():
            pass2(ks)

    group_tile(7)
    group_tile(6)

    @pl.when(x == 0)
    def _():
        for r in range(EARLY - 1, -1, -1):
            halo_part(r, msg_e1, EARLY + r, True)

    exchange_all(0, got_b1).wait_recv()

    def split(p):
        v = got_b1[p]
        count_b[p] = left(v, 2 * width)
        count_h[p] = left(v[:wt, :], 3 * width)

    over(peers, split, 8)
    sums = summed(got_b1)
    floor_b[...] = jnp.maximum(left(sums, 2 * width), 1.0)
    floor_h[...] = jnp.maximum(left(sums[:wt, :], 3 * width), 1.0)
    merge(got_b1, lambda p: count_b[p], floor_b[...], left(sums, width), row_b1)
    group_tile(5)

    @pl.when(has_next)
    def _():
        total[...] = base[...]
        base[...] = jnp.zeros_like(base)
        extension.wait_recv()

        def one(r, carry):
            here = pl.ds(pl.multiple_of(r * TILE, TILE), TILE)
            pivots = [pivot[f][:, :1] for f in every]
            means, line = window_tile(ext, here, t0 + rows + r * TILE, r, pivots)
            for f in every:
                pivot[f] = jnp.broadcast_to(means[f], zero.shape)
            msg_e1[pl.ds(r, 1), :] = line
            return carry

        lax.fori_loop(0, EARLY, one, 0)

    exchange_start(2, msg_e1, got_e1)
    over(bulk, lambda i: clip_tile(out, i + wt, i, row_b1, msg_b2, i), 2)
    exchange_start(1, msg_b2, got_b2)
    some = range(4)

    @pl.when(x < blocks_t - 2)
    def _():
        pass1(some)

    @pl.when(x == blocks_t - 2)
    def _():
        pass2(some)

    exchange_all(2, got_e1).wait_recv()

    def split_e(p):
        count_e[p] = left(got_e1[p], 2 * width)

    over(peers, split_e, peers)
    sums = summed(got_e1)
    floor_e = jnp.maximum(left(sums, 2 * width), 1.0)
    first_params, second_params = params.at[0], params.at[1]
    merge(got_e1, lambda p: count_e[p], floor_e, left(sums, width), first_params)

    @pl.when(has_next)
    def _():
        over(EARLY, lambda r: clip_tile(ext, r, r, first_params, msg_e2, r))

    @pl.when(x == 0)
    def _():
        over(
            EARLY,
            lambda r: clip_tile(out, r, EARLY + r, first_params, msg_e2, EARLY + r),
        )

    exchange_start(3, msg_e2, got_e2)
    group_tile(4)
    rest = range(4, len(around))

    @pl.when(x < blocks_t - 2)
    def _():
        pass1(rest)

    @pl.when(x == blocks_t - 2)
    def _():
        pass2(rest)

    second([0])
    group_tile(3)
    exchange_start(4, msg_g1, got_g1)
    second([1])
    exchange_all(3, got_e2).wait_recv()
    merge2(got_e2, floor_e, second_params)

    @pl.when(has_next)
    def _():
        telling.start()


    @pl.when(x == 0)
    def _():
        over(EARLY, lambda r: final_tile(r, EARLY + r, second_params))

    second([2,3])
    front = wt - EARLY
    exchange_all(4, got_g1).wait_recv()
    second([4])
    m2 = left(summed(got_g1), width)
    merge(got_g1, lambda p: count_h[p, :front, :], floor_h[:front, :], m2, row_g1)
    over(front, lambda i: clip_tile(out, wt - 1 - i, i, row_g1, msg_g2, i), front)
    exchange_start(5, msg_g2, got_g2)
    second([5])
    exchange_all(1, got_b2).wait_recv()
    merge2(got_b2, floor_b[...], row_b2)
    over(bulk, lambda i: final_tile(i + wt, i, row_b2), 2)


    @pl.when(has_prev)
    def _():
        telling.wait_recv()


    @pl.when(has_prev)
    def _():
        for r in range(EARLY - 1, -1, -1):
            finish(r, fore)
        for r in range(EARLY - 1, -1, -1):
            finish(r, rear)

    exchange_all(5, got_g2).wait_recv()
    merge2(got_g2, floor_h[:front, :], row_g2)
    over(front, lambda i: final_tile(wt - 1 - i, i, row_g2), front)

    for g, got in enumerate((got_b1, got_b2, got_e1, got_e2, got_g1, got_g2)):
        exchange_all(g, got).wait_send()

    @pl.when(has_prev)
    def _():
        extension.wait_send()

    @pl.when(has_next)
    def _():
        telling.wait_send()
        for k in range(len(around)):
            back(k).wait_send()
        for f, r in straight:
            direct(f, r).wait_send()

    @pl.when(hops1)
    def _():
        for k in range(len(around)):
            relay1(k).wait_send()

    @pl.when(hops2)
    def _():
        for k in range(len(around)):
            relay2(k).wait_send()


def per_device(blocks_t, peers, values, listed_from, listed_until):
    fields, rows, assets = values.shape
    tiles = rows // TILE
    wt = WINDOW // TILE
    bulk = tiles - wt
    f32 = jnp.float32
    vmem = pltpu.VMEM
    dma = pltpu.SemaphoreType.DMA
    around = EARLY * LATE
    groups = (bulk, bulk, 2 * EARLY, 2 * EARLY, wt - EARLY, wt - EARLY)
    scratch = [
        vmem((1, assets), jnp.int32),
        vmem((1, assets), jnp.int32),
        dma((2,)),
        pltpu.SemaphoreType.REGULAR((4,)),
        vmem((wt, TILE, LANES), f32),
        vmem((fields, WINDOW, assets), f32),
        vmem((around * TILE, assets), f32),
        vmem((around * TILE, assets), f32),
        vmem((fields, EARLY * TILE, assets), f32),
        vmem((2, 2 * EARLY, LANES), f32),
        vmem((2, 2 * EARLY, LANES), f32),
        vmem((fields, WINDOW, assets), f32),
        vmem((fields, TILE, assets), f32),
        vmem((fields, TILE, assets), f32),
        vmem((fields, TILE, assets), f32),
        vmem((fields, TILE, LANES), f32),
        vmem((fields, TILE, LANES), f32),
        *[vmem((n, LANES), f32) for n in groups],
        *[vmem((peers, n, LANES), f32) for n in groups],
        *[vmem((peers, n, LANES), f32) for n in (bulk, 2 * EARLY, wt)],
        *[vmem((n, LANES), f32) for n in (bulk, wt)],
        *[vmem((n, LANES), f32) for n in (bulk, bulk, wt - EARLY, wt - EARLY)],
        dma((fields, rows // WINDOW)),
        dma,
        dma,
        dma,
        dma,
        dma,
        dma,
        dma,
        dma,
        dma((fields, wt)),
        dma((around,)),
        dma((around,)),
        dma((6,)),
        dma((6,)),
    ]
    return pl.pallas_call(
        functools.partial(kernel, (blocks_t, peers)),
        out_shape=pltpu.VMEM(values.shape, values.dtype),
        in_specs=[
            pl.BlockSpec(memory_space=pltpu.HBM),
            pl.BlockSpec(memory_space=pltpu.HBM),
            pl.BlockSpec(memory_space=pltpu.HBM),
        ],
        out_specs=pl.BlockSpec(memory_space=pltpu.VMEM),
        scratch_shapes=scratch,
        compiler_params=pltpu.CompilerParams(
            collective_id=0,
            has_side_effects=True,
            vmem_limit_bytes=48 * 1024 * 1024,
        ),
    )(values, listed_from[None, :], listed_until[None, :])


def solution(mesh):
    in_specs = (P(None, "tm", "asset"), P("asset"), P("asset"))
    out_specs = P(None, "tm", "asset")
    body = functools.partial(per_device, mesh.shape["tm"], mesh.shape["asset"])
    return jax.shard_map(
        body, mesh=mesh, in_specs=in_specs, out_specs=out_specs, check_vma=False
    )
```

```python
import functools

import jax
import jax.numpy as jnp
from jax import lax
from jax.experimental import pallas as pl
from jax.experimental.pallas import tpu as pltpu
from jax.sharding import PartitionSpec as P

WINDOW = 64
EARLY = 3
BACK = ((3, 2), (3, 1), (2, 1), (3, 0), (2, 0))
EXTRA = 1
HALVES = 2
MARK = 4.0
TILE = 8
LANES = 128
CHUNK = 512
MESH = pl.DeviceIdType.MESH


def kernel(
    sizes,
    vals,
    opened_in,
    closed_in,
    out,
    opened,
    closed,
    list_sem,
    rounds,
    local_count,
    halo,
    hop1,
    hop2,
    ext,
    params,
    told,
    ring,
    total,
    base,
    suffix,
    ahead,
    pivot,
    msg_b1,
    msg_b2,
    msg_e1,
    msg_e2,
    msg_g1,
    msg_g2,
    got_b1,
    got_b2,
    got_e1,
    got_e2,
    got_g1,
    got_g2,
    count_b,
    count_e,
    count_h,
    floor_b,
    floor_h,
    row_b1,
    row_b2,
    row_g1,
    load_sem,
    direct_send,
    ext_send,
    ext_recv,
    told_send,
    told_recv,
    back_send,
    relay1_send,
    relay2_send,
    halo_recv,
    back_recv,
    hop1_recv,
    hop2_recv,
    ex_send,
    ex_recv,
):
    blocks_t, peers = sizes
    fields, rows, assets = vals.shape
    tiles = rows // TILE
    wt = WINDOW // TILE
    chunks = assets // CHUNK
    bulk = tiles - wt
    x = lax.axis_index("tm")
    me = lax.axis_index("asset")
    nxt = lax.rem(x + 1, blocks_t)
    prv = lax.rem(x + blocks_t - 1, blocks_t)
    t0 = x * rows

    dates = [
        pltpu.make_async_copy(opened_in, opened, list_sem.at[0]),
        pltpu.make_async_copy(closed_in, closed, list_sem.at[1]),
    ]
    for copy in dates:
        copy.start()

    def load(b):
        part = pl.ds(b * WINDOW, WINDOW)
        return pltpu.make_async_copy(
            vals.at[:, part, :], out.at[:, part, :], load_sem.at[b]
        )

    for b in range(rows // WINDOW):
        load(b).start()

    core = lax.rem(me, 2)
    chip = me // 2
    y, z = chip // 4, lax.rem(chip, 4)

    def at_place(dy, dz, dc):
        to = lax.rem(y + dy, 4) * 4 + lax.rem(z + dz, 4)
        return to * 2 + lax.rem(core + dc, 2)

    near = [at_place(0, 0, 1)]
    near += [at_place(1, 0, 0), at_place(3, 0, 0), at_place(0, 1, 0), at_place(0, 3, 0)]
    barrier = pltpu.get_barrier_semaphore()
    for t in (nxt, prv):
        pl.semaphore_signal(barrier, 1, device_id={"tm": t}, device_id_type=MESH)
    for peer in near:
        pl.semaphore_signal(barrier, 1, device_id={"asset": peer}, device_id_type=MESH)
    pl.semaphore_wait(barrier, 2 + len(near))

    def tell(i):
        for peer in near:
            pl.semaphore_signal(
                rounds.at[i], 1, device_id={"asset": peer}, device_id_type=MESH
            )

    def hear(i):
        pl.semaphore_wait(rounds.at[i], len(near))

    tell(0)

    tail = rows - WINDOW

    def tile_rows(r):
        return pl.ds(r * TILE, TILE)

    every = list(range(fields))
    kept, extra = every[: fields - EXTRA], every[fields - EXTRA :]
    tops = EARLY + (1 if EXTRA else 0)
    piece = assets // HALVES
    tiles_back = sorted({r for _, r in BACK}, reverse=True)
    around = [
        (f, r, h) for t in tiles_back for h in range(HALVES) for f, r in BACK if r == t
    ]

    def early(r):
        return every if r < EARLY else extra

    def grouped(r):
        return every if r > EARLY else kept

    def half(h):
        return pl.ds(h * piece, piece)

    straight = []
    for r in range(wt - 1, -1, -1):
        left_over = [f for f in every if (f, r) not in BACK]
        if r == EARLY:
            cuts = [kept[:-1], kept[-1:], extra]
        else:
            cuts = [left_over]
        straight.extend((r, cut) for cut in cuts if cut)

    def direct(i):
        r, cut = straight[i]
        which = pl.ds(cut[0], len(cut))
        return pltpu.make_async_remote_copy(
            src_ref=vals.at[which, pl.ds(tail + r * TILE, TILE), :],
            dst_ref=halo.at[which, tile_rows(r), :],
            send_sem=direct_send,
            recv_sem=halo_recv.at[i],
            device_id={"tm": nxt},
            device_id_type=MESH,
        )

    def back(k):
        f, r, h = around[k]
        return pltpu.make_async_remote_copy(
            src_ref=vals.at[f, pl.ds(tail + r * TILE, TILE), half(h)],
            dst_ref=hop1.at[tile_rows(k), :],
            send_sem=back_send,
            recv_sem=hop1_recv.at[k],
            device_id={"tm": prv},
            device_id_type=MESH,
        )

    def relay1(k):
        return pltpu.make_async_remote_copy(
            src_ref=hop1.at[tile_rows(k), :],
            dst_ref=hop2.at[tile_rows(k), :],
            send_sem=relay1_send,
            recv_sem=hop2_recv.at[k],
            device_id={"tm": prv},
            device_id_type=MESH,
        )

    def relay2(k):
        f, r, h = around[k]
        return pltpu.make_async_remote_copy(
            src_ref=hop2.at[tile_rows(k), :],
            dst_ref=halo.at[f, tile_rows(r), half(h)],
            send_sem=relay2_send,
            recv_sem=back_recv.at[k],
            device_id={"tm": prv},
            device_id_type=MESH,
        )

    def pass1(ks):
        for k in ks:
            back(k).wait_recv()
            relay1(k).start()

    def pass2(ks):
        for k in ks:
            relay1(k).wait_recv()
            relay2(k).start()

    def extension(i):
        which = (pl.ds(0, fields), pl.ds(fields - EXTRA, EXTRA))[i]
        part = (pl.ds(0, EARLY * TILE), pl.ds(EARLY * TILE, TILE))[i]
        return pltpu.make_async_remote_copy(
            src_ref=vals.at[which, part, :],
            dst_ref=ext.at[which, part, :],
            send_sem=ext_send.at[i],
            recv_sem=ext_recv.at[i],
            device_id={"tm": prv},
            device_id_type=MESH,
        )

    extensions = [extension(i) for i in range(2 if EXTRA else 1)]
    telling = pltpu.make_async_remote_copy(
        src_ref=params,
        dst_ref=told,
        send_sem=told_send,
        recv_sem=told_recv,
        device_id={"tm": nxt},
        device_id_type=MESH,
    )

    has_prev = x > 0
    has_next = x < blocks_t - 1
    last = x == blocks_t - 1
    hops1 = x != blocks_t - 2
    hops2 = x != blocks_t - 3
    @pl.when(has_prev)
    def _():
        for copy in extensions:
            copy.start()

    @pl.when(has_next)
    def _():
        for k in range(len(around)):
            back(k).start()
        for i in range(len(straight) - 1):
            direct(i).start()

    def hops(d):
        return min(d[0], 4 - d[0]) + min(d[1], 4 - d[1]) + d[2] / 2

    places = [(dy, dz, dc) for dy in range(4) for dz in range(4) for dc in range(2)]
    places = sorted(places[1:], key=hops, reverse=True)

    def exchange(g, msg, got, k, peer):
        return pltpu.make_async_remote_copy(
            src_ref=msg,
            dst_ref=got.at[k],
            send_sem=ex_send.at[g],
            recv_sem=ex_recv.at[g],
            device_id={"asset": peer},
            device_id_type=MESH,
        )

    def exchange_start(g, msg, got):
        for d in places:
            k = (d[0] * 4 + d[1]) * 2 + d[2]
            exchange(g, msg, got, k, at_place(*d)).start()
        got[0] = msg[...]

    def exchange_all(g, got):
        others = got.at[pl.ds(1, peers - 1)]
        return pltpu.make_async_remote_copy(
            src_ref=others,
            dst_ref=others,
            send_sem=ex_send.at[g],
            recv_sem=ex_recv.at[g],
            device_id={"asset": me},
            device_id_type=MESH,
        )

    sub = lax.broadcasted_iota(jnp.int32, (TILE, LANES), 0)
    lane = lax.broadcasted_iota(jnp.int32, (TILE, LANES), 1)
    subc = lax.broadcasted_iota(jnp.int32, (TILE, CHUNK), 0)
    width = fields * TILE

    def lanes(c):
        return pl.ds(c * CHUNK, CHUNK)

    def fold(v):
        acc = v[:, :LANES]
        for i in range(1, CHUNK // LANES):
            acc = acc + v[:, i * LANES : (i + 1) * LANES]
        return acc

    def across(v):
        return jnp.sum(v, axis=1, keepdims=True)

    def flat(columns):
        z = jnp.zeros((TILE, LANES), jnp.float32)
        for at, column in columns:
            z = jnp.where(lane == sub + at, column, z)
        return jnp.sum(z, axis=0, keepdims=True)

    def column(row, at):
        return across(jnp.where(lane == sub + at, row, 0.0))

    def listed(c, first):
        t = subc + first
        o = opened[:, lanes(c)]
        u = closed[:, lanes(c)]
        return t, o, u, (t >= o) & (t < u)

    def share(t, o, u, w):
        low = jnp.maximum(jnp.maximum(t - (WINDOW - 1), o), 0)
        high = jnp.minimum(t, u - 1)
        counted = jnp.maximum(high - low + 1, 1).astype(jnp.float32)
        return jnp.where(w, 1.0 / counted, 0.0)

    def moments(count, s, q, pivots, which):
        inverse = 1.0 / jnp.maximum(count, 1.0)
        columns = []
        means = []
        for f, s_l, q_l, pivot_f in zip(which, s, q, pivots):
            s_f, q_f = across(s_l), across(q_l)
            lift = s_f * inverse
            mean = pivot_f + lift
            means.append(mean)
            columns.append((f * TILE, mean))
            columns.append((width + f * TILE, jnp.maximum(q_f - s_f * lift, 0.0)))
        return means, columns

    def counts_at(count, at):
        return [(at + f * TILE, count) for f in range(fields)]

    zero = jnp.zeros((TILE, LANES), jnp.float32)

    for copy in dates:
        copy.wait()
    msg_b1[...] = jnp.zeros_like(msg_b1)
    base[...] = jnp.zeros_like(base)
    load(0).wait()

    def prefix(f, c, w, v):
        p = jnp.where(w, v, 0.0)
        for k in (1, 2, 4):
            p = p + jnp.where(subc >= k, pltpu.roll(p, k, 0), 0.0)
        p = p + base[f, :, lanes(c)]
        base[f, :, lanes(c)] = jnp.broadcast_to(p[TILE - 1 :, :], p.shape)
        return p

    def first_tile(r, carry):
        n = zero
        here = pl.ds(pl.multiple_of(r * TILE, TILE), TILE)
        for c in range(chunks):
            _, _, _, w = listed(c, t0 + r * TILE)
            n = n + fold(jnp.where(w, 1.0, 0.0))
            for f in range(fields):
                p = prefix(f, c, w, out[f, here, lanes(c)])
                ring[f, here, lanes(c)] = p
                out[f, here, lanes(c)] = p
        count = across(n)
        local_count[r] = jnp.broadcast_to(count, zero.shape)
        msg_b1[pl.ds(wt - 1 - r, 1), :] = flat(counts_at(count, 3 * width))
        return carry

    lax.fori_loop(0, wt, first_tile, 0)

    for f in range(fields):
        rough = zero
        for c in range(chunks):
            rough = rough + fold(base[f, :, lanes(c)])
        pivot[f] = jnp.broadcast_to(across(rough) * (1.0 / (WINDOW * assets)), zero.shape)

    def window_tile(ref, here, first, i, pivots, which):
        slot = pl.ds(pl.multiple_of(i * TILE, TILE), TILE)
        n = zero
        s = [zero] * fields
        q = [zero] * fields
        for c in range(chunks):
            t, o, u, w = listed(c, first)
            n = n + fold(jnp.where(w, 1.0, 0.0))
            part = share(t, o, u, w)
            for f in which:
                p = prefix(f, c, w, ref[f, here, lanes(c)])
                old = ring[f, slot, lanes(c)]
                ring[f, slot, lanes(c)] = p
                rolled = (p + (total[f, :, lanes(c)] - old)) * part
                ref[f, here, lanes(c)] = rolled
                d = jnp.where(w, rolled - pivots[f], 0.0)
                s[f] = s[f] + fold(d)
                q[f] = q[f] + fold(d * d)
        count = across(n)
        means, columns = moments(
            count, [s[f] for f in which], [q[f] for f in which], [pivots[f] for f in which], which)
        return means, flat(columns + counts_at(count, 2 * width))

    def bulk_tile(b, i, pivots):
        r = b * wt + i
        here = pl.ds(pl.multiple_of(r * TILE, TILE), TILE)
        means, line = window_tile(out, here, t0 + r * TILE, i, pivots, every)
        at = pl.ds(r - wt, 1)
        msg_b1[at, :] = msg_b1[at, :] + line
        return means

    def bulk_block(b):
        total[...] = base[...]
        base[...] = jnp.zeros_like(base)

        def pair(i, carry):
            pivots = [pivot[f][:, :1] for f in range(fields)]
            lower = bulk_tile(b, 2 * i, pivots)
            upper = bulk_tile(b, 2 * i + 1, pivots)
            for f in range(fields):
                pivot[f] = jnp.broadcast_to(upper[f], zero.shape)
            if b == 1:

                @pl.when(i == 0)
                def _():
                    for f in range(fields):
                        ahead[f] = jnp.broadcast_to(lower[f], zero.shape)

            return carry

        lax.fori_loop(0, wt // 2, pair, 0)

    for b in range(1, rows // WINDOW):
        hear(b - 1)
        tell(b)
        load(b).wait()
        bulk_block(b)
    hear(rows // WINDOW - 1)
    exchange_start(0, msg_b1, got_b1)


    @pl.when(last)
    def _():
        pass1(range(len(around)))

    def scaled(center, spread):
        inv = 1.0 / jnp.sqrt(jnp.maximum(spread, 0.0) + 0.1)
        wide = lax.broadcasted_iota(jnp.int32, center.shape, 1)
        return jnp.where(wide % (2 * width) < width, center, pltpu.roll(inv, width, 1))

    def left(v, by):
        return pltpu.roll(v, LANES - by, 1)

    def sum_over(term, shape):
        step = 8
        nothing = tuple(jnp.zeros(shape, jnp.float32) for _ in range(2))

        def some(i, acc):
            acc = list(acc)
            for j in range(step):
                acc[j % 2] = acc[j % 2] + term(i * step + j)
            return tuple(acc)

        if shape[0] <= TILE:
            acc = nothing
            for i in range(peers // step):
                acc = some(i, acc)
        else:
            acc = lax.fori_loop(0, peers // step, some, nothing)
        return acc[0] + acc[1]

    def merge(got, counts, floor, m2, rows_out):
        shape = rows_out.shape
        center = sum_over(lambda p: counts(p) * got[p], shape) / floor

        def spread_term(p):
            d = got[p] - center
            return counts(p) * d * d

        rows_out[...] = scaled(center, (sum_over(spread_term, shape) + m2) / floor)

    def summed(got):
        return sum_over(lambda p: got[p], got.shape[1:])

    def columns_of(row_in, row, which, at=0):
        line = jnp.broadcast_to(row_in[pl.ds(row, 1), :], zero.shape)
        center = {f: column(line, at + f * TILE) for f in which}
        inv = {f: column(line, at + width + f * TILE) for f in which}
        return center, inv

    def clipped_sums(ref, r, row, row_in, which, mark=0.0, at=0):
        here = pl.ds(pl.multiple_of(r * TILE, TILE), TILE)
        first = t0 + r * TILE if ref is out else t0 + rows + r * TILE
        center, inv = columns_of(row_in, row, which)
        s = {f: zero for f in which}
        q = {f: zero for f in which}
        for c in range(chunks):
            _, _, _, w = listed(c, first)
            for f in which:
                y = (ref[f, here, lanes(c)] - center[f]) * inv[f]
                y = jnp.clip(y, -3.0, 3.0)
                if ref is out:
                    ref[f, here, lanes(c)] = jnp.where(w, y, mark)
                y = jnp.where(w, y, 0.0)
                s[f] = s[f] + fold(y)
                q[f] = q[f] + fold(y * y)
        columns = []
        for f in which:
            columns.append((at + f * TILE, across(s[f])))
            columns.append((at + width + f * TILE, across(q[f])))
        return columns

    def clip_tile(ref, r, row, row_in, msg, msg_row, which, mark=0.0):
        columns = clipped_sums(ref, r, row, row_in, which, mark)
        msg[pl.ds(msg_row, 1), :] = flat(columns)

    def merge2(got, floor, rows_out):
        sums = summed(got)
        center = sums / floor
        spread = left(sums, width) / floor - center * center
        rows_out[...] = scaled(center, spread)

    def final_tile(r, row, row_in, which, at=0):
        here = pl.ds(pl.multiple_of(r * TILE, TILE), TILE)
        center, inv = columns_of(row_in, row, which, at)
        for c in range(chunks):
            _, _, _, w = listed(c, t0 + r * TILE)
            for f in which:
                y = (out[f, here, lanes(c)] - center[f]) * inv[f]
                out[f, here, lanes(c)] = jnp.where(w, y, 0.0)

    def over(n, step, unroll=1):
        def one(i, carry):
            step(i)
            return carry

        lax.fori_loop(0, n, one, 0, unroll=unroll)

    def arrival(f, r, h):
        if (f, r, h) in around:
            relay2(around.index((f, r, h))).wait_recv()
        elif h == 0:
            for i, (tile, cut) in enumerate(straight):
                if tile == r and cut[0] == f:
                    direct(i).wait_recv()

    def joined(f, c, here, past):
        h = jnp.where(past, halo[f, here, lanes(c)], 0.0)
        for j in (1, 2, 4):
            up = pltpu.roll(h, TILE - j, 0)
            h = h + jnp.where(subc < TILE - j, up, 0.0)
        before = suffix[f, :, lanes(c)]
        after = jnp.where(subc < TILE - 1, pltpu.roll(h, TILE - 1, 0), 0.0)
        suffix[f, :, lanes(c)] = before + jnp.broadcast_to(h[:1, :], h.shape)
        return out[f, here, lanes(c)] + (before + after)

    def before_mask(c, t, r):
        _, _, _, past = listed(c, t0 + r * TILE - WINDOW)
        return past & (t >= WINDOW)

    def halo_part(r, msg, row, counted_too, which):
        here = tile_rows(r)
        s = {f: zero for f in which}
        q = {f: zero for f in which}
        pivots = {f: ahead[f][:, :1] for f in which}
        for c in range(chunks):
            t, o, u, w = listed(c, t0 + r * TILE)
            past = before_mask(c, t, r)
            part = share(t, o, u, w)
            for f in which:
                rolled = joined(f, c, here, past) * part
                out[f, here, lanes(c)] = rolled
                d = jnp.where(w, rolled - pivots[f], 0.0)
                s[f] = s[f] + fold(d)
                q[f] = q[f] + fold(d * d)
        count = local_count[r][:, :1]
        means, columns = moments(
            count,
            [s[f] for f in which],
            [q[f] for f in which],
            [pivots[f] for f in which],
            which,
        )
        for f, mean in zip(which, means):
            ahead[f] = jnp.broadcast_to(mean, zero.shape)
        if counted_too:
            columns = columns + counts_at(count, 2 * width)
        at = pl.ds(row, 1)
        msg[at, :] = msg[at, :] + flat(columns)

    def group_tile(r, which):
        @pl.when(has_prev)
        def _():
            for f in which:
                arrival(f, r, 0)

        halo_part(r, msg_g1, wt - 1 - r, False, which)

    def finish(r, which):
        here = tile_rows(r)
        first = columns_of(told.at[0], r, which)
        then = columns_of(told.at[1], r, which)
        per = chunks // HALVES
        for h in range(HALVES):
            for f in which:
                arrival(f, r, h)
            for c in range(h * per, (h + 1) * per):
                t, o, u, w = listed(c, t0 + r * TILE)
                past = before_mask(c, t, r)
                part = share(t, o, u, w)
                for f in which:
                    y = joined(f, c, here, past) * part
                    y = jnp.clip((y - first[0][f]) * first[1][f], -3.0, 3.0)
                    y = (y - then[0][f]) * then[1][f]
                    out[f, here, lanes(c)] = jnp.where(w, y, 0.0)

    suffix[...] = jnp.zeros_like(suffix)
    msg_e1[...] = jnp.zeros_like(msg_e1)
    msg_g1[...] = jnp.zeros_like(msg_g1)
    msg_e2[...] = jnp.zeros_like(msg_e2)


    def second(ks):
        @pl.when((x == 0) | last)
        def _():
            pass2(ks)

    group_tile(7, every)
    group_tile(6, every)

    @pl.when(x == 0)
    def _():
        for r in range(tops - 1, -1, -1):
            halo_part(r, msg_e1, tops + r, True, early(r))

    exchange_all(0, got_b1).wait_recv()

    def split(p):
        v = got_b1[p]
        count_b[p] = left(v, 2 * width)
        count_h[p] = left(v[:wt, :], 3 * width)

    over(peers, split, 8)
    sums = summed(got_b1)
    floor_b[...] = jnp.maximum(left(sums, 2 * width), 1.0)
    floor_h[...] = jnp.maximum(left(sums[:wt, :], 3 * width), 1.0)
    merge(got_b1, lambda p: count_b[p], floor_b[...], left(sums, width), row_b1)
    group_tile(5, every)

    @pl.when(has_next)
    def _():
        total[...] = base[...]
        base[...] = jnp.zeros_like(base)
        for copy in extensions:
            copy.wait_recv()

        def one(r, which):
            here = pl.ds(pl.multiple_of(r * TILE, TILE), TILE)
            pivots = [pivot[f][:, :1] for f in every]
            means, line = window_tile(ext, here, t0 + rows + r * TILE, r, pivots, which)
            for f, mean in zip(which, means):
                pivot[f] = jnp.broadcast_to(mean, zero.shape)
            msg_e1[pl.ds(r, 1), :] = line

        over(EARLY, lambda r: one(r, every))
        if EXTRA:
            one(EARLY, extra)

    exchange_start(2, msg_e1, got_e1)
    pairs = bulk // 2

    def clip_pair(j):
        columns = clipped_sums(out, j + wt, j, row_b1, every)
        i = j + pairs
        columns += clipped_sums(out, i + wt, i, row_b1, every, at=2 * width)
        msg_b2[pl.ds(j, 1), :] = flat(columns)

    over(pairs, clip_pair)
    exchange_start(1, msg_b2, got_b2)
    some = range(6)

    @pl.when(x < blocks_t - 2)
    def _():
        pass1(some)

    @pl.when(x == blocks_t - 2)
    def _():
        pass2(some)

    group_tile(4, every)
    exchange_all(2, got_e1).wait_recv()

    def split_e(p):
        count_e[p] = left(got_e1[p], 2 * width)

    over(peers, split_e, peers)
    sums = summed(got_e1)
    floor_e = jnp.maximum(left(sums, 2 * width), 1.0)
    first_params, second_params = params.at[0], params.at[1]
    merge(got_e1, lambda p: count_e[p], floor_e, left(sums, width), first_params)

    @pl.when(has_next)
    def _():
        over(EARLY, lambda r: clip_tile(ext, r, r, first_params, msg_e2, r, every))
        for r in range(EARLY, tops):
            clip_tile(ext, r, r, first_params, msg_e2, r, extra)

    @pl.when(x == 0)
    def _():
        for r in range(tops):
            clip_tile(out, r, tops + r, first_params, msg_e2, tops + r, early(r))

    exchange_start(3, msg_e2, got_e2)
    rest = range(6, len(around))

    @pl.when(x < blocks_t - 2)
    def _():
        pass1(rest)

    @pl.when(x == blocks_t - 2)
    def _():
        pass2(rest)

    group_tile(3, kept[:-1])
    group_tile(3, kept[-1:])
    exchange_start(4, msg_g1, got_g1)
    second([0,1])
    second([2,3])
    exchange_all(3, got_e2).wait_recv()
    merge2(got_e2, floor_e, second_params)

    @pl.when(has_next)
    def _():
        telling.start()
        direct(len(straight) - 1).start()


    @pl.when(x == 0)
    def _():
        for r in range(tops):
            final_tile(r, tops + r, second_params, early(r))

    second([4,5])
    front = wt - EARLY
    exchange_all(4, got_g1).wait_recv()
    second([6,7])
    m2 = left(summed(got_g1), width)
    merge(got_g1, lambda p: count_h[p, :front, :], floor_h[:front, :], m2, row_g1)
    for r in range(wt - 1, EARLY - 1, -1):
        i = wt - 1 - r
        clip_tile(out, r, i, row_g1, msg_g2, i, grouped(r), MARK)
    exchange_start(5, msg_g2, got_g2)
    second([8,9])
    exchange_all(1, got_b2).wait_recv()
    low, high = floor_b[pl.ds(0, pairs), :], floor_b[pl.ds(pairs, pairs), :]
    wide = lax.broadcasted_iota(jnp.int32, low.shape, 1)
    both = jnp.where(wide < 2 * width, low, pltpu.roll(high, 2 * width, 1))
    merge2(got_b2, both, row_b2)

    def final_pair(j):
        final_tile(j + wt, j, row_b2, every)
        final_tile(j + pairs + wt, j, row_b2, every, 2 * width)

    over(pairs, final_pair)


    @pl.when(has_prev)
    def _():
        telling.wait_recv()


    @pl.when(has_prev)
    def _():
        for r in range(EARLY, tops):
            finish(r, extra)
        for r in range(EARLY - 1, -1, -1):
            finish(r, [f for f in every if (f, r) not in BACK])
            finish(r, [f for f in every if (f, r) in BACK])

    exchange_all(5, got_g2).wait_recv()
    merge2(got_g2, floor_h[:front, :], out.at[0, pl.ds(rows, front), pl.ds(0, LANES)])
    for g, got in enumerate((got_b1, got_b2, got_e1, got_e2, got_g1, got_g2)):
        exchange_all(g, got).wait_send()

    @pl.when(has_prev)
    def _():
        for copy in extensions:
            copy.wait_send()

    @pl.when(has_next)
    def _():
        telling.wait_send()
        for k in range(len(around)):
            back(k).wait_send()
        for i in range(len(straight)):
            direct(i).wait_send()

    @pl.when(hops1)
    def _():
        for k in range(len(around)):
            relay1(k).wait_send()

    @pl.when(hops2)
    def _():
        for k in range(len(around)):
            relay2(k).wait_send()


def writer(x_ref, o_ref, tile_ref, sem, sem_tile):
    fields, rows, assets = o_ref.shape
    wt = WINDOW // TILE
    step = (rows - WINDOW) // 2
    spans = []
    for f in range(fields):
        tops = EARLY + (1 if f >= fields - EXTRA else 0)
        spans.append((f, 0, tops * TILE))
        spans.extend((f, WINDOW + i * step, step) for i in range(2))
    copies = [
        pltpu.make_async_copy(
            x_ref.at[f, pl.ds(at, size), :], o_ref.at[f, pl.ds(at, size), :], sem.at[i]
        )
        for i, (f, at, size) in enumerate(spans)
    ]
    for copy in copies:
        copy.start()
    sub = lax.broadcasted_iota(jnp.int32, (TILE, LANES), 0)
    lane = lax.broadcasted_iota(jnp.int32, (TILE, LANES), 1)
    width = fields * TILE
    for i in range(wt - EARLY):
        r = wt - 1 - i
        many = fields if r > EARLY else fields - EXTRA
        here, there = pl.ds(r * TILE, TILE), pl.ds(i * TILE, TILE)
        line = jnp.broadcast_to(x_ref[0, pl.ds(rows + i, 1), :LANES], (TILE, LANES))

        def column(at):
            kept = jnp.where(lane == sub + at, line, 0.0)
            return jnp.sum(kept, axis=1, keepdims=True)

        for f in range(many):
            center, inv = column(f * TILE), column(width + f * TILE)
            for c in range(assets // CHUNK):
                part = pl.ds(c * CHUNK, CHUNK)
                y = x_ref[f, here, part]
                z = jnp.where(y > 3.5, 0.0, (y - center) * inv)
                tile_ref[f, there, part] = z
        copy = pltpu.make_async_copy(
            tile_ref.at[pl.ds(0, many), there, :],
            o_ref.at[pl.ds(0, many), here, :],
            sem_tile.at[i],
        )
        copy.start()
        copies.append(copy)
    for copy in copies:
        copy.wait()


def per_device(blocks_t, peers, values, listed_from, listed_until):
    fields, rows, assets = values.shape
    tiles = rows // TILE
    wt = WINDOW // TILE
    bulk = tiles - wt
    f32 = jnp.float32
    vmem = pltpu.VMEM
    dma = pltpu.SemaphoreType.DMA
    around = len(BACK) * HALVES
    tops = EARLY + (1 if EXTRA else 0)
    groups = (bulk, bulk // 2, 2 * tops, 2 * tops, wt - EARLY, wt - EARLY)
    scratch = [
        vmem((1, assets), jnp.int32),
        vmem((1, assets), jnp.int32),
        dma((2,)),
        pltpu.SemaphoreType.REGULAR((4,)),
        vmem((wt, TILE, LANES), f32),
        vmem((fields, WINDOW, assets), f32),
        vmem((around * TILE, assets // HALVES), f32),
        vmem((around * TILE, assets // HALVES), f32),
        vmem((fields, tops * TILE, assets), f32),
        vmem((2, 2 * tops, LANES), f32),
        vmem((2, 2 * tops, LANES), f32),
        vmem((fields, WINDOW, assets), f32),
        vmem((fields, TILE, assets), f32),
        vmem((fields, TILE, assets), f32),
        vmem((fields, TILE, assets), f32),
        vmem((fields, TILE, LANES), f32),
        vmem((fields, TILE, LANES), f32),
        *[vmem((n, LANES), f32) for n in groups],
        *[vmem((peers, n, LANES), f32) for n in groups],
        *[vmem((peers, n, LANES), f32) for n in (bulk, 2 * tops, wt)],
        *[vmem((n, LANES), f32) for n in (bulk, wt)],
        *[vmem((n, LANES), f32) for n in (bulk, bulk // 2, wt - EARLY)],
        dma((rows // WINDOW,)),
        dma,
        dma((2,)),
        dma((2,)),
        dma,
        dma,
        dma,
        dma,
        dma,
        dma((wt + 2,)),
        dma((around,)),
        dma((around,)),
        dma((around,)),
        dma((6,)),
        dma((6,)),
    ]
    clipped = pl.pallas_call(
        functools.partial(kernel, (blocks_t, peers)),
        out_shape=pltpu.VMEM((fields, rows + TILE, assets), values.dtype),
        in_specs=[
            pl.BlockSpec(memory_space=pltpu.HBM),
            pl.BlockSpec(memory_space=pltpu.HBM),
            pl.BlockSpec(memory_space=pltpu.HBM),
        ],
        out_specs=pl.BlockSpec(memory_space=pltpu.VMEM),
        scratch_shapes=scratch,
        compiler_params=pltpu.CompilerParams(
            collective_id=0,
            has_side_effects=True,
            vmem_limit_bytes=48 * 1024 * 1024,
        ),
    )(values, listed_from[None, :], listed_until[None, :])
    return pl.pallas_call(
        writer,
        out_shape=jax.ShapeDtypeStruct(values.shape, values.dtype),
        in_specs=[pl.BlockSpec(memory_space=pltpu.VMEM)],
        out_specs=pl.BlockSpec(memory_space=pltpu.HBM),
        scratch_shapes=[
            vmem((fields, WINDOW - EARLY * TILE, assets), f32),
            dma((3 * fields,)),
            dma((wt - EARLY,)),
        ],
        compiler_params=pltpu.CompilerParams(vmem_limit_bytes=8 * 1024 * 1024),
    )(pltpu.with_memory_space_constraint(clipped, pltpu.VMEM))


def solution(mesh):
    in_specs = (P(None, "tm", "asset"), P("asset"), P("asset"))
    out_specs = P(None, "tm", "asset")
    body = functools.partial(per_device, mesh.shape["tm"], mesh.shape["asset"])
    return jax.shard_map(
        body, mesh=mesh, in_specs=in_specs, out_specs=out_specs, check_vma=False
    )
```

```python
import functools

import jax
import jax.numpy as jnp
from jax import lax
from jax.experimental import pallas as pl
from jax.experimental.pallas import tpu as pltpu
from jax.sharding import PartitionSpec as P

WINDOW = 64
EARLY = 3
BACK = ((3, 2), (3, 1), (2, 1), (3, 0), (2, 0))
EXTRA = 1
HALVES = 2
MARK = 4.0
DEEP = 3
TILE = 8
LANES = 128
CHUNK = 512
MESH = pl.DeviceIdType.MESH


def kernel(
    sizes,
    vals,
    opened_in,
    closed_in,
    out,
    opened,
    closed,
    list_sem,
    rounds,
    local_count,
    halo,
    hop1,
    hop2,
    ext,
    params,
    told,
    ring,
    total,
    base,
    suffix,
    ahead,
    pivot,
    msg_b1,
    msg_b2,
    msg_e1,
    msg_e2,
    msg_g1,
    msg_g2,
    got_b1,
    got_b2,
    got_e1,
    got_e2,
    got_g1,
    got_g2,
    count_b,
    count_e,
    count_h,
    floor_b,
    floor_h,
    row_b1,
    row_b2,
    row_g1,
    load_sem,
    direct_send,
    ext_send,
    ext_recv,
    told_send,
    told_recv,
    back_send,
    relay1_send,
    relay2_send,
    halo_recv,
    back_recv,
    hop1_recv,
    hop2_recv,
    ex_send,
    ex_recv,
):
    blocks_t, peers = sizes
    fields, rows, assets = vals.shape
    tiles = rows // TILE
    wt = WINDOW // TILE
    chunks = assets // CHUNK
    bulk = tiles - wt
    x = lax.axis_index("tm")
    me = lax.axis_index("asset")
    nxt = lax.rem(x + 1, blocks_t)
    prv = lax.rem(x + blocks_t - 1, blocks_t)
    t0 = x * rows

    dates = [
        pltpu.make_async_copy(opened_in, opened, list_sem.at[0]),
        pltpu.make_async_copy(closed_in, closed, list_sem.at[1]),
    ]
    for copy in dates:
        copy.start()

    def load(b):
        part = pl.ds(b * WINDOW, WINDOW)
        return pltpu.make_async_copy(
            vals.at[:, part, :], out.at[:, part, :], load_sem.at[b]
        )

    for b in range(rows // WINDOW):
        load(b).start()

    core = lax.rem(me, 2)
    chip = me // 2
    y, z = chip // 4, lax.rem(chip, 4)

    def at_place(dy, dz, dc):
        to = lax.rem(y + dy, 4) * 4 + lax.rem(z + dz, 4)
        return to * 2 + lax.rem(core + dc, 2)

    near = [at_place(0, 0, 1)]
    near += [at_place(1, 0, 0), at_place(3, 0, 0), at_place(0, 1, 0), at_place(0, 3, 0)]
    barrier = pltpu.get_barrier_semaphore()
    for t in (nxt, prv):
        pl.semaphore_signal(barrier, 1, device_id={"tm": t}, device_id_type=MESH)
    for peer in near:
        pl.semaphore_signal(barrier, 1, device_id={"asset": peer}, device_id_type=MESH)
    pl.semaphore_wait(barrier, 2 + len(near))

    def tell(i):
        for peer in near:
            pl.semaphore_signal(
                rounds.at[i], 1, device_id={"asset": peer}, device_id_type=MESH
            )

    def hear(i):
        pl.semaphore_wait(rounds.at[i], len(near))

    tell(0)

    tail = rows - WINDOW

    def tile_rows(r):
        return pl.ds(r * TILE, TILE)

    def needed(at, r):
        skip = 1 if r == 0 else 0
        return pl.ds(at + skip, TILE - skip)


    every = list(range(fields))
    kept, extra = every[: fields - EXTRA], every[fields - EXTRA :]
    tops = EARLY + (1 if EXTRA else 0)
    piece = assets // HALVES
    tiles_back = sorted({r for _, r in BACK}, reverse=True)
    around = [
        (f, r, h) for t in tiles_back for h in range(HALVES) for f, r in BACK if r == t
    ]

    def early(r):
        return every if r < EARLY else extra

    def grouped(r):
        return every if r > EARLY else kept

    def half(h):
        return pl.ds(h * piece, piece)

    straight = []
    for r in range(wt - 1, -1, -1):
        left_over = [f for f in every if (f, r) not in BACK]
        if r == EARLY:
            cuts = [kept[:-1], kept[-1:], extra]
        else:
            cuts = [left_over]
        straight.extend((r, cut) for cut in cuts if cut)

    def direct(i):
        r, cut = straight[i]
        which = pl.ds(cut[0], len(cut))
        return pltpu.make_async_remote_copy(
            src_ref=vals.at[which, needed(tail + r * TILE, r), :],
            dst_ref=halo.at[which, needed(r * TILE, r), :],
            send_sem=direct_send,
            recv_sem=halo_recv.at[i],
            device_id={"tm": nxt},
            device_id_type=MESH,
        )

    def back(k):
        f, r, h = around[k]
        return pltpu.make_async_remote_copy(
            src_ref=vals.at[f, needed(tail + r * TILE, r), half(h)],
            dst_ref=hop1.at[needed(k * TILE, r), :],
            send_sem=back_send,
            recv_sem=hop1_recv.at[k],
            device_id={"tm": prv},
            device_id_type=MESH,
        )

    def relay1(k):
        part = needed(k * TILE, around[k][1])
        return pltpu.make_async_remote_copy(
            src_ref=hop1.at[part, :],
            dst_ref=hop2.at[part, :],
            send_sem=relay1_send,
            recv_sem=hop2_recv.at[k],
            device_id={"tm": prv},
            device_id_type=MESH,
        )

    def relay2(k):
        f, r, h = around[k]
        return pltpu.make_async_remote_copy(
            src_ref=hop2.at[needed(k * TILE, r), :],
            dst_ref=halo.at[f, needed(r * TILE, r), half(h)],
            send_sem=relay2_send,
            recv_sem=back_recv.at[k],
            device_id={"tm": prv},
            device_id_type=MESH,
        )

    def pass1(ks):
        for k in ks:
            back(k).wait_recv()
            relay1(k).start()

    def pass2(ks):
        for k in ks:
            relay1(k).wait_recv()
            relay2(k).start()

    def extension(i):
        which = (pl.ds(0, fields), pl.ds(fields - EXTRA, EXTRA))[i]
        part = (pl.ds(0, EARLY * TILE), pl.ds(EARLY * TILE, TILE))[i]
        return pltpu.make_async_remote_copy(
            src_ref=vals.at[which, part, :],
            dst_ref=ext.at[which, part, :],
            send_sem=ext_send.at[i],
            recv_sem=ext_recv.at[i],
            device_id={"tm": prv},
            device_id_type=MESH,
        )

    extensions = [extension(i) for i in range(2 if EXTRA else 1)]
    telling = pltpu.make_async_remote_copy(
        src_ref=params,
        dst_ref=told,
        send_sem=told_send,
        recv_sem=told_recv,
        device_id={"tm": nxt},
        device_id_type=MESH,
    )

    has_prev = x > 0
    has_next = x < blocks_t - 1
    last = x == blocks_t - 1
    hops1 = x != blocks_t - 2
    hops2 = x != blocks_t - 3
    @pl.when(has_prev)
    def _():
        for copy in extensions:
            copy.start()

    @pl.when(has_next)
    def _():
        for k in range(len(around)):
            back(k).start()
        for i in range(len(straight) - 1):
            direct(i).start()

    def hops(d):
        return min(d[0], 4 - d[0]) + min(d[1], 4 - d[1]) + d[2] / 2

    places = [(dy, dz, dc) for dy in range(4) for dz in range(4) for dc in range(2)]
    places = sorted(places[1:], key=hops, reverse=True)

    def exchange(g, msg, got, k, peer):
        return pltpu.make_async_remote_copy(
            src_ref=msg,
            dst_ref=got.at[k],
            send_sem=ex_send.at[g],
            recv_sem=ex_recv.at[g],
            device_id={"asset": peer},
            device_id_type=MESH,
        )

    def exchange_start(g, msg, got):
        for d in places:
            k = (d[0] * 4 + d[1]) * 2 + d[2]
            exchange(g, msg, got, k, at_place(*d)).start()
        got[0] = msg[...]

    def exchange_all(g, got):
        others = got.at[pl.ds(1, peers - 1)]
        return pltpu.make_async_remote_copy(
            src_ref=others,
            dst_ref=others,
            send_sem=ex_send.at[g],
            recv_sem=ex_recv.at[g],
            device_id={"asset": me},
            device_id_type=MESH,
        )

    sub = lax.broadcasted_iota(jnp.int32, (TILE, LANES), 0)
    lane = lax.broadcasted_iota(jnp.int32, (TILE, LANES), 1)
    subc = lax.broadcasted_iota(jnp.int32, (TILE, CHUNK), 0)
    width = fields * TILE

    def lanes(c):
        return pl.ds(c * CHUNK, CHUNK)

    def fold(v):
        acc = v[:, :LANES]
        for i in range(1, CHUNK // LANES):
            acc = acc + v[:, i * LANES : (i + 1) * LANES]
        return acc

    def across(v):
        return jnp.sum(v, axis=1, keepdims=True)

    def flat(columns):
        z = jnp.zeros((TILE, LANES), jnp.float32)
        for at, column in columns:
            z = jnp.where(lane == sub + at, column, z)
        return jnp.sum(z, axis=0, keepdims=True)

    def column(row, at):
        return across(jnp.where(lane == sub + at, row, 0.0))

    def listed(c, first):
        t = subc + first
        o = opened[:, lanes(c)]
        u = closed[:, lanes(c)]
        return t, o, u, (t >= o) & (t < u)

    def share(t, o, u, w):
        low = jnp.maximum(jnp.maximum(t - (WINDOW - 1), o), 0)
        high = jnp.minimum(t, u - 1)
        counted = jnp.maximum(high - low + 1, 1).astype(jnp.float32)
        return jnp.where(w, 1.0 / counted, 0.0)

    def moments(count, s, q, pivots, which):
        inverse = 1.0 / jnp.maximum(count, 1.0)
        columns = []
        means = []
        for f, s_l, q_l, pivot_f in zip(which, s, q, pivots):
            s_f, q_f = across(s_l), across(q_l)
            lift = s_f * inverse
            mean = pivot_f + lift
            means.append(mean)
            columns.append((f * TILE, mean))
            columns.append((width + f * TILE, jnp.maximum(q_f - s_f * lift, 0.0)))
        return means, columns

    def counts_at(count, at):
        return [(at + f * TILE, count) for f in range(fields)]

    zero = jnp.zeros((TILE, LANES), jnp.float32)

    for copy in dates:
        copy.wait()
    msg_b1[...] = jnp.zeros_like(msg_b1)
    base[...] = jnp.zeros_like(base)
    load(0).wait()

    def prefix(f, c, w, v):
        p = jnp.where(w, v, 0.0)
        for k in (1, 2, 4):
            p = p + jnp.where(subc >= k, pltpu.roll(p, k, 0), 0.0)
        p = p + base[f, :, lanes(c)]
        base[f, :, lanes(c)] = jnp.broadcast_to(p[TILE - 1 :, :], p.shape)
        return p

    def first_tile(r, carry):
        n = zero
        here = pl.ds(pl.multiple_of(r * TILE, TILE), TILE)
        for c in range(chunks):
            _, _, _, w = listed(c, t0 + r * TILE)
            n = n + fold(jnp.where(w, 1.0, 0.0))
            for f in range(fields):
                p = prefix(f, c, w, out[f, here, lanes(c)])
                ring[f, here, lanes(c)] = p
                out[f, here, lanes(c)] = p
        count = across(n)
        local_count[r] = jnp.broadcast_to(count, zero.shape)
        msg_b1[pl.ds(wt - 1 - r, 1), :] = flat(counts_at(count, 3 * width))
        return carry

    lax.fori_loop(0, wt, first_tile, 0)

    for f in range(fields):
        rough = zero
        for c in range(chunks):
            rough = rough + fold(base[f, :, lanes(c)])
        pivot[f] = jnp.broadcast_to(across(rough) * (1.0 / (WINDOW * assets)), zero.shape)

    def window_tile(ref, here, first, i, pivots, which):
        slot = pl.ds(pl.multiple_of(i * TILE, TILE), TILE)
        n = zero
        s = [zero] * fields
        q = [zero] * fields
        for c in range(chunks):
            t, o, u, w = listed(c, first)
            n = n + fold(jnp.where(w, 1.0, 0.0))
            part = share(t, o, u, w)
            for f in which:
                p = prefix(f, c, w, ref[f, here, lanes(c)])
                old = ring[f, slot, lanes(c)]
                ring[f, slot, lanes(c)] = p
                rolled = (p + (total[f, :, lanes(c)] - old)) * part
                ref[f, here, lanes(c)] = rolled
                d = jnp.where(w, rolled - pivots[f], 0.0)
                s[f] = s[f] + fold(d)
                q[f] = q[f] + fold(d * d)
        count = across(n)
        means, columns = moments(
            count, [s[f] for f in which], [q[f] for f in which], [pivots[f] for f in which], which)
        return means, flat(columns + counts_at(count, 2 * width))

    def bulk_tile(b, i, pivots):
        r = b * wt + i
        here = pl.ds(pl.multiple_of(r * TILE, TILE), TILE)
        means, line = window_tile(out, here, t0 + r * TILE, i, pivots, every)
        at = pl.ds(r - wt, 1)
        msg_b1[at, :] = msg_b1[at, :] + line
        return means

    def bulk_block(b):
        total[...] = base[...]
        base[...] = jnp.zeros_like(base)

        def pair(i, carry):
            pivots = [pivot[f][:, :1] for f in range(fields)]
            lower = bulk_tile(b, 2 * i, pivots)
            upper = bulk_tile(b, 2 * i + 1, pivots)
            for f in range(fields):
                pivot[f] = jnp.broadcast_to(upper[f], zero.shape)
            if b == 1:

                @pl.when(i == 0)
                def _():
                    for f in range(fields):
                        ahead[f] = jnp.broadcast_to(lower[f], zero.shape)

            return carry

        lax.fori_loop(0, wt // 2, pair, 0)

    for b in range(1, rows // WINDOW):
        hear(b - 1)
        tell(b)
        load(b).wait()
        bulk_block(b)
    hear(rows // WINDOW - 1)
    exchange_start(0, msg_b1, got_b1)


    @pl.when(last)
    def _():
        pass1(range(len(around)))

    def scaled(center, spread):
        inv = 1.0 / jnp.sqrt(jnp.maximum(spread, 0.0) + 0.1)
        wide = lax.broadcasted_iota(jnp.int32, center.shape, 1)
        return jnp.where(wide % (2 * width) < width, center, pltpu.roll(inv, width, 1))

    def left(v, by):
        return pltpu.roll(v, LANES - by, 1)

    def sum_over(term, shape):
        step = 8
        nothing = tuple(jnp.zeros(shape, jnp.float32) for _ in range(2))

        def some(i, acc):
            acc = list(acc)
            for j in range(step):
                acc[j % 2] = acc[j % 2] + term(i * step + j)
            return tuple(acc)

        if shape[0] <= TILE:
            acc = nothing
            for i in range(peers // step):
                acc = some(i, acc)
        else:
            acc = lax.fori_loop(0, peers // step, some, nothing)
        return acc[0] + acc[1]

    def merge(got, counts, floor, m2, rows_out):
        shape = rows_out.shape
        center = sum_over(lambda p: counts(p) * got[p], shape) / floor

        def spread_term(p):
            d = got[p] - center
            return counts(p) * d * d

        rows_out[...] = scaled(center, (sum_over(spread_term, shape) + m2) / floor)

    def summed(got):
        return sum_over(lambda p: got[p], got.shape[1:])

    def columns_of(row_in, row, which, at=0):
        line = jnp.broadcast_to(row_in[pl.ds(row, 1), :], zero.shape)
        center = {f: column(line, at + f * TILE) for f in which}
        inv = {f: column(line, at + width + f * TILE) for f in which}
        return center, inv

    def clipped_sums(ref, r, row, row_in, which, mark=0.0, at=0, read=0):
        here = pl.ds(pl.multiple_of(r * TILE, TILE), TILE)
        first = t0 + r * TILE if ref is out else t0 + rows + r * TILE
        center, inv = columns_of(row_in, row, which, read)
        s = {f: zero for f in which}
        q = {f: zero for f in which}
        for c in range(chunks):
            _, _, _, w = listed(c, first)
            for f in which:
                y = (ref[f, here, lanes(c)] - center[f]) * inv[f]
                y = jnp.clip(y, -3.0, 3.0)
                if ref is out:
                    ref[f, here, lanes(c)] = jnp.where(w, y, mark)
                y = jnp.where(w, y, 0.0)
                s[f] = s[f] + fold(y)
                q[f] = q[f] + fold(y * y)
        columns = []
        for f in which:
            columns.append((at + f * TILE, across(s[f])))
            columns.append((at + width + f * TILE, across(q[f])))
        return columns

    def clip_tile(ref, r, row, row_in, msg, msg_row, which, mark=0.0):
        columns = clipped_sums(ref, r, row, row_in, which, mark)
        msg[pl.ds(msg_row, 1), :] = flat(columns)

    def merge2(got, floor, rows_out):
        sums = summed(got)
        center = sums / floor
        spread = left(sums, width) / floor - center * center
        rows_out[...] = scaled(center, spread)

    def final_tile(r, row, row_in, which, at=0):
        here = pl.ds(pl.multiple_of(r * TILE, TILE), TILE)
        center, inv = columns_of(row_in, row, which, at)
        for c in range(chunks):
            _, _, _, w = listed(c, t0 + r * TILE)
            for f in which:
                y = (out[f, here, lanes(c)] - center[f]) * inv[f]
                out[f, here, lanes(c)] = jnp.where(w, y, 0.0)

    def over(n, step, unroll=1):
        def one(i, carry):
            step(i)
            return carry

        lax.fori_loop(0, n, one, 0, unroll=unroll)

    def arrival(f, r, h):
        if (f, r, h) in around:
            relay2(around.index((f, r, h))).wait_recv()
        elif h == 0:
            for i, (tile, cut) in enumerate(straight):
                if tile == r and cut[0] == f:
                    direct(i).wait_recv()

    def joined(f, c, here, past):
        h = jnp.where(past, halo[f, here, lanes(c)], 0.0)
        for j in (1, 2, 4):
            up = pltpu.roll(h, TILE - j, 0)
            h = h + jnp.where(subc < TILE - j, up, 0.0)
        before = suffix[f, :, lanes(c)]
        after = jnp.where(subc < TILE - 1, pltpu.roll(h, TILE - 1, 0), 0.0)
        suffix[f, :, lanes(c)] = before + jnp.broadcast_to(h[:1, :], h.shape)
        return out[f, here, lanes(c)] + (before + after)

    def before_mask(c, t, r):
        _, _, _, past = listed(c, t0 + r * TILE - WINDOW)
        return past & (t >= WINDOW)

    def halo_part(r, msg, row, counted_too, which):
        here = tile_rows(r)
        s = {f: zero for f in which}
        q = {f: zero for f in which}
        pivots = {f: ahead[f][:, :1] for f in which}
        for c in range(chunks):
            t, o, u, w = listed(c, t0 + r * TILE)
            past = before_mask(c, t, r)
            part = share(t, o, u, w)
            for f in which:
                rolled = joined(f, c, here, past) * part
                out[f, here, lanes(c)] = rolled
                d = jnp.where(w, rolled - pivots[f], 0.0)
                s[f] = s[f] + fold(d)
                q[f] = q[f] + fold(d * d)
        count = local_count[r][:, :1]
        means, columns = moments(
            count,
            [s[f] for f in which],
            [q[f] for f in which],
            [pivots[f] for f in which],
            which,
        )
        for f, mean in zip(which, means):
            ahead[f] = jnp.broadcast_to(mean, zero.shape)
        if counted_too:
            columns = columns + counts_at(count, 2 * width)
        at = pl.ds(row % DEEP if msg is msg_g1 else row, 1)
        shift = 2 * width * (row // DEEP) if msg is msg_g1 else 0
        msg[at, :] = msg[at, :] + flat([(n + shift, v) for n, v in columns])

    def group_tile(r, which):
        @pl.when(has_prev)
        def _():
            for f in which:
                arrival(f, r, 0)

        halo_part(r, msg_g1, wt - 1 - r, False, which)

    def finish(r, which):
        here = tile_rows(r)
        first = columns_of(told.at[0], r, which)
        then = columns_of(told.at[1], r, which)
        per = chunks // HALVES
        for h in range(HALVES):
            for f in which:
                arrival(f, r, h)
            for c in range(h * per, (h + 1) * per):
                t, o, u, w = listed(c, t0 + r * TILE)
                past = before_mask(c, t, r)
                part = share(t, o, u, w)
                for f in which:
                    y = joined(f, c, here, past) * part
                    y = jnp.clip((y - first[0][f]) * first[1][f], -3.0, 3.0)
                    y = (y - then[0][f]) * then[1][f]
                    out[f, here, lanes(c)] = jnp.where(w, y, 0.0)

    suffix[...] = jnp.zeros_like(suffix)
    msg_e1[...] = jnp.zeros_like(msg_e1)
    msg_g1[...] = jnp.zeros_like(msg_g1)
    msg_e2[...] = jnp.zeros_like(msg_e2)


    def second(ks):
        @pl.when((x == 0) | last)
        def _():
            pass2(ks)

    group_tile(7, every)
    group_tile(6, every)

    @pl.when(x == 0)
    def _():
        for r in range(tops - 1, -1, -1):
            halo_part(r, msg_e1, tops + r, True, early(r))

    exchange_all(0, got_b1).wait_recv()

    def doubled(v):
        high = pltpu.roll(pltpu.roll(v, wt - DEEP, 0), 2 * width, 1)
        return jnp.where(lane < 2 * width, v, high)

    def split(p):
        v = got_b1[p]
        count_b[p] = left(v, 2 * width)
        count_h[p] = doubled(left(v[:wt, :], 3 * width))

    over(peers, split, 8)
    sums = summed(got_b1)
    floor_b[...] = jnp.maximum(left(sums, 2 * width), 1.0)
    floor_h[...] = jnp.maximum(doubled(left(sums[:wt, :], 3 * width)), 1.0)
    merge(got_b1, lambda p: count_b[p], floor_b[...], left(sums, width), row_b1)
    group_tile(5, every)

    @pl.when(has_next)
    def _():
        total[...] = base[...]
        base[...] = jnp.zeros_like(base)
        for copy in extensions:
            copy.wait_recv()

        def one(r, which):
            here = pl.ds(pl.multiple_of(r * TILE, TILE), TILE)
            pivots = [pivot[f][:, :1] for f in every]
            means, line = window_tile(ext, here, t0 + rows + r * TILE, r, pivots, which)
            for f, mean in zip(which, means):
                pivot[f] = jnp.broadcast_to(mean, zero.shape)
            msg_e1[pl.ds(r, 1), :] = line

        over(EARLY, lambda r: one(r, every))
        if EXTRA:
            one(EARLY, extra)

    exchange_start(2, msg_e1, got_e1)
    pairs = bulk // 2

    def clip_pair(j):
        columns = clipped_sums(out, j + wt, j, row_b1, every)
        i = j + pairs
        columns += clipped_sums(out, i + wt, i, row_b1, every, at=2 * width)
        msg_b2[pl.ds(j, 1), :] = flat(columns)

    over(pairs, clip_pair)
    exchange_start(1, msg_b2, got_b2)
    some = range(6)

    @pl.when(x < blocks_t - 2)
    def _():
        pass1(some)

    @pl.when(x == blocks_t - 2)
    def _():
        pass2(some)

    group_tile(4, every)
    exchange_all(2, got_e1).wait_recv()

    def split_e(p):
        count_e[p] = left(got_e1[p], 2 * width)

    over(peers, split_e, peers)
    sums = summed(got_e1)
    floor_e = jnp.maximum(left(sums, 2 * width), 1.0)
    first_params, second_params = params.at[0], params.at[1, pl.ds(0, tops)]
    merge(got_e1, lambda p: count_e[p], floor_e, left(sums, width), first_params)

    @pl.when(has_next)
    def _():
        for r in range(tops):
            clip_tile(ext, r, r, first_params, msg_e2, r, early(r))

    @pl.when(x == 0)
    def _():
        for r in range(tops):
            columns = clipped_sums(
                out, r, tops + r, first_params, early(r), at=2 * width
            )
            at = pl.ds(r, 1)
            msg_e2[at, :] = msg_e2[at, :] + flat(columns)

    exchange_start(3, msg_e2, got_e2)
    rest = range(6, len(around))

    @pl.when(x < blocks_t - 2)
    def _():
        pass1(rest)

    @pl.when(x == blocks_t - 2)
    def _():
        pass2(rest)

    group_tile(3, kept[:-1])
    group_tile(3, kept[-1:])
    exchange_start(4, msg_g1, got_g1)
    second([0,1])
    second([2,3])
    exchange_all(3, got_e2).wait_recv()
    upper = pltpu.roll(pltpu.roll(floor_e, tops, 0), 2 * width, 1)
    wide = lax.broadcasted_iota(jnp.int32, floor_e.shape, 1)
    floor_e = jnp.where(wide < 2 * width, floor_e, upper)[:tops, :]
    merge2(got_e2, floor_e, second_params)

    @pl.when(has_next)
    def _():
        telling.start()
        direct(len(straight) - 1).start()


    @pl.when(x == 0)
    def _():
        for r in range(tops):
            final_tile(r, r, second_params, early(r), 2 * width)

    second([4,5])
    exchange_all(4, got_g1).wait_recv()
    second([6,7])
    m2 = left(summed(got_g1), width)
    merge(got_g1, lambda p: count_h[p, :DEEP, :], floor_h[:DEEP, :], m2, row_g1)
    packed = [[] for _ in range(DEEP)]
    for r in range(wt - 1, EARLY - 1, -1):
        i = wt - 1 - r
        at = 2 * width * (i // DEEP)
        packed[i % DEEP] += clipped_sums(
            out, r, i % DEEP, row_g1, grouped(r), MARK, at, at
        )
    for i in range(DEEP):
        msg_g2[pl.ds(i, 1), :] = flat(packed[i])
    exchange_start(5, msg_g2, got_g2)
    second([8,9])
    exchange_all(1, got_b2).wait_recv()
    low, high = floor_b[pl.ds(0, pairs), :], floor_b[pl.ds(pairs, pairs), :]
    wide = lax.broadcasted_iota(jnp.int32, low.shape, 1)
    both = jnp.where(wide < 2 * width, low, pltpu.roll(high, 2 * width, 1))
    merge2(got_b2, both, row_b2)

    def final_pair(j):
        final_tile(j + wt, j, row_b2, every)
        final_tile(j + pairs + wt, j, row_b2, every, 2 * width)

    over(pairs, final_pair)


    @pl.when(has_prev)
    def _():
        telling.wait_recv()


    @pl.when(has_prev)
    def _():
        for r in range(EARLY, tops):
            finish(r, extra)
        for r in range(EARLY - 1, -1, -1):
            finish(r, [f for f in every if (f, r) not in BACK])
            finish(r, [f for f in every if (f, r) in BACK])

    exchange_all(5, got_g2).wait_recv()
    merge2(got_g2, floor_h[:DEEP, :], out.at[0, pl.ds(rows, DEEP), pl.ds(0, LANES)])
    for g, got in enumerate((got_b1, got_b2, got_e1, got_e2, got_g1, got_g2)):
        exchange_all(g, got).wait_send()

    @pl.when(has_prev)
    def _():
        for copy in extensions:
            copy.wait_send()

    @pl.when(has_next)
    def _():
        telling.wait_send()
        for k in range(len(around)):
            back(k).wait_send()
        for i in range(len(straight)):
            direct(i).wait_send()

    @pl.when(hops1)
    def _():
        for k in range(len(around)):
            relay1(k).wait_send()

    @pl.when(hops2)
    def _():
        for k in range(len(around)):
            relay2(k).wait_send()


def writer(x_ref, o_ref, tile_ref, sem, sem_tile):
    fields, rows, assets = o_ref.shape
    wt = WINDOW // TILE
    step = (rows - WINDOW) // 2
    spans = []
    for f in range(fields):
        tops = EARLY + (1 if f >= fields - EXTRA else 0)
        spans.append((f, 0, tops * TILE))
        spans.extend((f, WINDOW + i * step, step) for i in range(2))
    copies = [
        pltpu.make_async_copy(
            x_ref.at[f, pl.ds(at, size), :], o_ref.at[f, pl.ds(at, size), :], sem.at[i]
        )
        for i, (f, at, size) in enumerate(spans)
    ]
    for copy in copies:
        copy.start()
    sub = lax.broadcasted_iota(jnp.int32, (TILE, LANES), 0)
    lane = lax.broadcasted_iota(jnp.int32, (TILE, LANES), 1)
    width = fields * TILE
    for i in range(wt - EARLY):
        r = wt - 1 - i
        many = fields if r > EARLY else fields - EXTRA
        here, there = pl.ds(r * TILE, TILE), pl.ds(i * TILE, TILE)
        row = x_ref[0, pl.ds(rows + i % DEEP, 1), :LANES]
        line = jnp.broadcast_to(row, (TILE, LANES))
        shift = 2 * width * (i // DEEP)

        def column(at):
            kept = jnp.where(lane == sub + at, line, 0.0)
            return jnp.sum(kept, axis=1, keepdims=True)

        for f in range(many):
            center = column(shift + f * TILE)
            inv = column(shift + width + f * TILE)
            for c in range(assets // CHUNK):
                part = pl.ds(c * CHUNK, CHUNK)
                y = x_ref[f, here, part]
                z = jnp.where(y > 3.5, 0.0, (y - center) * inv)
                tile_ref[f, there, part] = z
        copy = pltpu.make_async_copy(
            tile_ref.at[pl.ds(0, many), there, :],
            o_ref.at[pl.ds(0, many), here, :],
            sem_tile.at[i],
        )
        copy.start()
        copies.append(copy)
    for copy in copies:
        copy.wait()


def per_device(blocks_t, peers, values, listed_from, listed_until):
    fields, rows, assets = values.shape
    tiles = rows // TILE
    wt = WINDOW // TILE
    bulk = tiles - wt
    f32 = jnp.float32
    vmem = pltpu.VMEM
    dma = pltpu.SemaphoreType.DMA
    around = len(BACK) * HALVES
    tops = EARLY + (1 if EXTRA else 0)
    groups = (bulk, bulk // 2, 2 * tops, tops, DEEP, DEEP)
    scratch = [
        vmem((1, assets), jnp.int32),
        vmem((1, assets), jnp.int32),
        dma((2,)),
        pltpu.SemaphoreType.REGULAR((4,)),
        vmem((wt, TILE, LANES), f32),
        vmem((fields, WINDOW, assets), f32),
        vmem((around * TILE, assets // HALVES), f32),
        vmem((around * TILE, assets // HALVES), f32),
        vmem((fields, tops * TILE, assets), f32),
        vmem((2, 2 * tops, LANES), f32),
        vmem((2, 2 * tops, LANES), f32),
        vmem((fields, WINDOW, assets), f32),
        vmem((fields, TILE, assets), f32),
        vmem((fields, TILE, assets), f32),
        vmem((fields, TILE, assets), f32),
        vmem((fields, TILE, LANES), f32),
        vmem((fields, TILE, LANES), f32),
        *[vmem((n, LANES), f32) for n in groups],
        *[vmem((peers, n, LANES), f32) for n in groups],
        *[vmem((peers, n, LANES), f32) for n in (bulk, 2 * tops, wt)],
        *[vmem((n, LANES), f32) for n in (bulk, wt)],
        *[vmem((n, LANES), f32) for n in (bulk, bulk // 2, DEEP)],
        dma((rows // WINDOW,)),
        dma,
        dma((2,)),
        dma((2,)),
        dma,
        dma,
        dma,
        dma,
        dma,
        dma((wt + 2,)),
        dma((around,)),
        dma((around,)),
        dma((around,)),
        dma((6,)),
        dma((6,)),
    ]
    clipped = pl.pallas_call(
        functools.partial(kernel, (blocks_t, peers)),
        out_shape=pltpu.VMEM((fields, rows + TILE, assets), values.dtype),
        in_specs=[
            pl.BlockSpec(memory_space=pltpu.HBM),
            pl.BlockSpec(memory_space=pltpu.HBM),
            pl.BlockSpec(memory_space=pltpu.HBM),
        ],
        out_specs=pl.BlockSpec(memory_space=pltpu.VMEM),
        scratch_shapes=scratch,
        compiler_params=pltpu.CompilerParams(
            collective_id=0,
            has_side_effects=True,
            vmem_limit_bytes=48 * 1024 * 1024,
        ),
    )(values, listed_from[None, :], listed_until[None, :])
    return pl.pallas_call(
        writer,
        out_shape=jax.ShapeDtypeStruct(values.shape, values.dtype),
        in_specs=[pl.BlockSpec(memory_space=pltpu.VMEM)],
        out_specs=pl.BlockSpec(memory_space=pltpu.HBM),
        scratch_shapes=[
            vmem((fields, WINDOW - EARLY * TILE, assets), f32),
            dma((3 * fields,)),
            dma((wt - EARLY,)),
        ],
        compiler_params=pltpu.CompilerParams(vmem_limit_bytes=8 * 1024 * 1024),
    )(pltpu.with_memory_space_constraint(clipped, pltpu.VMEM))


def solution(mesh):
    in_specs = (P(None, "tm", "asset"), P("asset"), P("asset"))
    out_specs = P(None, "tm", "asset")
    body = functools.partial(per_device, mesh.shape["tm"], mesh.shape["asset"])
    return jax.shard_map(
        body, mesh=mesh, in_specs=in_specs, out_specs=out_specs, check_vma=False
    )
```

```python
import functools

import jax
import jax.numpy as jnp
from jax import lax
from jax.experimental import pallas as pl
from jax.experimental.pallas import tpu as pltpu
from jax.sharding import PartitionSpec as P

WINDOW = 64
EARLY = 3
BACK = ((3, 2), (3, 1), (2, 1), (3, 0), (2, 0))
EXTRA = 1
HALVES = 2
MARK = 4.0
DEEP = 3
TILE = 8
LANES = 128
CHUNK = 512
MESH = pl.DeviceIdType.MESH


def kernel(
    sizes,
    vals,
    opened_in,
    closed_in,
    out,
    opened,
    closed,
    list_sem,
    rounds,
    local_count,
    halo,
    hop1,
    hop2,
    ext,
    params,
    told,
    ring,
    total,
    base,
    suffix,
    ahead,
    pivot,
    msg_b1,
    msg_b2,
    msg_e1,
    msg_e2,
    msg_g1,
    msg_g2,
    got_b1,
    got_b2,
    got_e1,
    got_e2,
    got_g1,
    got_g2,
    count_b,
    count_e,
    count_h,
    floor_b,
    floor_h,
    row_b1,
    row_b2,
    row_g1,
    load_sem,
    direct_send,
    ext_send,
    ext_recv,
    told_send,
    told_recv,
    back_send,
    relay1_send,
    relay2_send,
    halo_recv,
    back_recv,
    hop1_recv,
    hop2_recv,
    ex_send,
    ex_recv,
):
    blocks_t, peers = sizes
    fields, rows, assets = vals.shape
    tiles = rows // TILE
    wt = WINDOW // TILE
    chunks = assets // CHUNK
    bulk = tiles - wt
    x = lax.axis_index("tm")
    me = lax.axis_index("asset")
    nxt = lax.rem(x + 1, blocks_t)
    prv = lax.rem(x + blocks_t - 1, blocks_t)
    t0 = x * rows

    dates = [
        pltpu.make_async_copy(opened_in, opened, list_sem.at[0]),
        pltpu.make_async_copy(closed_in, closed, list_sem.at[1]),
    ]
    for copy in dates:
        copy.start()

    def load(b):
        part = pl.ds(b * WINDOW, WINDOW)
        return pltpu.make_async_copy(
            vals.at[:, part, :], out.at[:, part, :], load_sem.at[b]
        )

    for b in range(rows // WINDOW):
        load(b).start()

    core = lax.rem(me, 2)
    chip = me // 2
    y, z = chip // 4, lax.rem(chip, 4)

    def at_place(dy, dz, dc):
        to = lax.rem(y + dy, 4) * 4 + lax.rem(z + dz, 4)
        return to * 2 + lax.rem(core + dc, 2)

    near = [at_place(0, 0, 1)]
    near += [at_place(1, 0, 0), at_place(3, 0, 0), at_place(0, 1, 0), at_place(0, 3, 0)]
    barrier = pltpu.get_barrier_semaphore()
    for t in (nxt, prv):
        pl.semaphore_signal(barrier, 1, device_id={"tm": t}, device_id_type=MESH)
    for peer in near:
        pl.semaphore_signal(barrier, 1, device_id={"asset": peer}, device_id_type=MESH)
    pl.semaphore_wait(barrier, 2 + len(near))

    def tell(i):
        for peer in near:
            pl.semaphore_signal(
                rounds.at[i], 1, device_id={"asset": peer}, device_id_type=MESH
            )

    def hear(i):
        pl.semaphore_wait(rounds.at[i], len(near))

    tell(0)

    tail = rows - WINDOW

    def tile_rows(r):
        return pl.ds(r * TILE, TILE)

    def needed(at, r):
        skip = 1 if r == 0 else 0
        return pl.ds(at + skip, TILE - skip)


    every = list(range(fields))
    kept, extra = every[: fields - EXTRA], every[fields - EXTRA :]
    tops = EARLY + (1 if EXTRA else 0)
    piece = assets // HALVES
    tiles_back = sorted({r for _, r in BACK}, reverse=True)
    around = [
        (f, r, h) for t in tiles_back for h in range(HALVES) for f, r in BACK if r == t
    ]

    def early(r):
        return every if r < EARLY else extra

    def grouped(r):
        return every if r > EARLY else kept

    def half(h):
        return pl.ds(h * piece, piece)

    straight = []
    for r in range(wt - 1, -1, -1):
        left_over = [f for f in every if (f, r) not in BACK]
        if r == EARLY:
            cuts = [kept[:-1], kept[-1:], extra]
        else:
            cuts = [left_over]
        straight.extend((r, cut) for cut in cuts if cut)

    def direct(i):
        r, cut = straight[i]
        which = pl.ds(cut[0], len(cut))
        return pltpu.make_async_remote_copy(
            src_ref=vals.at[which, needed(tail + r * TILE, r), :],
            dst_ref=halo.at[which, needed(r * TILE, r), :],
            send_sem=direct_send,
            recv_sem=halo_recv.at[i],
            device_id={"tm": nxt},
            device_id_type=MESH,
        )

    def back(k):
        f, r, h = around[k]
        return pltpu.make_async_remote_copy(
            src_ref=vals.at[f, needed(tail + r * TILE, r), half(h)],
            dst_ref=hop1.at[needed(k * TILE, r), :],
            send_sem=back_send,
            recv_sem=hop1_recv.at[k],
            device_id={"tm": prv},
            device_id_type=MESH,
        )

    def relay1(k):
        part = needed(k * TILE, around[k][1])
        return pltpu.make_async_remote_copy(
            src_ref=hop1.at[part, :],
            dst_ref=hop2.at[part, :],
            send_sem=relay1_send,
            recv_sem=hop2_recv.at[k],
            device_id={"tm": prv},
            device_id_type=MESH,
        )

    def relay2(k):
        f, r, h = around[k]
        return pltpu.make_async_remote_copy(
            src_ref=hop2.at[needed(k * TILE, r), :],
            dst_ref=halo.at[f, needed(r * TILE, r), half(h)],
            send_sem=relay2_send,
            recv_sem=back_recv.at[k],
            device_id={"tm": prv},
            device_id_type=MESH,
        )

    def pass1(ks):
        for k in ks:
            back(k).wait_recv()
            relay1(k).start()

    def pass2(ks):
        for k in ks:
            relay1(k).wait_recv()
            relay2(k).start()

    def extension(i):
        which = (pl.ds(0, fields), pl.ds(fields - EXTRA, EXTRA))[i]
        part = (pl.ds(0, EARLY * TILE), pl.ds(EARLY * TILE, TILE))[i]
        return pltpu.make_async_remote_copy(
            src_ref=vals.at[which, part, :],
            dst_ref=ext.at[which, part, :],
            send_sem=ext_send.at[i],
            recv_sem=ext_recv.at[i],
            device_id={"tm": prv},
            device_id_type=MESH,
        )

    extensions = [extension(i) for i in range(2 if EXTRA else 1)]
    telling = pltpu.make_async_remote_copy(
        src_ref=params,
        dst_ref=told,
        send_sem=told_send,
        recv_sem=told_recv,
        device_id={"tm": nxt},
        device_id_type=MESH,
    )

    has_prev = x > 0
    has_next = x < blocks_t - 1
    last = x == blocks_t - 1
    hops1 = x != blocks_t - 2
    hops2 = x != blocks_t - 3
    @pl.when(has_prev)
    def _():
        for copy in extensions:
            copy.start()

    @pl.when(has_next)
    def _():
        for k in range(len(around)):
            back(k).start()
        for i in range(len(straight) - 1):
            direct(i).start()

    def hops(d):
        return min(d[0], 4 - d[0]) + min(d[1], 4 - d[1]) + d[2] / 2

    places = [(dy, dz, dc) for dy in range(4) for dz in range(4) for dc in range(2)]
    places = sorted(places[1:], key=hops, reverse=True)

    def exchange(g, msg, got, k, peer):
        return pltpu.make_async_remote_copy(
            src_ref=msg,
            dst_ref=got.at[k],
            send_sem=ex_send.at[g],
            recv_sem=ex_recv.at[g],
            device_id={"asset": peer},
            device_id_type=MESH,
        )

    def exchange_start(g, msg, got):
        for d in places:
            k = (d[0] * 4 + d[1]) * 2 + d[2]
            exchange(g, msg, got, k, at_place(*d)).start()
        got[0] = msg[...]

    def exchange_all(g, got):
        others = got.at[pl.ds(1, peers - 1)]
        return pltpu.make_async_remote_copy(
            src_ref=others,
            dst_ref=others,
            send_sem=ex_send.at[g],
            recv_sem=ex_recv.at[g],
            device_id={"asset": me},
            device_id_type=MESH,
        )

    sub = lax.broadcasted_iota(jnp.int32, (TILE, LANES), 0)
    lane = lax.broadcasted_iota(jnp.int32, (TILE, LANES), 1)
    subc = lax.broadcasted_iota(jnp.int32, (TILE, CHUNK), 0)
    width = fields * TILE

    def lanes(c):
        return pl.ds(c * CHUNK, CHUNK)

    def fold(v):
        acc = v[:, :LANES]
        for i in range(1, CHUNK // LANES):
            acc = acc + v[:, i * LANES : (i + 1) * LANES]
        return acc

    def across(v):
        return jnp.sum(v, axis=1, keepdims=True)

    def flat(columns):
        z = jnp.zeros((TILE, LANES), jnp.float32)
        for at, column in columns:
            z = jnp.where(lane == sub + at, column, z)
        return jnp.sum(z, axis=0, keepdims=True)

    def column(row, at):
        return across(jnp.where(lane == sub + at, row, 0.0))

    def listed(c, first):
        t = subc + first
        o = opened[:, lanes(c)]
        u = closed[:, lanes(c)]
        return t, o, u, (t >= o) & (t < u)

    def share(t, o, u, w):
        low = jnp.maximum(jnp.maximum(t - (WINDOW - 1), o), 0)
        high = jnp.minimum(t, u - 1)
        counted = jnp.maximum(high - low + 1, 1).astype(jnp.float32)
        return jnp.where(w, 1.0 / counted, 0.0)

    def moments(count, s, q, pivots, which):
        inverse = 1.0 / jnp.maximum(count, 1.0)
        columns = []
        means = []
        for f, s_l, q_l, pivot_f in zip(which, s, q, pivots):
            s_f, q_f = across(s_l), across(q_l)
            lift = s_f * inverse
            mean = pivot_f + lift
            means.append(mean)
            columns.append((f * TILE, mean))
            columns.append((width + f * TILE, jnp.maximum(q_f - s_f * lift, 0.0)))
        return means, columns

    def counts_at(count, at):
        return [(at + f * TILE, count) for f in range(fields)]

    zero = jnp.zeros((TILE, LANES), jnp.float32)

    for copy in dates:
        copy.wait()
    msg_b1[...] = jnp.zeros_like(msg_b1)
    base[...] = jnp.zeros_like(base)
    load(0).wait()

    def prefix(f, c, w, v):
        p = jnp.where(w, v, 0.0)
        for k in (1, 2, 4):
            p = p + jnp.where(subc >= k, pltpu.roll(p, k, 0), 0.0)
        p = p + base[f, :, lanes(c)]
        base[f, :, lanes(c)] = jnp.broadcast_to(p[TILE - 1 :, :], p.shape)
        return p

    def first_tile(r, carry):
        n = zero
        here = pl.ds(pl.multiple_of(r * TILE, TILE), TILE)
        for c in range(chunks):
            _, _, _, w = listed(c, t0 + r * TILE)
            n = n + fold(jnp.where(w, 1.0, 0.0))
            for f in range(fields):
                p = prefix(f, c, w, out[f, here, lanes(c)])
                ring[f, here, lanes(c)] = p
                out[f, here, lanes(c)] = p
        count = across(n)
        local_count[r] = jnp.broadcast_to(count, zero.shape)
        msg_b1[pl.ds(wt - 1 - r, 1), :] = flat(counts_at(count, 3 * width))
        return carry

    lax.fori_loop(0, wt, first_tile, 0)

    for f in range(fields):
        rough = zero
        for c in range(chunks):
            rough = rough + fold(base[f, :, lanes(c)])
        pivot[f] = jnp.broadcast_to(across(rough) * (1.0 / (WINDOW * assets)), zero.shape)

    def window_tile(ref, here, first, i, pivots, which):
        slot = pl.ds(pl.multiple_of(i * TILE, TILE), TILE)
        n = zero
        s = [zero] * fields
        q = [zero] * fields
        for c in range(chunks):
            t, o, u, w = listed(c, first)
            n = n + fold(jnp.where(w, 1.0, 0.0))
            part = share(t, o, u, w)
            for f in which:
                p = prefix(f, c, w, ref[f, here, lanes(c)])
                old = ring[f, slot, lanes(c)]
                ring[f, slot, lanes(c)] = p
                rolled = (p + (total[f, :, lanes(c)] - old)) * part
                ref[f, here, lanes(c)] = rolled
                d = jnp.where(w, rolled - pivots[f], 0.0)
                s[f] = s[f] + fold(d)
                q[f] = q[f] + fold(d * d)
        count = across(n)
        means, columns = moments(
            count, [s[f] for f in which], [q[f] for f in which], [pivots[f] for f in which], which)
        return means, flat(columns + counts_at(count, 2 * width))

    def bulk_tile(b, i, pivots):
        r = b * wt + i
        here = pl.ds(pl.multiple_of(r * TILE, TILE), TILE)
        means, line = window_tile(out, here, t0 + r * TILE, i, pivots, every)
        at = pl.ds(r - wt, 1)
        msg_b1[at, :] = msg_b1[at, :] + line
        return means

    def bulk_block(b):
        total[...] = base[...]
        base[...] = jnp.zeros_like(base)

        def pair(i, carry):
            pivots = [pivot[f][:, :1] for f in range(fields)]
            lower = bulk_tile(b, 2 * i, pivots)
            upper = bulk_tile(b, 2 * i + 1, pivots)
            for f in range(fields):
                pivot[f] = jnp.broadcast_to(upper[f], zero.shape)
            if b == 1:

                @pl.when(i == 0)
                def _():
                    for f in range(fields):
                        ahead[f] = jnp.broadcast_to(lower[f], zero.shape)

            return carry

        lax.fori_loop(0, wt // 2, pair, 0)

    for b in range(1, rows // WINDOW):
        hear(b - 1)
        tell(b)
        load(b).wait()
        bulk_block(b)
    hear(rows // WINDOW - 1)
    exchange_start(0, msg_b1, got_b1)


    @pl.when(last)
    def _():
        pass1(range(len(around)))

    def scaled(center, spread):
        inv = 1.0 / jnp.sqrt(jnp.maximum(spread, 0.0) + 0.1)
        wide = lax.broadcasted_iota(jnp.int32, center.shape, 1)
        return jnp.where(wide % (2 * width) < width, center, pltpu.roll(inv, width, 1))

    def left(v, by):
        return pltpu.roll(v, LANES - by, 1)

    def sum_over(term, shape):
        step = 8
        nothing = tuple(jnp.zeros(shape, jnp.float32) for _ in range(2))

        def some(i, acc):
            acc = list(acc)
            for j in range(step):
                acc[j % 2] = acc[j % 2] + term(i * step + j)
            return tuple(acc)

        if shape[0] <= TILE:
            acc = nothing
            for i in range(peers // step):
                acc = some(i, acc)
        else:
            acc = lax.fori_loop(0, peers // step, some, nothing)
        return acc[0] + acc[1]

    def merge(got, counts, floor, m2, rows_out):
        shape = rows_out.shape
        center = sum_over(lambda p: counts(p) * got[p], shape) / floor

        def spread_term(p):
            d = got[p] - center
            return counts(p) * d * d

        rows_out[...] = scaled(center, (sum_over(spread_term, shape) + m2) / floor)

    def summed(got):
        return sum_over(lambda p: got[p], got.shape[1:])

    def columns_of(row_in, row, which, at=0):
        line = jnp.broadcast_to(row_in[pl.ds(row, 1), :], zero.shape)
        center = {f: column(line, at + f * TILE) for f in which}
        inv = {f: column(line, at + width + f * TILE) for f in which}
        return center, inv

    def clipped_sums(ref, r, row, row_in, which, mark=0.0, at=0, read=0):
        here = pl.ds(pl.multiple_of(r * TILE, TILE), TILE)
        first = t0 + r * TILE if ref is out else t0 + rows + r * TILE
        center, inv = columns_of(row_in, row, which, read)
        s = {f: zero for f in which}
        q = {f: zero for f in which}
        for c in range(chunks):
            _, _, _, w = listed(c, first)
            for f in which:
                y = (ref[f, here, lanes(c)] - center[f]) * inv[f]
                y = jnp.clip(y, -3.0, 3.0)
                if ref is out:
                    ref[f, here, lanes(c)] = jnp.where(w, y, mark)
                y = jnp.where(w, y, 0.0)
                s[f] = s[f] + fold(y)
                q[f] = q[f] + fold(y * y)
        columns = []
        for f in which:
            columns.append((at + f * TILE, across(s[f])))
            columns.append((at + width + f * TILE, across(q[f])))
        return columns

    def clip_tile(ref, r, row, row_in, msg, msg_row, which, mark=0.0):
        columns = clipped_sums(ref, r, row, row_in, which, mark)
        msg[pl.ds(msg_row, 1), :] = flat(columns)

    def merge2(got, floor, rows_out):
        sums = summed(got)
        center = sums / floor
        spread = left(sums, width) / floor - center * center
        rows_out[...] = scaled(center, spread)

    def final_tile(r, row, row_in, which, at=0):
        here = pl.ds(pl.multiple_of(r * TILE, TILE), TILE)
        center, inv = columns_of(row_in, row, which, at)
        for c in range(chunks):
            _, _, _, w = listed(c, t0 + r * TILE)
            for f in which:
                y = (out[f, here, lanes(c)] - center[f]) * inv[f]
                out[f, here, lanes(c)] = jnp.where(w, y, 0.0)

    def over(n, step, unroll=1):
        def one(i, carry):
            step(i)
            return carry

        lax.fori_loop(0, n, one, 0, unroll=unroll)

    def arrival(f, r, h):
        if (f, r, h) in around:
            relay2(around.index((f, r, h))).wait_recv()
        elif h == 0:
            for i, (tile, cut) in enumerate(straight):
                if tile == r and cut[0] == f:
                    direct(i).wait_recv()

    def joined(f, c, here, past):
        h = jnp.where(past, halo[f, here, lanes(c)], 0.0)
        for j in (1, 2, 4):
            up = pltpu.roll(h, TILE - j, 0)
            h = h + jnp.where(subc < TILE - j, up, 0.0)
        before = suffix[f, :, lanes(c)]
        after = jnp.where(subc < TILE - 1, pltpu.roll(h, TILE - 1, 0), 0.0)
        suffix[f, :, lanes(c)] = before + jnp.broadcast_to(h[:1, :], h.shape)
        return out[f, here, lanes(c)] + (before + after)

    def before_mask(c, t, r):
        _, _, _, past = listed(c, t0 + r * TILE - WINDOW)
        return past & (t >= WINDOW)

    def halo_part(r, msg, row, counted_too, which):
        here = tile_rows(r)
        s = {f: zero for f in which}
        q = {f: zero for f in which}
        pivots = {f: ahead[f][:, :1] for f in which}
        for c in range(chunks):
            t, o, u, w = listed(c, t0 + r * TILE)
            past = before_mask(c, t, r)
            part = share(t, o, u, w)
            for f in which:
                rolled = joined(f, c, here, past) * part
                out[f, here, lanes(c)] = rolled
                d = jnp.where(w, rolled - pivots[f], 0.0)
                s[f] = s[f] + fold(d)
                q[f] = q[f] + fold(d * d)
        count = local_count[r][:, :1]
        means, columns = moments(
            count,
            [s[f] for f in which],
            [q[f] for f in which],
            [pivots[f] for f in which],
            which,
        )
        for f, mean in zip(which, means):
            ahead[f] = jnp.broadcast_to(mean, zero.shape)
        if counted_too:
            columns = columns + counts_at(count, 2 * width)
        at = pl.ds(row % DEEP if msg is msg_g1 else row, 1)
        shift = 2 * width * (row // DEEP) if msg is msg_g1 else 0
        msg[at, :] = msg[at, :] + flat([(n + shift, v) for n, v in columns])

    def group_tile(r, which):
        @pl.when(has_prev)
        def _():
            for f in which:
                arrival(f, r, 0)

        halo_part(r, msg_g1, wt - 1 - r, False, which)

    def finish(r, which):
        here = tile_rows(r)
        first = columns_of(told.at[0], r, which)
        then = columns_of(told.at[1], r, which)
        per = chunks // HALVES
        for h in range(HALVES):
            for f in which:
                arrival(f, r, h)
            for c in range(h * per, (h + 1) * per):
                t, o, u, w = listed(c, t0 + r * TILE)
                past = before_mask(c, t, r)
                part = share(t, o, u, w)
                for f in which:
                    y = joined(f, c, here, past) * part
                    y = jnp.clip((y - first[0][f]) * first[1][f], -3.0, 3.0)
                    y = (y - then[0][f]) * then[1][f]
                    out[f, here, lanes(c)] = jnp.where(w, y, 0.0)

    suffix[...] = jnp.zeros_like(suffix)
    msg_e1[...] = jnp.zeros_like(msg_e1)
    msg_g1[...] = jnp.zeros_like(msg_g1)
    msg_e2[...] = jnp.zeros_like(msg_e2)


    def second(ks):
        @pl.when((x == 0) | last)
        def _():
            pass2(ks)

    group_tile(7, every)
    group_tile(6, every)

    @pl.when(x == 0)
    def _():
        for r in range(tops - 1, -1, -1):
            halo_part(r, msg_e1, tops + r, True, early(r))

    exchange_all(0, got_b1).wait_recv()

    def doubled(v):
        high = pltpu.roll(pltpu.roll(v, wt - DEEP, 0), 2 * width, 1)
        return jnp.where(lane < 2 * width, v, high)

    def split(p):
        v = got_b1[p]
        count_b[p] = left(v, 2 * width)
        count_h[p] = doubled(left(v[:wt, :], 3 * width))

    over(peers, split, 8)
    sums = summed(got_b1)
    floor_b[...] = jnp.maximum(left(sums, 2 * width), 1.0)
    floor_h[...] = jnp.maximum(doubled(left(sums[:wt, :], 3 * width)), 1.0)
    merge(got_b1, lambda p: count_b[p], floor_b[...], left(sums, width), row_b1)
    group_tile(5, every)

    @pl.when(has_next)
    def _():
        total[...] = base[...]
        base[...] = jnp.zeros_like(base)
        for copy in extensions:
            copy.wait_recv()

        def one(r, which):
            here = pl.ds(pl.multiple_of(r * TILE, TILE), TILE)
            pivots = [pivot[f][:, :1] for f in every]
            means, line = window_tile(ext, here, t0 + rows + r * TILE, r, pivots, which)
            for f, mean in zip(which, means):
                pivot[f] = jnp.broadcast_to(mean, zero.shape)
            msg_e1[pl.ds(r, 1), :] = line

        over(EARLY, lambda r: one(r, every), EARLY)
        if EXTRA:
            one(EARLY, extra)

    exchange_start(2, msg_e1, got_e1)
    pairs = bulk // 2

    def clip_pair(j):
        columns = clipped_sums(out, j + wt, j, row_b1, every)
        i = j + pairs
        columns += clipped_sums(out, i + wt, i, row_b1, every, at=2 * width)
        msg_b2[pl.ds(j, 1), :] = flat(columns)

    over(pairs, clip_pair)
    exchange_start(1, msg_b2, got_b2)
    some = range(6)

    @pl.when(x < blocks_t - 2)
    def _():
        pass1(some)

    @pl.when(x == blocks_t - 2)
    def _():
        pass2(some)

    group_tile(4, every)
    exchange_all(2, got_e1).wait_recv()

    def split_e(p):
        count_e[p] = left(got_e1[p], 2 * width)

    over(peers, split_e, peers)
    sums = summed(got_e1)
    floor_e = jnp.maximum(left(sums, 2 * width), 1.0)
    first_params, second_params = params.at[0], params.at[1, pl.ds(0, tops)]
    merge(got_e1, lambda p: count_e[p], floor_e, left(sums, width), first_params)

    @pl.when(has_next)
    def _():
        for r in range(tops):
            clip_tile(ext, r, r, first_params, msg_e2, r, early(r))

    @pl.when(x == 0)
    def _():
        for r in range(tops):
            columns = clipped_sums(
                out, r, tops + r, first_params, early(r), at=2 * width
            )
            at = pl.ds(r, 1)
            msg_e2[at, :] = msg_e2[at, :] + flat(columns)

    exchange_start(3, msg_e2, got_e2)
    rest = range(6, len(around))

    @pl.when(x < blocks_t - 2)
    def _():
        pass1(rest)

    @pl.when(x == blocks_t - 2)
    def _():
        pass2(rest)

    group_tile(3, kept[:-1])
    group_tile(3, kept[-1:])
    exchange_start(4, msg_g1, got_g1)
    second([0,1])
    second([2,3])
    exchange_all(3, got_e2).wait_recv()
    upper = pltpu.roll(pltpu.roll(floor_e, tops, 0), 2 * width, 1)
    wide = lax.broadcasted_iota(jnp.int32, floor_e.shape, 1)
    floor_e = jnp.where(wide < 2 * width, floor_e, upper)[:tops, :]
    merge2(got_e2, floor_e, second_params)

    @pl.when(has_next)
    def _():
        telling.start()
        direct(len(straight) - 1).start()


    @pl.when(x == 0)
    def _():
        for r in range(tops):
            final_tile(r, r, second_params, early(r), 2 * width)

    second([4,5])
    exchange_all(4, got_g1).wait_recv()
    second([6,7])
    m2 = left(summed(got_g1), width)
    merge(got_g1, lambda p: count_h[p, :DEEP, :], floor_h[:DEEP, :], m2, row_g1)
    packed = [[] for _ in range(DEEP)]
    for r in range(wt - 1, EARLY - 1, -1):
        i = wt - 1 - r
        at = 2 * width * (i // DEEP)
        packed[i % DEEP] += clipped_sums(
            out, r, i % DEEP, row_g1, grouped(r), MARK, at, at
        )
    for i in range(DEEP):
        msg_g2[pl.ds(i, 1), :] = flat(packed[i])
    exchange_start(5, msg_g2, got_g2)
    second([8,9])
    exchange_all(1, got_b2).wait_recv()
    low, high = floor_b[pl.ds(0, pairs), :], floor_b[pl.ds(pairs, pairs), :]
    wide = lax.broadcasted_iota(jnp.int32, low.shape, 1)
    both = jnp.where(wide < 2 * width, low, pltpu.roll(high, 2 * width, 1))
    merge2(got_b2, both, row_b2)

    def final_pair(j):
        final_tile(j + wt, j, row_b2, every)
        final_tile(j + pairs + wt, j, row_b2, every, 2 * width)

    over(pairs, final_pair)


    @pl.when(has_prev)
    def _():
        telling.wait_recv()


    @pl.when(has_prev)
    def _():
        for r in range(EARLY, tops):
            finish(r, extra)
        for r in range(EARLY - 1, -1, -1):
            finish(r, [f for f in every if (f, r) not in BACK])
            finish(r, [f for f in every if (f, r) in BACK])

    exchange_all(5, got_g2).wait_recv()
    merge2(got_g2, floor_h[:DEEP, :], out.at[0, pl.ds(rows, DEEP), pl.ds(0, LANES)])
    for g, got in enumerate((got_b1, got_b2, got_e1, got_e2, got_g1, got_g2)):
        exchange_all(g, got).wait_send()

    @pl.when(has_prev)
    def _():
        for copy in extensions:
            copy.wait_send()

    @pl.when(has_next)
    def _():
        telling.wait_send()
        for k in range(len(around)):
            back(k).wait_send()
        for i in range(len(straight)):
            direct(i).wait_send()

    @pl.when(hops1)
    def _():
        for k in range(len(around)):
            relay1(k).wait_send()

    @pl.when(hops2)
    def _():
        for k in range(len(around)):
            relay2(k).wait_send()


def writer(x_ref, o_ref, tile_ref, sem, sem_tile):
    fields, rows, assets = o_ref.shape
    wt = WINDOW // TILE
    step = (rows - WINDOW) // 2
    spans = []
    for f in range(fields):
        tops = EARLY + (1 if f >= fields - EXTRA else 0)
        spans.append((f, 0, tops * TILE))
        spans.extend((f, WINDOW + i * step, step) for i in range(2))
    copies = [
        pltpu.make_async_copy(
            x_ref.at[f, pl.ds(at, size), :], o_ref.at[f, pl.ds(at, size), :], sem.at[i]
        )
        for i, (f, at, size) in enumerate(spans)
    ]
    for copy in copies:
        copy.start()
    sub = lax.broadcasted_iota(jnp.int32, (TILE, LANES), 0)
    lane = lax.broadcasted_iota(jnp.int32, (TILE, LANES), 1)
    width = fields * TILE
    for i in range(wt - EARLY):
        r = wt - 1 - i
        many = fields if r > EARLY else fields - EXTRA
        here, there = pl.ds(r * TILE, TILE), pl.ds(i * TILE, TILE)
        row = x_ref[0, pl.ds(rows + i % DEEP, 1), :LANES]
        line = jnp.broadcast_to(row, (TILE, LANES))
        shift = 2 * width * (i // DEEP)

        def column(at):
            kept = jnp.where(lane == sub + at, line, 0.0)
            return jnp.sum(kept, axis=1, keepdims=True)

        for f in range(many):
            center = column(shift + f * TILE)
            inv = column(shift + width + f * TILE)
            for c in range(assets // CHUNK):
                part = pl.ds(c * CHUNK, CHUNK)
                y = x_ref[f, here, part]
                z = jnp.where(y > 3.5, 0.0, (y - center) * inv)
                tile_ref[f, there, part] = z
        copy = pltpu.make_async_copy(
            tile_ref.at[pl.ds(0, many), there, :],
            o_ref.at[pl.ds(0, many), here, :],
            sem_tile.at[i],
        )
        copy.start()
        copies.append(copy)
    for copy in copies:
        copy.wait()


def per_device(blocks_t, peers, values, listed_from, listed_until):
    fields, rows, assets = values.shape
    tiles = rows // TILE
    wt = WINDOW // TILE
    bulk = tiles - wt
    f32 = jnp.float32
    vmem = pltpu.VMEM
    dma = pltpu.SemaphoreType.DMA
    around = len(BACK) * HALVES
    tops = EARLY + (1 if EXTRA else 0)
    groups = (bulk, bulk // 2, 2 * tops, tops, DEEP, DEEP)
    scratch = [
        vmem((1, assets), jnp.int32),
        vmem((1, assets), jnp.int32),
        dma((2,)),
        pltpu.SemaphoreType.REGULAR((4,)),
        vmem((wt, TILE, LANES), f32),
        vmem((fields, WINDOW, assets), f32),
        vmem((around * TILE, assets // HALVES), f32),
        vmem((around * TILE, assets // HALVES), f32),
        vmem((fields, tops * TILE, assets), f32),
        vmem((2, 2 * tops, LANES), f32),
        vmem((2, 2 * tops, LANES), f32),
        vmem((fields, WINDOW, assets), f32),
        vmem((fields, TILE, assets), f32),
        vmem((fields, TILE, assets), f32),
        vmem((fields, TILE, assets), f32),
        vmem((fields, TILE, LANES), f32),
        vmem((fields, TILE, LANES), f32),
        *[vmem((n, LANES), f32) for n in groups],
        *[vmem((peers, n, LANES), f32) for n in groups],
        *[vmem((peers, n, LANES), f32) for n in (bulk, 2 * tops, wt)],
        *[vmem((n, LANES), f32) for n in (bulk, wt)],
        *[vmem((n, LANES), f32) for n in (bulk, bulk // 2, DEEP)],
        dma((rows // WINDOW,)),
        dma,
        dma((2,)),
        dma((2,)),
        dma,
        dma,
        dma,
        dma,
        dma,
        dma((wt + 2,)),
        dma((around,)),
        dma((around,)),
        dma((around,)),
        dma((6,)),
        dma((6,)),
    ]
    clipped = pl.pallas_call(
        functools.partial(kernel, (blocks_t, peers)),
        out_shape=pltpu.VMEM((fields, rows + TILE, assets), values.dtype),
        in_specs=[
            pl.BlockSpec(memory_space=pltpu.HBM),
            pl.BlockSpec(memory_space=pltpu.HBM),
            pl.BlockSpec(memory_space=pltpu.HBM),
        ],
        out_specs=pl.BlockSpec(memory_space=pltpu.VMEM),
        scratch_shapes=scratch,
        compiler_params=pltpu.CompilerParams(
            collective_id=0,
            has_side_effects=True,
            vmem_limit_bytes=48 * 1024 * 1024,
        ),
    )(values, listed_from[None, :], listed_until[None, :])
    return pl.pallas_call(
        writer,
        out_shape=jax.ShapeDtypeStruct(values.shape, values.dtype),
        in_specs=[pl.BlockSpec(memory_space=pltpu.VMEM)],
        out_specs=pl.BlockSpec(memory_space=pltpu.HBM),
        scratch_shapes=[
            vmem((fields, WINDOW - EARLY * TILE, assets), f32),
            dma((3 * fields,)),
            dma((wt - EARLY,)),
        ],
        compiler_params=pltpu.CompilerParams(vmem_limit_bytes=8 * 1024 * 1024),
    )(pltpu.with_memory_space_constraint(clipped, pltpu.VMEM))


def solution(mesh):
    in_specs = (P(None, "tm", "asset"), P("asset"), P("asset"))
    out_specs = P(None, "tm", "asset")
    body = functools.partial(per_device, mesh.shape["tm"], mesh.shape["asset"])
    return jax.shard_map(
        body, mesh=mesh, in_specs=in_specs, out_specs=out_specs, check_vma=False
    )
```

```python
import functools

import jax
import jax.numpy as jnp
from jax import lax
from jax.experimental import pallas as pl
from jax.experimental.pallas import tpu as pltpu
from jax.sharding import PartitionSpec as P

WINDOW = 64
EARLY = 3
BACK = ((3, 2), (3, 1), (2, 1), (3, 0), (2, 0))
EXTRA = 1
HALVES = 2
MARK = 4.0
DEEP = 3
TILE = 8
LANES = 128
CHUNK = 512
MESH = pl.DeviceIdType.MESH


def kernel(
    sizes,
    vals,
    opened_in,
    closed_in,
    out,
    opened,
    closed,
    list_sem,
    rounds,
    local_count,
    halo,
    hop1,
    hop2,
    ext,
    params,
    told,
    ring,
    total,
    base,
    suffix,
    ahead,
    pivot,
    msg_b1,
    msg_b2,
    msg_e1,
    msg_e2,
    msg_g1,
    msg_g2,
    got_b1,
    got_b2,
    got_e1,
    got_e2,
    got_g1,
    got_g2,
    count_b,
    count_e,
    count_h,
    floor_b,
    floor_h,
    row_b1,
    row_b2,
    row_g1,
    load_sem,
    direct_send,
    ext_send,
    ext_recv,
    told_send,
    told_recv,
    back_send,
    relay1_send,
    relay2_send,
    halo_recv,
    back_recv,
    hop1_recv,
    hop2_recv,
    ex_send,
    ex_recv,
):
    blocks_t, peers = sizes
    fields, rows, assets = vals.shape
    tiles = rows // TILE
    wt = WINDOW // TILE
    chunks = assets // CHUNK
    bulk = tiles - wt
    x = lax.axis_index("tm")
    me = lax.axis_index("asset")
    nxt = lax.rem(x + 1, blocks_t)
    prv = lax.rem(x + blocks_t - 1, blocks_t)
    t0 = x * rows

    dates = [
        pltpu.make_async_copy(opened_in, opened, list_sem.at[0]),
        pltpu.make_async_copy(closed_in, closed, list_sem.at[1]),
    ]
    for copy in dates:
        copy.start()

    def load(b):
        part = pl.ds(b * WINDOW, WINDOW)
        return pltpu.make_async_copy(
            vals.at[:, part, :], out.at[:, part, :], load_sem.at[b]
        )

    for b in range(rows // WINDOW):
        load(b).start()

    core = lax.rem(me, 2)
    chip = me // 2
    y, z = chip // 4, lax.rem(chip, 4)

    def at_place(dy, dz, dc):
        to = lax.rem(y + dy, 4) * 4 + lax.rem(z + dz, 4)
        return to * 2 + lax.rem(core + dc, 2)

    near = [at_place(0, 0, 1)]
    near += [at_place(1, 0, 0), at_place(3, 0, 0), at_place(0, 1, 0), at_place(0, 3, 0)]
    barrier = pltpu.get_barrier_semaphore()
    for t in (nxt, prv):
        pl.semaphore_signal(barrier, 1, device_id={"tm": t}, device_id_type=MESH)
    for peer in near:
        pl.semaphore_signal(barrier, 1, device_id={"asset": peer}, device_id_type=MESH)
    pl.semaphore_wait(barrier, 2 + len(near))

    def tell(i):
        for peer in near:
            pl.semaphore_signal(
                rounds.at[i], 1, device_id={"asset": peer}, device_id_type=MESH
            )

    def hear(i):
        pl.semaphore_wait(rounds.at[i], len(near))

    tell(0)

    tail = rows - WINDOW

    def tile_rows(r):
        return pl.ds(r * TILE, TILE)

    def needed(at, r):
        skip = 1 if r == 0 else 0
        return pl.ds(at + skip, TILE - skip)


    every = list(range(fields))
    kept, extra = every[: fields - EXTRA], every[fields - EXTRA :]
    tops = EARLY + (1 if EXTRA else 0)
    piece = assets // HALVES
    tiles_back = sorted({r for _, r in BACK}, reverse=True)
    around = [
        (f, r, h) for t in tiles_back for h in range(HALVES) for f, r in BACK if r == t
    ]

    def early(r):
        return every if r < EARLY else extra

    def grouped(r):
        return every if r > EARLY else kept

    def half(h):
        return pl.ds(h * piece, piece)

    straight = []
    for r in range(wt - 1, -1, -1):
        left_over = [f for f in every if (f, r) not in BACK]
        if r == EARLY:
            cuts = [kept[:-1], kept[-1:], extra]
        else:
            cuts = [left_over]
        straight.extend((r, cut) for cut in cuts if cut)

    def direct(i):
        r, cut = straight[i]
        which = pl.ds(cut[0], len(cut))
        return pltpu.make_async_remote_copy(
            src_ref=vals.at[which, needed(tail + r * TILE, r), :],
            dst_ref=halo.at[which, needed(r * TILE, r), :],
            send_sem=direct_send,
            recv_sem=halo_recv.at[i],
            device_id={"tm": nxt},
            device_id_type=MESH,
        )

    def back(k):
        f, r, h = around[k]
        return pltpu.make_async_remote_copy(
            src_ref=vals.at[f, needed(tail + r * TILE, r), half(h)],
            dst_ref=hop1.at[needed(k * TILE, r), :],
            send_sem=back_send,
            recv_sem=hop1_recv.at[k],
            device_id={"tm": prv},
            device_id_type=MESH,
        )

    def relay1(k):
        part = needed(k * TILE, around[k][1])
        return pltpu.make_async_remote_copy(
            src_ref=hop1.at[part, :],
            dst_ref=hop2.at[part, :],
            send_sem=relay1_send,
            recv_sem=hop2_recv.at[k],
            device_id={"tm": prv},
            device_id_type=MESH,
        )

    def relay2(k):
        f, r, h = around[k]
        return pltpu.make_async_remote_copy(
            src_ref=hop2.at[needed(k * TILE, r), :],
            dst_ref=halo.at[f, needed(r * TILE, r), half(h)],
            send_sem=relay2_send,
            recv_sem=back_recv.at[k],
            device_id={"tm": prv},
            device_id_type=MESH,
        )

    def pass1(ks):
        for k in ks:
            back(k).wait_recv()
            relay1(k).start()

    def pass2(ks):
        for k in ks:
            relay1(k).wait_recv()
            relay2(k).start()

    def extension(i):
        which = (pl.ds(0, fields), pl.ds(fields - EXTRA, EXTRA))[i]
        part = (pl.ds(0, EARLY * TILE), pl.ds(EARLY * TILE, TILE))[i]
        return pltpu.make_async_remote_copy(
            src_ref=vals.at[which, part, :],
            dst_ref=ext.at[which, part, :],
            send_sem=ext_send.at[i],
            recv_sem=ext_recv.at[i],
            device_id={"tm": prv},
            device_id_type=MESH,
        )

    extensions = [extension(i) for i in range(2 if EXTRA else 1)]
    telling = pltpu.make_async_remote_copy(
        src_ref=params,
        dst_ref=told,
        send_sem=told_send,
        recv_sem=told_recv,
        device_id={"tm": nxt},
        device_id_type=MESH,
    )

    has_prev = x > 0
    has_next = x < blocks_t - 1
    last = x == blocks_t - 1
    hops1 = x != blocks_t - 2
    hops2 = x != blocks_t - 3
    @pl.when(has_prev)
    def _():
        for copy in extensions:
            copy.start()

    @pl.when(has_next)
    def _():
        for k in range(len(around)):
            back(k).start()
        for i in range(len(straight) - 1):
            direct(i).start()

    def hops(d):
        return min(d[0], 4 - d[0]) + min(d[1], 4 - d[1]) + d[2] / 2

    places = [(dy, dz, dc) for dy in range(4) for dz in range(4) for dc in range(2)]
    places = sorted(places[1:], key=hops, reverse=True)

    def exchange(g, msg, got, k, peer):
        return pltpu.make_async_remote_copy(
            src_ref=msg,
            dst_ref=got.at[k],
            send_sem=ex_send.at[g],
            recv_sem=ex_recv.at[g],
            device_id={"asset": peer},
            device_id_type=MESH,
        )

    def exchange_start(g, msg, got):
        for d in places:
            k = (d[0] * 4 + d[1]) * 2 + d[2]
            exchange(g, msg, got, k, at_place(*d)).start()
        got[0] = msg[...]

    def exchange_all(g, got):
        others = got.at[pl.ds(1, peers - 1)]
        return pltpu.make_async_remote_copy(
            src_ref=others,
            dst_ref=others,
            send_sem=ex_send.at[g],
            recv_sem=ex_recv.at[g],
            device_id={"asset": me},
            device_id_type=MESH,
        )

    sub = lax.broadcasted_iota(jnp.int32, (TILE, LANES), 0)
    lane = lax.broadcasted_iota(jnp.int32, (TILE, LANES), 1)
    subc = lax.broadcasted_iota(jnp.int32, (TILE, CHUNK), 0)
    width = fields * TILE

    def lanes(c):
        return pl.ds(c * CHUNK, CHUNK)

    def fold(v):
        acc = v[:, :LANES]
        for i in range(1, CHUNK // LANES):
            acc = acc + v[:, i * LANES : (i + 1) * LANES]
        return acc

    def across(v):
        return jnp.sum(v, axis=1, keepdims=True)

    def flat(columns):
        z = jnp.zeros((TILE, LANES), jnp.float32)
        for at, column in columns:
            z = jnp.where(lane == sub + at, column, z)
        return jnp.sum(z, axis=0, keepdims=True)

    def column(row, at):
        return across(jnp.where(lane == sub + at, row, 0.0))

    def listed(c, first):
        t = subc + first
        o = opened[:, lanes(c)]
        u = closed[:, lanes(c)]
        return t, o, u, (t >= o) & (t < u)

    def share(t, o, u, w):
        low = jnp.maximum(jnp.maximum(t - (WINDOW - 1), o), 0)
        high = jnp.minimum(t, u - 1)
        counted = jnp.maximum(high - low + 1, 1).astype(jnp.float32)
        return jnp.where(w, 1.0 / counted, 0.0)

    def moments(count, s, q, pivots, which):
        inverse = 1.0 / jnp.maximum(count, 1.0)
        columns = []
        means = []
        for f, s_l, q_l, pivot_f in zip(which, s, q, pivots):
            s_f, q_f = across(s_l), across(q_l)
            lift = s_f * inverse
            mean = pivot_f + lift
            means.append(mean)
            columns.append((f * TILE, mean))
            columns.append((width + f * TILE, jnp.maximum(q_f - s_f * lift, 0.0)))
        return means, columns

    def counts_at(count, at):
        return [(at + f * TILE, count) for f in range(fields)]

    zero = jnp.zeros((TILE, LANES), jnp.float32)

    for copy in dates:
        copy.wait()
    msg_b1[...] = jnp.zeros_like(msg_b1)
    base[...] = jnp.zeros_like(base)
    load(0).wait()

    def prefix(f, c, w, v):
        p = jnp.where(w, v, 0.0)
        for k in (1, 2, 4):
            p = p + jnp.where(subc >= k, pltpu.roll(p, k, 0), 0.0)
        p = p + base[f, :, lanes(c)]
        base[f, :, lanes(c)] = jnp.broadcast_to(p[TILE - 1 :, :], p.shape)
        return p

    def first_tile(r, carry):
        n = zero
        here = pl.ds(pl.multiple_of(r * TILE, TILE), TILE)
        for c in range(chunks):
            _, _, _, w = listed(c, t0 + r * TILE)
            n = n + fold(jnp.where(w, 1.0, 0.0))
            for f in range(fields):
                p = prefix(f, c, w, out[f, here, lanes(c)])
                ring[f, here, lanes(c)] = p
                out[f, here, lanes(c)] = p
        count = across(n)
        local_count[r] = jnp.broadcast_to(count, zero.shape)
        msg_b1[pl.ds(wt - 1 - r, 1), :] = flat(counts_at(count, 3 * width))
        return carry

    lax.fori_loop(0, wt, first_tile, 0)

    for f in range(fields):
        rough = zero
        for c in range(chunks):
            rough = rough + fold(base[f, :, lanes(c)])
        pivot[f] = jnp.broadcast_to(across(rough) * (1.0 / (WINDOW * assets)), zero.shape)

    def window_tile(ref, here, first, i, pivots, which):
        slot = pl.ds(pl.multiple_of(i * TILE, TILE), TILE)
        n = zero
        s = [zero] * fields
        q = [zero] * fields
        for c in range(chunks):
            t, o, u, w = listed(c, first)
            n = n + fold(jnp.where(w, 1.0, 0.0))
            part = share(t, o, u, w)
            for f in which:
                p = prefix(f, c, w, ref[f, here, lanes(c)])
                old = ring[f, slot, lanes(c)]
                ring[f, slot, lanes(c)] = p
                rolled = (p + (total[f, :, lanes(c)] - old)) * part
                ref[f, here, lanes(c)] = rolled
                d = jnp.where(w, rolled - pivots[f], 0.0)
                s[f] = s[f] + fold(d)
                q[f] = q[f] + fold(d * d)
        count = across(n)
        means, columns = moments(
            count, [s[f] for f in which], [q[f] for f in which], [pivots[f] for f in which], which)
        return means, flat(columns + counts_at(count, 2 * width))

    def bulk_tile(b, i, pivots):
        r = b * wt + i
        here = pl.ds(pl.multiple_of(r * TILE, TILE), TILE)
        means, line = window_tile(out, here, t0 + r * TILE, i, pivots, every)
        at = pl.ds(r - wt, 1)
        msg_b1[at, :] = msg_b1[at, :] + line
        return means

    def bulk_block(b):
        total[...] = base[...]
        base[...] = jnp.zeros_like(base)

        def pair(i, carry):
            pivots = [pivot[f][:, :1] for f in range(fields)]
            lower = bulk_tile(b, 2 * i, pivots)
            upper = bulk_tile(b, 2 * i + 1, pivots)
            for f in range(fields):
                pivot[f] = jnp.broadcast_to(upper[f], zero.shape)
            if b == 1:

                @pl.when(i == 0)
                def _():
                    for f in range(fields):
                        ahead[f] = jnp.broadcast_to(lower[f], zero.shape)

            return carry

        lax.fori_loop(0, wt // 2, pair, 0)

    for b in range(1, rows // WINDOW):
        hear(b - 1)
        tell(b)
        load(b).wait()
        bulk_block(b)
    hear(rows // WINDOW - 1)
    exchange_start(0, msg_b1, got_b1)


    @pl.when(last)
    def _():
        pass1(range(len(around)))

    def scaled(center, spread):
        inv = 1.0 / jnp.sqrt(jnp.maximum(spread, 0.0) + 0.1)
        wide = lax.broadcasted_iota(jnp.int32, center.shape, 1)
        return jnp.where(wide % (2 * width) < width, center, pltpu.roll(inv, width, 1))

    def left(v, by):
        return pltpu.roll(v, LANES - by, 1)

    def sum_over(term, shape):
        step = 8
        nothing = tuple(jnp.zeros(shape, jnp.float32) for _ in range(2))

        def some(i, acc):
            acc = list(acc)
            for j in range(step):
                acc[j % 2] = acc[j % 2] + term(i * step + j)
            return tuple(acc)

        if shape[0] <= TILE:
            acc = nothing
            for i in range(peers // step):
                acc = some(i, acc)
        else:
            acc = lax.fori_loop(0, peers // step, some, nothing)
        return acc[0] + acc[1]

    def merge(got, counts, floor, m2, rows_out):
        shape = rows_out.shape
        center = sum_over(lambda p: counts(p) * got[p], shape) / floor

        def spread_term(p):
            d = got[p] - center
            return counts(p) * d * d

        rows_out[...] = scaled(center, (sum_over(spread_term, shape) + m2) / floor)

    def summed(got):
        return sum_over(lambda p: got[p], got.shape[1:])

    def columns_of(row_in, row, which, at=0):
        line = jnp.broadcast_to(row_in[pl.ds(row, 1), :], zero.shape)
        center = {f: column(line, at + f * TILE) for f in which}
        inv = {f: column(line, at + width + f * TILE) for f in which}
        return center, inv

    def clipped_sums(ref, r, row, row_in, which, mark=0.0, at=0, read=0):
        here = pl.ds(pl.multiple_of(r * TILE, TILE), TILE)
        first = t0 + r * TILE if ref is out else t0 + rows + r * TILE
        center, inv = columns_of(row_in, row, which, read)
        s = {f: zero for f in which}
        q = {f: zero for f in which}
        for c in range(chunks):
            _, _, _, w = listed(c, first)
            for f in which:
                y = (ref[f, here, lanes(c)] - center[f]) * inv[f]
                y = jnp.clip(y, -3.0, 3.0)
                if ref is out:
                    ref[f, here, lanes(c)] = jnp.where(w, y, mark)
                y = jnp.where(w, y, 0.0)
                s[f] = s[f] + fold(y)
                q[f] = q[f] + fold(y * y)
        columns = []
        for f in which:
            columns.append((at + f * TILE, across(s[f])))
            columns.append((at + width + f * TILE, across(q[f])))
        return columns

    def clip_tile(ref, r, row, row_in, msg, msg_row, which, mark=0.0):
        columns = clipped_sums(ref, r, row, row_in, which, mark)
        msg[pl.ds(msg_row, 1), :] = flat(columns)

    def merge2(got, floor, rows_out):
        sums = summed(got)
        center = sums / floor
        spread = left(sums, width) / floor - center * center
        rows_out[...] = scaled(center, spread)

    def final_tile(r, row, row_in, which, at=0):
        here = pl.ds(pl.multiple_of(r * TILE, TILE), TILE)
        center, inv = columns_of(row_in, row, which, at)
        for c in range(chunks):
            _, _, _, w = listed(c, t0 + r * TILE)
            for f in which:
                y = (out[f, here, lanes(c)] - center[f]) * inv[f]
                out[f, here, lanes(c)] = jnp.where(w, y, 0.0)

    def over(n, step, unroll=1):
        def one(i, carry):
            step(i)
            return carry

        lax.fori_loop(0, n, one, 0, unroll=unroll)

    def arrival(f, r, h):
        if (f, r, h) in around:
            relay2(around.index((f, r, h))).wait_recv()
        elif h == 0:
            for i, (tile, cut) in enumerate(straight):
                if tile == r and cut[0] == f:
                    direct(i).wait_recv()

    def joined(f, c, here, past):
        h = jnp.where(past, halo[f, here, lanes(c)], 0.0)
        for j in (1, 2, 4):
            up = pltpu.roll(h, TILE - j, 0)
            h = h + jnp.where(subc < TILE - j, up, 0.0)
        before = suffix[f, :, lanes(c)]
        after = jnp.where(subc < TILE - 1, pltpu.roll(h, TILE - 1, 0), 0.0)
        suffix[f, :, lanes(c)] = before + jnp.broadcast_to(h[:1, :], h.shape)
        return out[f, here, lanes(c)] + (before + after)

    def before_mask(c, t, r):
        _, _, _, past = listed(c, t0 + r * TILE - WINDOW)
        return past & (t >= WINDOW)

    def halo_part(r, msg, row, counted_too, which):
        here = tile_rows(r)
        s = {f: zero for f in which}
        q = {f: zero for f in which}
        pivots = {f: ahead[f][:, :1] for f in which}
        for c in range(chunks):
            t, o, u, w = listed(c, t0 + r * TILE)
            past = before_mask(c, t, r)
            part = share(t, o, u, w)
            for f in which:
                rolled = joined(f, c, here, past) * part
                out[f, here, lanes(c)] = rolled
                d = jnp.where(w, rolled - pivots[f], 0.0)
                s[f] = s[f] + fold(d)
                q[f] = q[f] + fold(d * d)
        count = local_count[r][:, :1]
        means, columns = moments(
            count,
            [s[f] for f in which],
            [q[f] for f in which],
            [pivots[f] for f in which],
            which,
        )
        for f, mean in zip(which, means):
            ahead[f] = jnp.broadcast_to(mean, zero.shape)
        if counted_too:
            columns = columns + counts_at(count, 2 * width)
        at = pl.ds(row % DEEP if msg is msg_g1 else row, 1)
        shift = 2 * width * (row // DEEP) if msg is msg_g1 else 0
        msg[at, :] = msg[at, :] + flat([(n + shift, v) for n, v in columns])

    def group_tile(r, which):
        @pl.when(has_prev)
        def _():
            for f in which:
                arrival(f, r, 0)

        halo_part(r, msg_g1, wt - 1 - r, False, which)

    def finish(r, which):
        here = tile_rows(r)
        first = columns_of(told.at[0], r, which)
        then = columns_of(told.at[1], r, which)
        per = chunks // HALVES
        for h in range(HALVES):
            for f in which:
                arrival(f, r, h)
            for c in range(h * per, (h + 1) * per):
                t, o, u, w = listed(c, t0 + r * TILE)
                past = before_mask(c, t, r)
                part = share(t, o, u, w)
                for f in which:
                    y = joined(f, c, here, past) * part
                    y = jnp.clip((y - first[0][f]) * first[1][f], -3.0, 3.0)
                    y = (y - then[0][f]) * then[1][f]
                    out[f, here, lanes(c)] = jnp.where(w, y, 0.0)

    suffix[...] = jnp.zeros_like(suffix)
    msg_e1[...] = jnp.zeros_like(msg_e1)
    msg_g1[...] = jnp.zeros_like(msg_g1)
    msg_e2[...] = jnp.zeros_like(msg_e2)


    def second(ks):
        @pl.when((x == 0) | last)
        def _():
            pass2(ks)

    group_tile(7, every)
    group_tile(6, every)

    @pl.when(x == 0)
    def _():
        for r in range(tops - 1, -1, -1):
            halo_part(r, msg_e1, tops + r, True, early(r))

    exchange_all(0, got_b1).wait_recv()

    def doubled(v):
        high = pltpu.roll(pltpu.roll(v, wt - DEEP, 0), 2 * width, 1)
        return jnp.where(lane < 2 * width, v, high)

    def split(p):
        v = got_b1[p]
        count_b[p] = left(v, 2 * width)
        count_h[p] = doubled(left(v[:wt, :], 3 * width))

    over(peers, split, 8)
    sums = summed(got_b1)
    floor_b[...] = jnp.maximum(left(sums, 2 * width), 1.0)
    floor_h[...] = jnp.maximum(doubled(left(sums[:wt, :], 3 * width)), 1.0)
    merge(got_b1, lambda p: count_b[p], floor_b[...], left(sums, width), row_b1)
    group_tile(5, every)

    @pl.when(has_next)
    def _():
        total[...] = base[...]
        base[...] = jnp.zeros_like(base)
        for copy in extensions:
            copy.wait_recv()

        def one(r, which):
            here = pl.ds(pl.multiple_of(r * TILE, TILE), TILE)
            pivots = [pivot[f][:, :1] for f in every]
            means, line = window_tile(ext, here, t0 + rows + r * TILE, r, pivots, which)
            for f, mean in zip(which, means):
                pivot[f] = jnp.broadcast_to(mean, zero.shape)
            msg_e1[pl.ds(r, 1), :] = line

        over(EARLY, lambda r: one(r, every), EARLY)
        if EXTRA:
            one(EARLY, extra)

    exchange_start(2, msg_e1, got_e1)
    pairs = bulk // 2

    def clip_pair(j):
        columns = clipped_sums(out, j + wt, j, row_b1, every)
        i = j + pairs
        columns += clipped_sums(out, i + wt, i, row_b1, every, at=2 * width)
        msg_b2[pl.ds(j, 1), :] = flat(columns)

    over(pairs, clip_pair)
    exchange_start(1, msg_b2, got_b2)
    some = range(6)

    @pl.when(x < blocks_t - 2)
    def _():
        pass1(some)

    @pl.when(x == blocks_t - 2)
    def _():
        pass2(some)

    group_tile(4, every)
    exchange_all(2, got_e1).wait_recv()

    def split_e(p):
        count_e[p] = left(got_e1[p], 2 * width)

    over(peers, split_e, peers)
    sums = summed(got_e1)
    floor_e = jnp.maximum(left(sums, 2 * width), 1.0)
    first_params, second_params = params.at[0], params.at[1, pl.ds(0, tops)]
    merge(got_e1, lambda p: count_e[p], floor_e, left(sums, width), first_params)

    @pl.when(has_next)
    def _():
        for r in range(tops):
            clip_tile(ext, r, r, first_params, msg_e2, r, early(r))

    @pl.when(x == 0)
    def _():
        for r in range(tops):
            columns = clipped_sums(
                out, r, tops + r, first_params, early(r), at=2 * width
            )
            at = pl.ds(r, 1)
            msg_e2[at, :] = msg_e2[at, :] + flat(columns)

    exchange_start(3, msg_e2, got_e2)
    rest = range(6, len(around))

    @pl.when(x < blocks_t - 2)
    def _():
        pass1(rest)

    @pl.when(x == blocks_t - 2)
    def _():
        pass2(rest)

    group_tile(3, kept[:-1])
    group_tile(3, kept[-1:])
    exchange_start(4, msg_g1, got_g1)
    second([0,1])
    second([2,3])
    exchange_all(3, got_e2).wait_recv()
    upper = pltpu.roll(pltpu.roll(floor_e, tops, 0), 2 * width, 1)
    wide = lax.broadcasted_iota(jnp.int32, floor_e.shape, 1)
    floor_e = jnp.where(wide < 2 * width, floor_e, upper)[:tops, :]
    merge2(got_e2, floor_e, second_params)

    @pl.when(has_next)
    def _():
        telling.start()
        direct(len(straight) - 1).start()


    @pl.when(x == 0)
    def _():
        for r in range(tops):
            final_tile(r, r, second_params, early(r), 2 * width)

    second([4,5])
    exchange_all(4, got_g1).wait_recv()
    second([6,7])
    m2 = left(summed(got_g1), width)
    merge(got_g1, lambda p: count_h[p, :DEEP, :], floor_h[:DEEP, :], m2, row_g1)
    packed = [[] for _ in range(DEEP)]
    for r in range(wt - 1, EARLY - 1, -1):
        i = wt - 1 - r
        at = 2 * width * (i // DEEP)
        packed[i % DEEP] += clipped_sums(
            out, r, i % DEEP, row_g1, grouped(r), MARK, at, at
        )
    for i in range(DEEP):
        msg_g2[pl.ds(i, 1), :] = flat(packed[i])
    exchange_start(5, msg_g2, got_g2)
    second([8,9])
    exchange_all(1, got_b2).wait_recv()
    low, high = floor_b[pl.ds(0, pairs), :], floor_b[pl.ds(pairs, pairs), :]
    wide = lax.broadcasted_iota(jnp.int32, low.shape, 1)
    both = jnp.where(wide < 2 * width, low, pltpu.roll(high, 2 * width, 1))
    merge2(got_b2, both, row_b2)

    def final_pair(j):
        final_tile(j + wt, j, row_b2, every)
        final_tile(j + pairs + wt, j, row_b2, every, 2 * width)

    over(pairs, final_pair)


    @pl.when(has_prev)
    def _():
        telling.wait_recv()


    @pl.when(has_prev)
    def _():
        for r in range(EARLY, tops):
            finish(r, extra)
        for r in range(EARLY - 1, -1, -1):
            finish(r, [f for f in every if (f, r) not in BACK])
            finish(r, [f for f in every if (f, r) in BACK])

    exchange_all(5, got_g2).wait_recv()
    merge2(got_g2, floor_h[:DEEP, :], out.at[0, pl.ds(rows, DEEP), pl.ds(0, LANES)])
    for g, got in enumerate((got_b1, got_b2, got_e1, got_e2, got_g1, got_g2)):
        exchange_all(g, got).wait_send()

    @pl.when(has_prev)
    def _():
        for copy in extensions:
            copy.wait_send()

    @pl.when(has_next)
    def _():
        telling.wait_send()
        for k in range(len(around)):
            back(k).wait_send()
        for i in range(len(straight)):
            direct(i).wait_send()

    @pl.when(hops1)
    def _():
        for k in range(len(around)):
            relay1(k).wait_send()

    @pl.when(hops2)
    def _():
        for k in range(len(around)):
            relay2(k).wait_send()


def writer(x_ref, o_ref, tile_ref, sem, sem_tile):
    fields, rows, assets = o_ref.shape
    wt = WINDOW // TILE
    step = (rows - WINDOW) // 4
    spans = []
    for f in range(fields):
        tops = EARLY + (1 if f >= fields - EXTRA else 0)
        spans.append((f, 0, tops * TILE))
        spans.extend((f, WINDOW + i * step, step) for i in range(4))
    copies = [
        pltpu.make_async_copy(
            x_ref.at[f, pl.ds(at, size), :], o_ref.at[f, pl.ds(at, size), :], sem.at[i]
        )
        for i, (f, at, size) in enumerate(spans)
    ]
    for copy in copies:
        copy.start()
    sub = lax.broadcasted_iota(jnp.int32, (TILE, LANES), 0)
    lane = lax.broadcasted_iota(jnp.int32, (TILE, LANES), 1)
    width = fields * TILE
    for i in range(wt - EARLY):
        r = wt - 1 - i
        many = fields if r > EARLY else fields - EXTRA
        here, there = pl.ds(r * TILE, TILE), pl.ds(i * TILE, TILE)
        row = x_ref[0, pl.ds(rows + i % DEEP, 1), :LANES]
        line = jnp.broadcast_to(row, (TILE, LANES))
        shift = 2 * width * (i // DEEP)

        def column(at):
            kept = jnp.where(lane == sub + at, line, 0.0)
            return jnp.sum(kept, axis=1, keepdims=True)

        for f in range(many):
            center = column(shift + f * TILE)
            inv = column(shift + width + f * TILE)
            for c in range(assets // CHUNK):
                part = pl.ds(c * CHUNK, CHUNK)
                y = x_ref[f, here, part]
                z = jnp.where(y > 3.5, 0.0, (y - center) * inv)
                tile_ref[f, there, part] = z
        copy = pltpu.make_async_copy(
            tile_ref.at[pl.ds(0, many), there, :],
            o_ref.at[pl.ds(0, many), here, :],
            sem_tile.at[i],
        )
        copy.start()
        copies.append(copy)
    for copy in copies:
        copy.wait()


def per_device(blocks_t, peers, values, listed_from, listed_until):
    fields, rows, assets = values.shape
    tiles = rows // TILE
    wt = WINDOW // TILE
    bulk = tiles - wt
    f32 = jnp.float32
    vmem = pltpu.VMEM
    dma = pltpu.SemaphoreType.DMA
    around = len(BACK) * HALVES
    tops = EARLY + (1 if EXTRA else 0)
    groups = (bulk, bulk // 2, 2 * tops, tops, DEEP, DEEP)
    scratch = [
        vmem((1, assets), jnp.int32),
        vmem((1, assets), jnp.int32),
        dma((2,)),
        pltpu.SemaphoreType.REGULAR((4,)),
        vmem((wt, TILE, LANES), f32),
        vmem((fields, WINDOW, assets), f32),
        vmem((around * TILE, assets // HALVES), f32),
        vmem((around * TILE, assets // HALVES), f32),
        vmem((fields, tops * TILE, assets), f32),
        vmem((2, 2 * tops, LANES), f32),
        vmem((2, 2 * tops, LANES), f32),
        vmem((fields, WINDOW, assets), f32),
        vmem((fields, TILE, assets), f32),
        vmem((fields, TILE, assets), f32),
        vmem((fields, TILE, assets), f32),
        vmem((fields, TILE, LANES), f32),
        vmem((fields, TILE, LANES), f32),
        *[vmem((n, LANES), f32) for n in groups],
        *[vmem((peers, n, LANES), f32) for n in groups],
        *[vmem((peers, n, LANES), f32) for n in (bulk, 2 * tops, wt)],
        *[vmem((n, LANES), f32) for n in (bulk, wt)],
        *[vmem((n, LANES), f32) for n in (bulk, bulk // 2, DEEP)],
        dma((rows // WINDOW,)),
        dma,
        dma((2,)),
        dma((2,)),
        dma,
        dma,
        dma,
        dma,
        dma,
        dma((wt + 2,)),
        dma((around,)),
        dma((around,)),
        dma((around,)),
        dma((6,)),
        dma((6,)),
    ]
    clipped = pl.pallas_call(
        functools.partial(kernel, (blocks_t, peers)),
        out_shape=pltpu.VMEM((fields, rows + TILE, assets), values.dtype),
        in_specs=[
            pl.BlockSpec(memory_space=pltpu.HBM),
            pl.BlockSpec(memory_space=pltpu.HBM),
            pl.BlockSpec(memory_space=pltpu.HBM),
        ],
        out_specs=pl.BlockSpec(memory_space=pltpu.VMEM),
        scratch_shapes=scratch,
        compiler_params=pltpu.CompilerParams(
            collective_id=0,
            has_side_effects=True,
            vmem_limit_bytes=48 * 1024 * 1024,
        ),
    )(values, listed_from[None, :], listed_until[None, :])
    return pl.pallas_call(
        writer,
        out_shape=jax.ShapeDtypeStruct(values.shape, values.dtype),
        in_specs=[pl.BlockSpec(memory_space=pltpu.VMEM)],
        out_specs=pl.BlockSpec(memory_space=pltpu.HBM),
        scratch_shapes=[
            vmem((fields, WINDOW - EARLY * TILE, assets), f32),
            dma((5 * fields,)),
            dma((wt - EARLY,)),
        ],
        compiler_params=pltpu.CompilerParams(vmem_limit_bytes=8 * 1024 * 1024),
    )(pltpu.with_memory_space_constraint(clipped, pltpu.VMEM))


def solution(mesh):
    in_specs = (P(None, "tm", "asset"), P("asset"), P("asset"))
    out_specs = P(None, "tm", "asset")
    body = functools.partial(per_device, mesh.shape["tm"], mesh.shape["asset"])
    return jax.shard_map(
        body, mesh=mesh, in_specs=in_specs, out_specs=out_specs, check_vma=False
    )
```
